32 devices in a mesh: gx: 4 (over z), gy: 8 (over y, x, core).
Axes of the slice: x: 2, y: 2, z: 4, core: 2. Of those that a mesh axis runs over, the one named last changes fastest.
Arguments:
- right_side: float32 [512, 2048], P('gx', 'gy'), may hold values from -1.2 to 1.2
- shift: float32 [512, 2048], P('gx', 'gy'), may hold values from 0.0001 to 0.004
Outputs:
- solution: float32 [512, 2048], P('gx', 'gy')
- residual: float32 [512, 2048], P('gx', 'gy')
The draws below stay inside these ranges and needn't reach their ends.
All inputs are finite; a program needn't handle non-finite values.
Results may differ from the reference program's by a relative error of at most 0.0003.
Values sent between devices are 32-bit elements; how exact they have to be, the bound alone decides.
No kernel may reach another device: no remote copies, remote signals or barrier semaphores. Data moves between devices by JAX's collectives and lax.ppermute only.
A program may use at most 128 MiB of HBM per device.

```python
import math
import jax
import jax.numpy as jnp

LEVELS = 4
COARSE_SWEEPS = 6
NX = 512
NY = 2048


def draw_right_side(key, part):
    return jnp.clip(0.2 * jax.random.normal(key, (NX, NY), jnp.float32), -1.2, 1.2)


def steps_of(own_key, shape, shards, smallest, largest):
    def one(position, shards_of):
        draws = jax.random.uniform(jax.random.fold_in(jax.random.fold_in(own_key, 6), position), (shards_of,), jnp.float32, smallest / len(shards), largest / len(shards))
        return jnp.repeat(jnp.exp(draws), shape[position] // shards_of).reshape((-1,) + (1,) * (len(shape) - position - 1))

    factor_of = one(*shards[0])
    for cut in shards[1:]:
        factor_of = factor_of * one(*cut)
    return factor_of


def setup_inputs(seed: int = 0) -> dict:
    key_list = jax.random.split(jax.random.key(seed), 3)
    right_side = draw_right_side(jax.random.fold_in(key_list[2], 71), 0)
    shift = jnp.clip(jnp.exp(math.log(0.004) - 3.6888795 * jax.random.uniform(key_list[1], (NX, NY), jnp.float32) ** steps_of(key_list[1], (NX, NY), ((0, 4), (1, 8)), -0.2, 0.2)), 0.0001, 0.004)
    return dict(right_side=right_side, shift=shift)


damping = 0.8


def restrict(values):
    rows, columns = values.shape
    blocks = values.reshape(rows // 2, 2, columns // 2, 2)
    return 0.25 * (blocks[:, 0, :, 0] + blocks[:, 1, :, 0] + blocks[:, 0, :, 1] + blocks[:, 1, :, 1])


def prolong(values):
    rows, columns = values.shape
    copies = jnp.broadcast_to(values[:, None, :, None], (rows, 2, columns, 2))
    return copies.reshape(2 * rows, 2 * columns)


def operate_padded(padded, shifts, level):
    centre = padded[1:-1, 1:-1]
    beside = padded[2:, 1:-1] + padded[:-2, 1:-1] + padded[1:-1, 2:] + padded[1:-1, :-2]
    return 4.0 ** (-level) * (4.0 * centre - beside) + shifts * centre


def apply_operator(field, shifts, level):
    return operate_padded(jnp.pad(field, 1), shifts, level)


def sweeps(iterate, source, shifts, level, count):
    diagonal = 4.0 ** (1 - level) + shifts
    for turn in range(count):
        if iterate is None:
            iterate = damping * source / diagonal
        else:
            iterate = iterate + damping * (source - apply_operator(iterate, shifts, level)) / diagonal
    return iterate


def coarse_solve(iterate, source, shifts):
    unit_total = jnp.sum(apply_operator(jnp.ones_like(source), shifts, LEVELS))
    if iterate is None:
        left = jnp.sum(source)
        iterate = jnp.zeros_like(source) + left / unit_total
    else:
        left = jnp.sum(source - apply_operator(iterate, shifts, LEVELS))
        iterate = iterate + left / unit_total
    return sweeps(iterate, source, shifts, LEVELS, COARSE_SWEEPS)


def vcycle(level, iterate, source, shift_list):
    shifts = shift_list[level]
    if level == LEVELS:
        return coarse_solve(iterate, source, shifts)
    iterate = sweeps(iterate, source, shifts, level, 2)
    coarse_rhs = restrict(source - apply_operator(iterate, shifts, level))
    iterate = iterate + prolong(vcycle(level + 1, None, coarse_rhs, shift_list))
    return sweeps(iterate, source, shifts, level, 2)


def fcycle(level, source, shift_list):
    shifts = shift_list[level]
    if level == LEVELS:
        return coarse_solve(None, source, shifts)
    iterate = sweeps(None, source, shifts, level, 2)
    coarse_rhs = restrict(source - apply_operator(iterate, shifts, level))
    correction = fcycle(level + 1, coarse_rhs, shift_list)
    correction = vcycle(level + 1, correction, coarse_rhs, shift_list)
    iterate = iterate + prolong(correction)
    return sweeps(iterate, source, shifts, level, 2)


def reference(right_side, shift):
    shift_list = [shift]
    for level in range(LEVELS):
        shift_list.append(restrict(shift_list[-1]))
    solution = fcycle(0, right_side, shift_list)
    residual = right_side - apply_operator(solution, shift, 0)
    return solution, residual
```

```python
import numpy as np
import jax
import jax.numpy as jnp
from jax import lax
from jax.experimental import pallas as pl
from jax.experimental.pallas import tpu as pltpu
from jax.sharding import PartitionSpec as P

LEVELS = 4
COARSE_SWEEPS = 6
DAMPING = 0.8
HALO = 24


def f32dot_right(values, onehot):
    high = values.astype(jnp.bfloat16)
    rest = values - high.astype(jnp.float32)
    middle = rest.astype(jnp.bfloat16)
    low = (rest - middle.astype(jnp.float32)).astype(jnp.bfloat16)
    rows = values.shape[0]
    stacked = jnp.concatenate([high, middle, low], axis=0)
    out = jnp.dot(stacked, onehot, preferred_element_type=jnp.float32)
    return (out[2 * rows :] + out[rows : 2 * rows]) + out[:rows]


def f32dot_left(onehot, values):
    high = values.astype(jnp.bfloat16)
    rest = values - high.astype(jnp.float32)
    middle = rest.astype(jnp.bfloat16)
    low = (rest - middle.astype(jnp.float32)).astype(jnp.bfloat16)
    total = jnp.dot(onehot, low, preferred_element_type=jnp.float32)
    total = total + jnp.dot(onehot, middle, preferred_element_type=jnp.float32)
    return total + jnp.dot(onehot, high, preferred_element_type=jnp.float32)


def around(v):
    rows, columns = v.shape
    up = pltpu.roll(v, 1, 0)
    down = pltpu.roll(v, rows - 1, 0)
    left = pltpu.roll(v, 1, 1)
    right = pltpu.roll(v, columns - 1, 1)
    return (up + down) + (left + right)


def sweep(v, g, w):
    return (1.0 - DAMPING) * v + w * (g + around(v))


class Sizes:
    def __init__(self, rows, columns, nx, ny):
        self.rows, self.columns, self.nx, self.ny = rows, columns, nx, ny
        self.p, self.q = rows // 16, columns // 16
        self.lanes = self.p * self.q
        self.devices = nx * ny

        def up(n):
            return -(-n // 128) * 128

        self.ext_rows = [(rows + 2 * HALO) >> l for l in range(3)]
        self.ext_columns = [up((columns + 2 * HALO) >> l) for l in range(3)]

    def column_at(self, level):
        own, halo, width = self.columns >> level, HALO >> level, self.ext_columns[level]
        lane = np.arange(width)
        inside = (lane < own + halo) | (lane >= width - halo)
        return np.where(lane < own + halo, lane, lane - width), inside

    def row_at(self, level):
        own, halo, height = self.rows >> level, HALO >> level, self.ext_rows[level]
        row = np.arange(height)
        return np.where(row < own + halo, row, row - height)

    def restrict_columns(self):
        fine, fine_in = self.column_at(0)
        coarse, coarse_in = self.column_at(1)
        hit = (fine[:, None] // 2 == coarse[None, :]) & fine_in[:, None] & coarse_in[None, :]
        return hit.astype(jnp.bfloat16)

    def pack_columns(self):
        x = np.arange(self.columns // 2)[:, None, None]
        r = np.arange(4)[None, :, None]
        lane = np.arange(self.lanes)[None, None, :]
        hit = x // 2 == 4 * (lane // self.p) + r
        return hit.reshape(self.columns // 2, 4 * self.lanes).astype(jnp.bfloat16)

    def pack_rows(self, fields):
        count = self.rows // 4
        f = np.arange(fields)
        s = np.arange(4)
        k = np.arange(count)
        hit = (f[:, None, None, None] == f[None, None, :, None]) & (k[None, None, None, :] % 4 == s[None, :, None, None])
        hit = hit.reshape(fields * 4, fields * count)
        pad = -hit.shape[0] % 8
        return np.pad(hit, ((0, pad), (0, 0))).astype(jnp.bfloat16)

    def spread_rows(self):
        k = self.row_at(1) // 2
        count = self.rows // 4
        block = k // count
        s = (k % count) % 4
        slot = (block + 1) * 4 + s
        return (slot[:, None] == np.arange(16)[None, :]).astype(jnp.bfloat16)

    def spread_columns(self):
        column, inside = self.column_at(1)
        m = column // 2
        count = self.columns // 4
        block = m // count
        r = (m % count) % 4
        q = (m % count) // 4
        beside = np.arange(2)[:, None, None, None]
        rr = np.arange(4)[None, :, None, None]
        lane = np.arange(self.lanes)[None, None, :, None]
        hit = ((block != 0) == beside) & (r == rr) & (q == lane // self.p) & inside
        return hit.reshape(8 * self.lanes, -1).astype(jnp.bfloat16)


def iota(shape, axis):
    return lax.broadcasted_iota(jnp.int32, shape, axis)


def inside_mask(sizes, level, gx, gy):
    shape = (sizes.ext_rows[level], sizes.ext_columns[level])
    own_r, own_c, halo = sizes.rows >> level, sizes.columns >> level, HALO >> level
    row, column = iota(shape, 0), iota(shape, 1)
    last_row = jnp.where(gx < sizes.nx - 1, own_r + halo, own_r)
    first_row = jnp.where(gx > 0, own_r + halo, shape[0])
    last_column = jnp.where(gy < sizes.ny - 1, own_c + halo, own_c)
    first_column = jnp.where(gy > 0, shape[1] - halo, shape[1])
    return ((row < last_row) | (row >= first_row)) & ((column < last_column) | (column >= first_column))


def pair_rows(scratch, values):
    rows, columns = values.shape
    outs = []
    for t in range(columns // 128):
        scratch[t, :rows, :] = values[:, t * 128 : (t + 1) * 128]
    for t in range(columns // 128):
        outs.append(scratch[t, pl.ds(0, rows // 2, stride=2), :] + scratch[t, pl.ds(1, rows // 2, stride=2), :])
    return jnp.concatenate(outs, axis=1)


def pack(sizes, scratch, fields, columns_ref, rows_ref, out_ref):
    own_r, own_c = sizes.rows // 2, sizes.columns // 2
    count = own_r // 2
    summed = jnp.concatenate([pair_rows(scratch, f[:own_r, :own_c]) for f in fields], axis=0)
    spread = f32dot_right(summed, columns_ref[...])
    shape = spread.shape
    keep = ((iota(shape, 0) % count) // 4) == (iota(shape, 1) % sizes.p)
    spread = jnp.where(keep, spread, 0.0)
    out = f32dot_left(rows_ref[...], spread)
    n = 4 * len(fields)
    for r in range(4):
        out_ref[r * n : (r + 1) * n, :] = out[:n, r * sizes.lanes : (r + 1) * sizes.lanes]


def down_kernel(sizes, at_ref, g_ref, s_ref, left_ref, right_ref, rc_ref, pc_ref, pr_ref,
                g0_ref, d0_ref, w0_ref, v0_ref, c1_ref, d1_ref, w1_ref, v1_ref, out_ref, scratch):
    gx, gy = at_ref[0], at_ref[1]
    rows, columns = sizes.ext_rows[0], sizes.ext_columns[0]
    lane = iota((rows, 128), 1)
    beside = []
    for k in range(2):
        beside.append(jnp.where(lane < HALO, right_ref[k], left_ref[k]))
    g = jnp.concatenate([g_ref[...], beside[0]], axis=1)
    sigma = jnp.concatenate([s_ref[...], beside[1]], axis=1)
    d = 4.0 + sigma
    w = jnp.where(inside_mask(sizes, 0, gx, gy), DAMPING / d, 0.0)
    v = w * g
    v = sweep(v, g, w)
    r = g - d * v + around(v)
    g0_ref[...] = g
    d0_ref[...] = d
    w0_ref[...] = w
    v0_ref[...] = v
    half = rows // 2
    both = jnp.concatenate([pair_rows(scratch, r), pair_rows(scratch, sigma)], axis=0)
    both = f32dot_right(both, rc_ref[...])
    g, sigma = both[:half], both[half:]
    d = 4.0 + sigma
    w = jnp.where(inside_mask(sizes, 1, gx, gy), DAMPING / d, 0.0)
    v = w * g
    v = sweep(v, g, w)
    r = g - d * v + around(v)
    c1_ref[...] = g
    d1_ref[...] = d
    w1_ref[...] = w
    v1_ref[...] = v
    pack(sizes, scratch, [r, sigma], pc_ref, pr_ref, out_ref)


class Coarse:
    def __init__(self, sizes, d_refs, w_refs, g_refs, v_refs, t_refs):
        self.z = sizes
        self.d, self.w, self.g, self.v, self.t = d_refs, w_refs, g_refs, v_refs, t_refs
        shape = (sizes.ny, sizes.lanes)
        lane, row = iota(shape, 1), iota(shape, 0)
        p, q = lane % sizes.p, lane // sizes.p
        self.first_p, self.last_p = p == 0, p == sizes.p - 1
        self.first_q, self.last_q = q == 0, q == sizes.q - 1
        self.first_row, self.last_row = row == 0, row == sizes.ny - 1

    def blocks(self, body):
        if self.z.nx <= 4:
            for gx in range(self.z.nx):
                body((gx + 1) * self.z.ny)
        else:
            def step(gx, carry):
                body(pl.multiple_of((gx + 1) * self.z.ny, 8))
                return carry

            lax.fori_loop(0, self.z.nx, step, 0)

    def at(self, ref, s, r, base):
        return ref[s, r, pl.ds(base, self.z.ny), :]

    def put(self, ref, s, r, base, value):
        ref[s, r, pl.ds(base, self.z.ny), :] = value

    def neighbours(self, ref, s, r, n, base):
        z = self.z
        if r < n - 1:
            right = self.at(ref, s, r + 1, base)
        else:
            x = self.at(ref, s, 0, base)
            moved = jnp.where(self.last_row, 0.0, pltpu.roll(x, z.ny - 1, 0))
            right = pltpu.roll(jnp.where(self.first_q, moved, x), z.lanes - z.p, 1)
        if r > 0:
            left = self.at(ref, s, r - 1, base)
        else:
            x = self.at(ref, s, n - 1, base)
            moved = jnp.where(self.first_row, 0.0, pltpu.roll(x, 1, 0))
            left = pltpu.roll(jnp.where(self.last_q, moved, x), z.p, 1)
        if s < n - 1:
            down = self.at(ref, s + 1, r, base)
        else:
            here = pltpu.roll(self.at(ref, 0, r, base), z.lanes - 1, 1)
            there = pltpu.roll(self.at(ref, 0, r, base + z.ny), z.p - 1, 1)
            down = jnp.where(self.last_p, there, here)
        if s > 0:
            up = self.at(ref, s - 1, r, base)
        else:
            here = pltpu.roll(self.at(ref, n - 1, r, base), 1, 1)
            there = pltpu.roll(self.at(ref, n - 1, r, base - z.ny), z.lanes - z.p + 1, 1)
            up = jnp.where(self.first_p, there, here)
        return (up + down) + (left + right)

    def each(self, level, body):
        n = 1 << (LEVELS - level)

        def block(base):
            for s in range(n):
                for r in range(n):
                    body(s, r, n, base)

        self.blocks(block)

    def first_sweep(self, level):
        l = level - 2

        def body(s, r, n, base):
            self.put(self.v[l], s, r, base, self.at(self.w[l], s, r, base) * self.at(self.g[l], s, r, base))

        self.each(level, body)

    def sweep(self, level, source, target):
        l = level - 2

        def body(s, r, n, base):
            v = self.at(source, s, r, base)
            total = self.at(self.g[l], s, r, base) + self.neighbours(source, s, r, n, base)
            self.put(target, s, r, base, (1.0 - DAMPING) * v + self.at(self.w[l], s, r, base) * total)

        self.each(level, body)

    def two_sweeps(self, level):
        l = level - 2
        self.sweep(level, self.v[l], self.t[l])
        self.sweep(level, self.t[l], self.v[l])

    def start(self, level):
        l = level - 2
        self.first_sweep(level)
        self.sweep(level, self.v[l], self.t[l])
        self.v[l], self.t[l] = self.t[l], self.v[l]

    def residual(self, level, s, r, n, base):
        l = level - 2
        v = self.at(self.v[l], s, r, base)
        g = self.at(self.g[l], s, r, base)
        return (g - self.at(self.d[l], s, r, base) * v) + self.neighbours(self.v[l], s, r, n, base)

    def restrict(self, level):
        l = level - 2
        n = 1 << (LEVELS - level)

        def block(base):
            for s in range(n // 2):
                for r in range(n // 2):
                    parts = [self.residual(level, 2 * s + a, 2 * r + b, n, base) for a in (0, 1) for b in (0, 1)]
                    self.put(self.g[l + 1], s, r, base, (parts[0] + parts[1]) + (parts[2] + parts[3]))

        self.blocks(block)

    def prolong(self, level):
        l = level - 2

        def body(s, r, n, base):
            e = self.at(self.v[l + 1], s // 2, r // 2, base)
            self.put(self.v[l], s, r, base, self.at(self.v[l], s, r, base) + e)

        self.each(level, body)

    def total(self, of):
        z = self.z
        if z.nx <= 4:
            parts = [of((gx + 1) * z.ny) for gx in range(z.nx)]
            value = parts[0]
            for part in parts[1:]:
                value = value + part
        else:
            value = lax.fori_loop(
                0, z.nx, lambda gx, acc: acc + of(pl.multiple_of((gx + 1) * z.ny, 8)),
                jnp.zeros((z.ny, z.lanes), jnp.float32))
        return jnp.sum(jnp.sum(value, axis=0, keepdims=True), axis=1, keepdims=True)

    def unit(self):
        z = self.z
        top = LEVELS - 2
        missing = 2.0 * (z.nx * z.p + z.ny * z.q) - 0.0
        cells = 4.0
        total = self.total(lambda base: self.at(self.d[top], 0, 0, base) - cells)
        return total + missing

    def coarse(self, fresh, unit):
        top = LEVELS - 2
        v, t, g = self.v[top], self.t[top], self.g[top]
        if fresh:
            left = self.total(lambda base: self.at(g, 0, 0, base)) / unit

            def body(base):
                self.put(v, 0, 0, base, jnp.broadcast_to(left, (self.z.ny, self.z.lanes)))
        else:
            left = self.total(lambda base: self.residual(LEVELS, 0, 0, 1, base)) / unit

            def body(base):
                self.put(v, 0, 0, base, self.at(v, 0, 0, base) + left)

        self.blocks(body)
        for turn in range(COARSE_SWEEPS // 2):
            self.sweep(LEVELS, v, t)
            self.sweep(LEVELS, t, v)

    def vcycle(self, level, fresh, unit):
        if level == LEVELS:
            self.coarse(fresh, unit)
            return
        if fresh:
            self.start(level)
        else:
            self.two_sweeps(level)
        self.restrict(level)
        self.vcycle(level + 1, True, unit)
        self.prolong(level)
        self.two_sweeps(level)

    def fcycle(self, level, unit):
        if level == LEVELS:
            self.coarse(True, unit)
            return
        self.start(level)
        self.restrict(level)
        self.fcycle(level + 1, unit)
        self.vcycle(level + 1, False, unit)
        self.prolong(level)
        self.two_sweeps(level)

    def clear_ends(self):
        z = self.z
        zero = jnp.zeros((z.ny, z.lanes), jnp.float32)
        for refs in (self.v, self.t):
            for ref in refs:
                n = ref.shape[0]
                for s in range(n):
                    for r in range(n):
                        ref[s, r, : z.ny, :] = zero
                        ref[s, r, (z.nx + 1) * z.ny :, :] = zero

    def take(self, y_ref, target, count, offset, add):
        z = self.z

        def block(base):
            for s in range(4):
                for r in range(4):
                    first = (base - z.ny) * 4 * count + r * count + offset + s
                    value = y_ref[pl.ds(first, z.ny, stride=4 * count), :]
                    self.put(target, s, r, base, value + add if add else value)

        self.blocks(block)

    def spread(self, gx, gy, rows_ref, columns_ref, e_ref):
        z = self.z
        row = (gx + 1) * z.ny + gy
        lane = iota((1, z.lanes), 1)
        low_half = lane // z.p < z.q // 2
        has_left, has_right = gy > 0, gy < z.ny - 1
        e_ref[12:, :] = jnp.zeros((4, 8 * z.lanes), jnp.float32)
        for dx in range(3):
            base = row + (dx - 1) * z.ny
            for s in range(4):
                for r in range(4):
                    ref = self.v[0]
                    own = ref[s, r, pl.ds(base, 1), :]
                    left = ref[s, r, pl.ds(jnp.where(has_left, base - 1, 0), 1), :]
                    right = ref[s, r, pl.ds(jnp.where(has_right, base + 1, 0), 1), :]
                    k = dx * 4 + s
                    e_ref[k : k + 1, r * z.lanes : (r + 1) * z.lanes] = own
                    e_ref[k : k + 1, (4 + r) * z.lanes : (5 + r) * z.lanes] = jnp.where(low_half, right, left)
        spread = f32dot_left(rows_ref[...], e_ref[...])
        shape = spread.shape
        index = iota(shape, 0)
        own_r, halo = z.rows // 2, HALO // 2
        cell = jnp.where(index < own_r + halo, index, index - shape[0]) + 2 * z.rows
        keep = ((cell // 8) % z.p) == (iota(shape, 1) % z.p)
        spread = jnp.where(keep, spread, 0.0)
        return f32dot_right(spread, columns_ref[...])


def level_shape(sizes, level):
    n = 1 << (LEVELS - level)
    return (n, n, (sizes.nx + 2) * sizes.ny, sizes.lanes)


def middle_kernel(sizes, at_ref, y_ref, c1_ref, d1_ref, w1_ref, v1_ref, sr_ref, sc_ref, pc_ref, pr_ref,
                  d2_ref, d3_ref, d4_ref, w2_ref, w3_ref, w4_ref, e1_ref, out_ref,
                  g2, g3, g4, v2, v3, v4, t2, t3, t4, e_ref, scratch):
    gx, gy = at_ref[0], at_ref[1]
    m = Coarse(sizes, [d2_ref, d3_ref, d4_ref], [w2_ref, w3_ref, w4_ref], [g2, g3, g4], [v2, v3, v4], [t2, t3, t4])
    m.clear_ends()
    m.take(y_ref, g2, 8, 0, 0.0)
    m.take(y_ref, d2_ref, 8, 4, 4.0)
    for l in range(2):
        n = 2 >> l

        def block(base):
            for s in range(n):
                for r in range(n):
                    parts = [m.at(m.d[l], 2 * s + a, 2 * r + b, base) for a in (0, 1) for b in (0, 1)]
                    m.put(m.d[l + 1], s, r, base, ((parts[0] + parts[1]) + (parts[2] + parts[3])) - 12.0)

        m.blocks(block)
    for l in range(3):
        def body(s, r, n, base):
            m.put(m.w[l], s, r, base, DAMPING / m.at(m.d[l], s, r, base))

        m.each(l + 2, body)
    unit = m.unit()
    m.fcycle(2, unit)
    m.vcycle(2, False, unit)
    g, d, w = c1_ref[...], d1_ref[...], w1_ref[...]
    v = v1_ref[...] + jnp.where(w > 0.0, m.spread(gx, gy, sr_ref, sc_ref, e_ref), 0.0)
    for turn in range(4):
        v = sweep(v, g, w)
    e1_ref[...] = v
    r = g - d * v + around(v)
    pack(sizes, scratch, [r], pc_ref, pr_ref, out_ref)


def up_kernel(sizes, at_ref, y_ref, d2_ref, d3_ref, d4_ref, w2_ref, w3_ref, w4_ref, c1_ref, w1_ref, e1_ref,
              g0_ref, d0_ref, w0_ref, v0_ref, sr_ref, sc_ref, rt_ref,
              solution_ref, residual_ref, g2, g3, g4, v2, v3, v4, t2, t3, t4, e_ref, scratch):
    gx, gy = at_ref[0], at_ref[1]
    m = Coarse(sizes, [d2_ref, d3_ref, d4_ref], [w2_ref, w3_ref, w4_ref], [g2, g3, g4], [v2, v3, v4], [t2, t3, t4])
    m.clear_ends()
    m.take(y_ref, g2, 4, 0, 0.0)
    unit = m.unit()
    m.vcycle(2, True, unit)
    g, w = c1_ref[...], w1_ref[...]
    v = e1_ref[...] + jnp.where(w > 0.0, m.spread(gx, gy, sr_ref, sc_ref, e_ref), 0.0)
    for turn in range(2):
        v = sweep(v, g, w)
    wide = f32dot_right(v, rt_ref[...])
    half = wide.shape[0]
    tiles = wide.shape[1] // 128
    for t in range(tiles):
        part = wide[:, t * 128 : (t + 1) * 128]
        scratch[t, pl.ds(0, half, stride=2), :] = part
        scratch[t, pl.ds(1, half, stride=2), :] = part
    g, d, w = g0_ref[...], d0_ref[...], w0_ref[...]
    v = v0_ref[...] + jnp.concatenate([scratch[t] for t in range(tiles)], axis=1)
    for turn in range(2):
        v = sweep(v, g, w)
    r = g - d * v + around(v)
    solution_ref[...] = v[: sizes.rows, : sizes.columns]
    residual_ref[...] = r[: sizes.rows, : sizes.columns]


def vmem(count):
    return [pl.BlockSpec(memory_space=pltpu.VMEM)] * count


def call(kernel, sizes, outs, scratch, *operands):
    shapes = [jax.ShapeDtypeStruct(shape, jnp.float32) for shape in outs]
    return pl.pallas_call(
        lambda *refs: kernel(sizes, *refs),
        name=kernel.__name__,
        out_shape=shapes,
        in_specs=[pl.BlockSpec(memory_space=pltpu.SMEM)] + vmem(len(operands) - 1),
        out_specs=vmem(len(outs)),
        scratch_shapes=[pltpu.VMEM(shape, jnp.float32) for shape in scratch],
    )(*operands)


def ring(values, axis, step):
    count = lax.axis_size(axis)
    return lax.ppermute(values, axis, [(i, (i + step) % count) for i in range(count)])


def gather(block, axes):
    count = lax.axis_size(axes)
    copies = jnp.broadcast_to(block[None], (count,) + block.shape)
    out = lax.all_to_all(copies, axes, 0, 0, tiled=True)
    return out.reshape(count * block.shape[0], block.shape[1])


def body(right_side, shift):
    nx, ny = lax.axis_size("gx"), lax.axis_size("gy")
    rows, columns = right_side.shape
    z = Sizes(rows, columns, nx, ny)
    at = jnp.stack([lax.axis_index("gx"), lax.axis_index("gy")]).astype(jnp.int32)
    both = jnp.stack([right_side, shift])
    below = ring(both[:, :HALO], "gx", -1)
    above = ring(both[:, rows - HALO :], "gx", 1)
    both = jnp.concatenate([both, below, above], axis=1)
    right = ring(both[:, :, :128], "gy", -1)
    left = ring(both[:, :, columns - 128 :], "gy", 1)
    restrict_columns = z.restrict_columns()
    pack_columns, spread_rows, spread_columns = z.pack_columns(), z.spread_rows(), z.spread_columns()
    fine, half = (z.ext_rows[0], z.ext_columns[0]), (z.ext_rows[1], z.ext_columns[1])
    tiles = (z.ext_columns[0] // 128, z.ext_rows[0], 128)
    g0, d0, w0, v0, c1, d1, w1, v1, packed = call(
        down_kernel, z, [fine] * 4 + [half] * 4 + [(32, z.lanes)], [tiles],
        at, both[0], both[1], left, right, restrict_columns, pack_columns, z.pack_rows(2))
    y = gather(packed, ("gx", "gy"))
    slabs = [level_shape(z, level) for level in (2, 3, 4)]
    work = slabs * 3 + [(16, 8 * z.lanes), tiles]
    d2, d3, d4, w2, w3, w4, e1, packed = call(
        middle_kernel, z, slabs * 2 + [half, (16, z.lanes)], work,
        at, y, c1, d1, w1, v1, spread_rows, spread_columns, pack_columns, z.pack_rows(1))
    y = gather(packed, ("gx", "gy"))
    return call(
        up_kernel, z, [(rows, columns)] * 2, work,
        at, y, d2, d3, d4, w2, w3, w4, c1, w1, e1, g0, d0, w0, v0,
        spread_rows, spread_columns, restrict_columns.T)


def solution(mesh):
    specs = (P("gx", "gy"), P("gx", "gy"))

    def run(right_side, shift):
        out = body(right_side, shift)
        return out[0], out[1]

    return jax.shard_map(run, mesh=mesh, in_specs=specs, out_specs=specs, check_vma=False)
```

```python
import numpy as np
import jax
import jax.numpy as jnp
from jax import lax
from jax.experimental import pallas as pl
from jax.experimental.pallas import tpu as pltpu
from jax.sharding import PartitionSpec as P

LEVELS = 4
COARSE_SWEEPS = 6
DAMPING = 0.8
HALO = 48


def f32dot_right(values, onehot):
    high = values.astype(jnp.bfloat16)
    rest = values - high.astype(jnp.float32)
    middle = rest.astype(jnp.bfloat16)
    low = (rest - middle.astype(jnp.float32)).astype(jnp.bfloat16)
    rows = values.shape[0]
    stacked = jnp.concatenate([high, middle, low], axis=0)
    out = jnp.dot(stacked, onehot, preferred_element_type=jnp.float32)
    return (out[2 * rows :] + out[rows : 2 * rows]) + out[:rows]


def f32dot_left(onehot, values):
    high = values.astype(jnp.bfloat16)
    rest = values - high.astype(jnp.float32)
    middle = rest.astype(jnp.bfloat16)
    low = (rest - middle.astype(jnp.float32)).astype(jnp.bfloat16)
    total = jnp.dot(onehot, low, preferred_element_type=jnp.float32)
    total = total + jnp.dot(onehot, middle, preferred_element_type=jnp.float32)
    return total + jnp.dot(onehot, high, preferred_element_type=jnp.float32)


def around(v):
    rows, columns = v.shape
    up = pltpu.roll(v, 1, 0)
    down = pltpu.roll(v, rows - 1, 0)
    left = pltpu.roll(v, 1, 1)
    right = pltpu.roll(v, columns - 1, 1)
    return (up + down) + (left + right)


def sweep(v, g, w):
    return (1.0 - DAMPING) * v + w * (g + around(v))


class Sizes:
    def __init__(self, rows, columns, nx, ny):
        self.rows, self.columns, self.nx, self.ny = rows, columns, nx, ny
        self.p, self.q = rows // 16, columns // 16
        self.lanes = self.p * self.q
        self.devices = nx * ny

        def up(n):
            return -(-n // 128) * 128

        self.ext_rows = [(rows + 2 * HALO) >> l for l in range(3)]
        self.ext_columns = [up((columns + 2 * HALO) >> l) for l in range(3)]

    def column_at(self, level):
        own, halo, width = self.columns >> level, HALO >> level, self.ext_columns[level]
        lane = np.arange(width)
        inside = (lane < own + halo) | (lane >= width - halo)
        return np.where(lane < own + halo, lane, lane - width), inside

    def row_at(self, level):
        own, halo, height = self.rows >> level, HALO >> level, self.ext_rows[level]
        row = np.arange(height)
        return np.where(row < own + halo, row, row - height)

    def restrict_columns(self, level):
        fine, fine_in = self.column_at(level)
        coarse, coarse_in = self.column_at(level + 1)
        hit = (fine[:, None] // 2 == coarse[None, :]) & fine_in[:, None] & coarse_in[None, :]
        return hit.astype(jnp.bfloat16)

    def pack_columns(self, level, pairs):
        n = 1 << (LEVELS - level)
        own = self.columns >> level
        x = np.arange(self.ext_columns[2])[:, None, None]
        cell = x // 2 if pairs else x
        r = np.arange(n)[None, :, None]
        lane = np.arange(self.lanes)[None, None, :]
        hit = (cell == n * (lane // self.p) + r) & (cell < own)
        return hit.reshape(len(x), n * self.lanes).astype(jnp.bfloat16)

    def pack_rows(self, level, fields):
        n = 1 << (LEVELS - level)
        count = self.rows >> level
        f = np.arange(fields)
        s = np.arange(n)
        k = np.arange(count)
        hit = (f[:, None, None, None] == f[None, None, :, None]) & (k[None, None, None, :] % n == s[None, :, None, None])
        hit = hit.reshape(fields * n, fields * count)
        pad = -hit.shape[0] % 8
        return np.pad(hit, ((0, pad), (0, 0))).astype(jnp.bfloat16)

    def spread_rows(self, level):
        n = 1 << (LEVELS - level)
        k = self.row_at(level - 1) // 2
        count = self.rows >> level
        slot = (k // count + 1) * n + (k % count) % n
        width = 3 * n + (-3 * n) % 8
        return (slot[:, None] == np.arange(width)[None, :]).astype(jnp.bfloat16)

    def spread_columns(self, level):
        n = 1 << (LEVELS - level)
        column, inside = self.column_at(level - 1)
        m = column // 2
        count = self.columns >> level
        block = m // count
        r = (m % count) % n
        q = (m % count) // n
        beside = np.arange(2)[:, None, None, None]
        rr = np.arange(n)[None, :, None, None]
        lane = np.arange(self.lanes)[None, None, :, None]
        hit = ((block != 0) == beside) & (r == rr) & (q == lane // self.p) & inside
        return hit.reshape(2 * n * self.lanes, -1).astype(jnp.bfloat16)


def iota(shape, axis):
    return lax.broadcasted_iota(jnp.int32, shape, axis)


def inside_mask(sizes, level, gx, gy):
    shape = (sizes.ext_rows[level], sizes.ext_columns[level])
    own_r, own_c, halo = sizes.rows >> level, sizes.columns >> level, HALO >> level
    row, column = iota(shape, 0), iota(shape, 1)
    last_row = jnp.where(gx < sizes.nx - 1, own_r + halo, own_r)
    first_row = jnp.where(gx > 0, own_r + halo, shape[0])
    last_column = jnp.where(gy < sizes.ny - 1, own_c + halo, own_c)
    first_column = jnp.where(gy > 0, shape[1] - halo, shape[1])
    return ((row < last_row) | (row >= first_row)) & ((column < last_column) | (column >= first_column))


def pair_rows(scratch, values):
    rows, columns = values.shape
    outs = []
    for t in range(columns // 128):
        scratch[t, :rows, :] = values[:, t * 128 : (t + 1) * 128]
    for t in range(columns // 128):
        outs.append(scratch[t, pl.ds(0, rows // 2, stride=2), :] + scratch[t, pl.ds(1, rows // 2, stride=2), :])
    return jnp.concatenate(outs, axis=1)


def double_rows(scratch, values):
    rows, columns = values.shape
    for t in range(columns // 128):
        part = values[:, t * 128 : (t + 1) * 128]
        scratch[t, pl.ds(0, rows, stride=2), :] = part
        scratch[t, pl.ds(1, rows, stride=2), :] = part
    return jnp.concatenate([scratch[t, : 2 * rows, :] for t in range(columns // 128)], axis=1)


def pack(sizes, level, fields, columns_ref, rows_ref, out_ref):
    n = 1 << (LEVELS - level)
    count = sizes.rows >> level
    spread = f32dot_right(jnp.concatenate(fields, axis=0), columns_ref[...])
    shape = spread.shape
    keep = ((iota(shape, 0) % count) // n) == (iota(shape, 1) % sizes.p)
    out = f32dot_left(rows_ref[...], jnp.where(keep, spread, 0.0))
    height = n * len(fields)
    block = jnp.concatenate([out[:height, r * sizes.lanes : (r + 1) * sizes.lanes] for r in range(n)], axis=0)
    copies = max(1, 8 // block.shape[0])
    block = jnp.concatenate([block] * copies, axis=0)
    for k in range(out_ref.shape[0] // block.shape[0]):
        out_ref[k * block.shape[0] : (k + 1) * block.shape[0], :] = block


def strip_kernel(sizes, at_ref, g_ref, s_ref, below_ref, above_ref, left_ref, right_ref):
    last = sizes.columns - 128
    for rows, sources in ((slice(0, sizes.rows), (g_ref, s_ref)),
                          (slice(sizes.rows, sizes.rows + HALO), (below_ref.at[0], below_ref.at[1])),
                          (slice(sizes.rows + HALO, sizes.rows + 2 * HALO), (above_ref.at[0], above_ref.at[1]))):
        g, s = sources
        first_g, first_s = g[:, :128], s[:, :128]
        last_g, last_s = g[:, last:], s[:, last:]
        lane = iota(first_g.shape, 1)
        left_ref[rows, :] = jnp.where(lane < HALO, first_g, pltpu.roll(first_s, HALO, 1))
        right_ref[rows, :] = jnp.where(lane >= 128 - HALO, last_g, pltpu.roll(last_s, 128 - HALO, 1))


def coefficients(sizes, level, gx, gy, sigma):
    d = 4.0 + sigma
    return d, jnp.where(inside_mask(sizes, level, gx, gy), DAMPING / d, 0.0)


def down_kernel(sizes, at_ref, g_ref, s_ref, below_ref, above_ref, left_ref, right_ref, rc0_ref, rc1_ref, pc_ref, pr_ref,
                g0_ref, d0_ref, w0_ref, v0_ref, c1_ref, d1_ref, w1_ref, v1_ref, d2_ref, w2_ref, out_ref, scratch):
    gx, gy = at_ref[0], at_ref[1]
    rows = sizes.ext_rows[0]
    lane = iota((rows, 128), 1)
    from_left, from_right = left_ref[...], right_ref[...]
    g = jnp.where(lane < HALO, from_right, from_left)
    sigma = jnp.where(lane < HALO, pltpu.roll(from_right, 128 - HALO, 1), pltpu.roll(from_left, HALO, 1))
    g = jnp.concatenate([jnp.concatenate([g_ref[...], below_ref[0], above_ref[0]], axis=0), g], axis=1)
    sigma = jnp.concatenate([jnp.concatenate([s_ref[...], below_ref[1], above_ref[1]], axis=0), sigma], axis=1)
    d, w = coefficients(sizes, 0, gx, gy, sigma)
    v = w * g
    v = sweep(v, g, w)
    r = g - d * v + around(v)
    g0_ref[...] = g
    d0_ref[...] = d
    w0_ref[...] = w
    v0_ref[...] = v
    half = rows // 2
    both = jnp.concatenate([pair_rows(scratch, r), pair_rows(scratch, sigma)], axis=0)
    both = f32dot_right(both, rc0_ref[...])
    g, sigma = both[:half], both[half:]
    d, w = coefficients(sizes, 1, gx, gy, sigma)
    v = w * g
    v = sweep(v, g, w)
    r = g - d * v + around(v)
    c1_ref[...] = g
    d1_ref[...] = d
    w1_ref[...] = w
    v1_ref[...] = v
    half = half // 2
    both = jnp.concatenate([pair_rows(scratch, r), pair_rows(scratch, sigma)], axis=0)
    both = f32dot_right(both, rc1_ref[...])
    g, sigma = both[:half], both[half:]
    d, w = coefficients(sizes, 2, gx, gy, sigma)
    d2_ref[...] = d
    w2_ref[...] = w
    own = sizes.rows // 4
    pack(sizes, 2, [g[:own], sigma[:own]], pc_ref, pr_ref, out_ref)


class Coarse:
    def __init__(self, sizes, first, d_refs, w_refs, g_refs, v_refs, t_refs):
        self.z = sizes
        self.first = first
        self.d, self.w, self.g, self.v, self.t = d_refs, w_refs, g_refs, v_refs, t_refs
        shape = (sizes.ny, sizes.lanes)
        lane, row = iota(shape, 1), iota(shape, 0)
        p, q = lane % sizes.p, lane // sizes.p
        self.first_p, self.last_p = p == 0, p == sizes.p - 1
        self.first_q, self.last_q = q == 0, q == sizes.q - 1
        self.first_row, self.last_row = row == 0, row == sizes.ny - 1

    def blocks(self, body):
        if self.z.nx <= 4:
            for gx in range(self.z.nx):
                body((gx + 1) * self.z.ny)
        else:
            def step(gx, carry):
                body(pl.multiple_of((gx + 1) * self.z.ny, 8))
                return carry

            lax.fori_loop(0, self.z.nx, step, 0)

    def at(self, ref, s, r, base):
        return ref[s, r, pl.ds(base, self.z.ny), :]

    def put(self, ref, s, r, base, value):
        ref[s, r, pl.ds(base, self.z.ny), :] = value

    def neighbours(self, ref, s, r, n, base):
        z = self.z
        if r < n - 1:
            right = self.at(ref, s, r + 1, base)
        else:
            x = self.at(ref, s, 0, base)
            moved = jnp.where(self.last_row, 0.0, pltpu.roll(x, z.ny - 1, 0))
            right = pltpu.roll(jnp.where(self.first_q, moved, x), z.lanes - z.p, 1)
        if r > 0:
            left = self.at(ref, s, r - 1, base)
        else:
            x = self.at(ref, s, n - 1, base)
            moved = jnp.where(self.first_row, 0.0, pltpu.roll(x, 1, 0))
            left = pltpu.roll(jnp.where(self.last_q, moved, x), z.p, 1)
        if s < n - 1:
            down = self.at(ref, s + 1, r, base)
        else:
            here = pltpu.roll(self.at(ref, 0, r, base), z.lanes - 1, 1)
            there = pltpu.roll(self.at(ref, 0, r, base + z.ny), z.p - 1, 1)
            down = jnp.where(self.last_p, there, here)
        if s > 0:
            up = self.at(ref, s - 1, r, base)
        else:
            here = pltpu.roll(self.at(ref, n - 1, r, base), 1, 1)
            there = pltpu.roll(self.at(ref, n - 1, r, base - z.ny), z.lanes - z.p + 1, 1)
            up = jnp.where(self.first_p, there, here)
        return (up + down) + (left + right)

    def each(self, level, body):
        n = 1 << (LEVELS - level)

        def block(base):
            for s in range(n):
                for r in range(n):
                    body(s, r, n, base)

        self.blocks(block)

    def first_sweep(self, level):
        l = level - self.first

        def body(s, r, n, base):
            self.put(self.v[l], s, r, base, self.at(self.w[l], s, r, base) * self.at(self.g[l], s, r, base))

        self.each(level, body)

    def sweep(self, level, source, target):
        l = level - self.first

        def body(s, r, n, base):
            v = self.at(source, s, r, base)
            total = self.at(self.g[l], s, r, base) + self.neighbours(source, s, r, n, base)
            self.put(target, s, r, base, (1.0 - DAMPING) * v + self.at(self.w[l], s, r, base) * total)

        self.each(level, body)

    def two_sweeps(self, level):
        l = level - self.first
        self.sweep(level, self.v[l], self.t[l])
        self.sweep(level, self.t[l], self.v[l])

    def start(self, level):
        l = level - self.first
        self.first_sweep(level)
        self.sweep(level, self.v[l], self.t[l])
        self.v[l], self.t[l] = self.t[l], self.v[l]

    def residual(self, level, s, r, n, base):
        l = level - self.first
        v = self.at(self.v[l], s, r, base)
        g = self.at(self.g[l], s, r, base)
        return (g - self.at(self.d[l], s, r, base) * v) + self.neighbours(self.v[l], s, r, n, base)

    def restrict(self, level):
        l = level - self.first
        n = 1 << (LEVELS - level)

        def block(base):
            for s in range(n // 2):
                for r in range(n // 2):
                    parts = [self.residual(level, 2 * s + a, 2 * r + b, n, base) for a in (0, 1) for b in (0, 1)]
                    self.put(self.g[l + 1], s, r, base, (parts[0] + parts[1]) + (parts[2] + parts[3]))

        self.blocks(block)

    def prolong(self, level):
        l = level - self.first

        def body(s, r, n, base):
            e = self.at(self.v[l + 1], s // 2, r // 2, base)
            self.put(self.v[l], s, r, base, self.at(self.v[l], s, r, base) + e)

        self.each(level, body)

    def total(self, of):
        z = self.z
        if z.nx <= 4:
            parts = [of((gx + 1) * z.ny) for gx in range(z.nx)]
            value = parts[0]
            for part in parts[1:]:
                value = value + part
        else:
            value = lax.fori_loop(
                0, z.nx, lambda gx, acc: acc + of(pl.multiple_of((gx + 1) * z.ny, 8)),
                jnp.zeros((z.ny, z.lanes), jnp.float32))
        return jnp.sum(jnp.sum(value, axis=0, keepdims=True), axis=1, keepdims=True)

    def unit(self):
        z = self.z
        top = LEVELS - self.first
        missing = 2.0 * (z.nx * z.p + z.ny * z.q) - 0.0
        cells = 4.0
        total = self.total(lambda base: self.at(self.d[top], 0, 0, base) - cells)
        return total + missing

    def coarse(self, fresh, unit):
        top = LEVELS - self.first
        v, t, g = self.v[top], self.t[top], self.g[top]
        if fresh:
            left = self.total(lambda base: self.at(g, 0, 0, base)) / unit

            def body(base):
                self.put(v, 0, 0, base, jnp.broadcast_to(left, (self.z.ny, self.z.lanes)))
        else:
            left = self.total(lambda base: self.residual(LEVELS, 0, 0, 1, base)) / unit

            def body(base):
                self.put(v, 0, 0, base, self.at(v, 0, 0, base) + left)

        self.blocks(body)
        for turn in range(COARSE_SWEEPS // 2):
            self.sweep(LEVELS, v, t)
            self.sweep(LEVELS, t, v)

    def vcycle(self, level, fresh, unit):
        if level == LEVELS:
            self.coarse(fresh, unit)
            return
        if fresh:
            self.start(level)
        else:
            self.two_sweeps(level)
        self.restrict(level)
        self.vcycle(level + 1, True, unit)
        self.prolong(level)
        self.two_sweeps(level)

    def fcycle(self, level, unit):
        if level == LEVELS:
            self.coarse(True, unit)
            return
        self.start(level)
        self.restrict(level)
        self.fcycle(level + 1, unit)
        self.vcycle(level + 1, False, unit)
        self.prolong(level)
        self.two_sweeps(level)

    def clear_ends(self):
        z = self.z
        zero = jnp.zeros((z.ny, z.lanes), jnp.float32)
        for refs in (self.v, self.t):
            for ref in refs:
                n = ref.shape[0]
                for s in range(n):
                    for r in range(n):
                        ref[s, r, : z.ny, :] = zero
                        ref[s, r, (z.nx + 1) * z.ny :, :] = zero

    def take(self, y_ref, target, offset, height):
        z = self.z
        n = target.shape[0]

        def block(base):
            for s in range(n):
                for r in range(n):
                    first = (base - z.ny) * n * height + r * height + offset + s
                    self.put(target, s, r, base, y_ref[pl.ds(first, z.ny, stride=n * height), :])

        self.blocks(block)

    def take_cores(self, even_ref, odd_ref, target, offset, height, add):
        z = self.z
        n = target.shape[0]
        half = z.ny // 2

        def block(base):
            for s in range(n):
                for r in range(n):
                    first = (base - z.ny) // 2 * n * height + r * height + offset + s
                    for core, ref in ((0, even_ref), (1, odd_ref)):
                        value = ref[pl.ds(first, half, stride=n * height), :]
                        target[s, r, pl.ds(base + core, half, stride=2), :] = value + add if add else value

        self.blocks(block)

    def spread(self, gx, gy, rows_ref, columns_ref, e_ref):
        z = self.z
        n = 1 << (LEVELS - self.first)
        row = (gx + 1) * z.ny + gy
        lane = iota((1, z.lanes), 1)
        low_half = lane // z.p < z.q // 2
        has_left, has_right = gy > 0, gy < z.ny - 1
        e_ref[...] = jnp.zeros(e_ref.shape, jnp.float32)
        ref = self.v[0]
        for dx in range(3):
            base = row + (dx - 1) * z.ny
            for s in range(n):
                for r in range(n):
                    own = ref[s, r, pl.ds(base, 1), :]
                    left = ref[s, r, pl.ds(jnp.where(has_left, base - 1, 0), 1), :]
                    right = ref[s, r, pl.ds(jnp.where(has_right, base + 1, 0), 1), :]
                    k = dx * n + s
                    e_ref[k : k + 1, r * z.lanes : (r + 1) * z.lanes] = own
                    e_ref[k : k + 1, (n + r) * z.lanes : (n + r + 1) * z.lanes] = jnp.where(low_half, right, left)
        spread = f32dot_left(rows_ref[...], e_ref[...])
        shape = spread.shape
        index = iota(shape, 0)
        above = self.first - 1
        own_r, halo = z.rows >> above, HALO >> above
        cell = jnp.where(index < own_r + halo, index, index - shape[0]) + 2 * z.rows
        keep = ((cell // (2 * n)) % z.p) == (iota(shape, 1) % z.p)
        return f32dot_right(jnp.where(keep, spread, 0.0), columns_ref[...])


def level_shape(sizes, level):
    n = 1 << (LEVELS - level)
    return (n, n, (sizes.nx + 2) * sizes.ny, sizes.lanes)


def middle_kernel(sizes, at_ref, y_ref, other_ref, c1_ref, d1_ref, w1_ref, v1_ref, w2l_ref, d2l_ref, sr_ref, sc_ref,
                  rc1_ref, pc_ref, pr_ref,
                  d3_ref, d4_ref, w3_ref, w4_ref, e1_ref, c2_ref, e2_ref, out_ref,
                  d2, w2, g2, g3, g4, v2, v3, v4, t2, t3, t4, e_ref, scratch):
    gx, gy = at_ref[0], at_ref[1]
    m = Coarse(sizes, 2, [d2, d3_ref, d4_ref], [w2, w3_ref, w4_ref], [g2, g3, g4], [v2, v3, v4], [t2, t3, t4])
    m.clear_ends()
    core = lax.rem(gy, 2)

    @pl.when(core == 0)
    def _():
        m.take_cores(y_ref, other_ref, g2, 0, 8, 0.0)
        m.take_cores(y_ref, other_ref, d2, 4, 8, 4.0)

    @pl.when(core == 1)
    def _():
        m.take_cores(other_ref, y_ref, g2, 0, 8, 0.0)
        m.take_cores(other_ref, y_ref, d2, 4, 8, 4.0)

    for l in range(2):
        n = 2 >> l

        def block(base):
            for s in range(n):
                for r in range(n):
                    parts = [m.at(m.d[l], 2 * s + a, 2 * r + b, base) for a in (0, 1) for b in (0, 1)]
                    m.put(m.d[l + 1], s, r, base, ((parts[0] + parts[1]) + (parts[2] + parts[3])) - 12.0)

        m.blocks(block)
    for l in range(3):
        def body(s, r, n, base):
            m.put(m.w[l], s, r, base, DAMPING / m.at(m.d[l], s, r, base))

        m.each(l + 2, body)
    unit = m.unit()
    m.fcycle(2, unit)
    m.vcycle(2, False, unit)
    g, d, w = c1_ref[...], d1_ref[...], w1_ref[...]
    v = v1_ref[...] + jnp.where(w > 0.0, m.spread(gx, gy, sr_ref, sc_ref, e_ref), 0.0)
    for turn in range(4):
        v = sweep(v, g, w)
    e1_ref[...] = v
    r = g - d * v + around(v)
    g = f32dot_right(pair_rows(scratch, r), rc1_ref[...])
    d, w = d2l_ref[...], w2l_ref[...]
    v = w * g
    v = sweep(v, g, w)
    r = g - d * v + around(v)
    c2_ref[...] = g
    e2_ref[...] = v
    pack(sizes, 3, [pair_rows(scratch, r[: sizes.rows // 4])], pc_ref, pr_ref, out_ref)


def up_kernel(sizes, at_ref, y_ref, d3_ref, d4_ref, w3_ref, w4_ref, c2_ref, w2_ref, e2_ref, c1_ref, w1_ref, e1_ref,
              g0_ref, d0_ref, w0_ref, v0_ref, sr_ref, sc_ref, pc1_ref, pc0_ref,
              solution_ref, residual_ref, g3, g4, v3, v4, t3, t4, e_ref, scratch):
    gx, gy = at_ref[0], at_ref[1]
    m = Coarse(sizes, 3, [d3_ref, d4_ref], [w3_ref, w4_ref], [g3, g4], [v3, v4], [t3, t4])
    m.clear_ends()
    m.take(y_ref, g3, 0, 2)
    m.vcycle(3, True, m.unit())
    g, w = c2_ref[...], w2_ref[...]
    v = e2_ref[...] + jnp.where(w > 0.0, m.spread(gx, gy, sr_ref, sc_ref, e_ref), 0.0)
    for turn in range(2):
        v = sweep(v, g, w)
    g, w = c1_ref[...], w1_ref[...]
    v = e1_ref[...] + double_rows(scratch, f32dot_right(v, pc1_ref[...]))
    for turn in range(2):
        v = sweep(v, g, w)
    g, d, w = g0_ref[...], d0_ref[...], w0_ref[...]
    v = v0_ref[...] + double_rows(scratch, f32dot_right(v, pc0_ref[...]))
    for turn in range(2):
        v = sweep(v, g, w)
    r = g - d * v + around(v)
    solution_ref[...] = v[: sizes.rows, : sizes.columns]
    residual_ref[...] = r[: sizes.rows, : sizes.columns]


def vmem(count):
    return [pl.BlockSpec(memory_space=pltpu.VMEM)] * count


def call(kernel, sizes, outs, scratch, *operands):
    shapes = [jax.ShapeDtypeStruct(shape, jnp.float32) for shape in outs]
    return pl.pallas_call(
        lambda *refs: kernel(sizes, *refs),
        name=kernel.__name__,
        out_shape=shapes,
        in_specs=[pl.BlockSpec(memory_space=pltpu.SMEM)] + vmem(len(operands) - 1),
        out_specs=vmem(len(outs)),
        scratch_shapes=[pltpu.VMEM(shape, jnp.float32) for shape in scratch],
    )(*operands)


def ring(values, axis, step):
    count = lax.axis_size(axis)
    return lax.ppermute(values, axis, [(i, (i + step) % count) for i in range(count)])


def gather(copies):
    return lax.all_to_all(copies, ("gx", "gy"), 0, 0, tiled=True)


def gather_by_core(copies, nx, ny):
    index = np.arange(nx * ny)
    groups = [index[core::2].tolist() for core in range(2)]
    own = lax.all_to_all(copies, ("gx", "gy"), 0, 0, tiled=True, axis_index_groups=groups)
    return own, lax.ppermute(own, "gy", [(j, j ^ 1) for j in range(ny)])


def body(right_side, shift):
    nx, ny = lax.axis_size("gx"), lax.axis_size("gy")
    rows, columns = right_side.shape
    z = Sizes(rows, columns, nx, ny)
    at = jnp.stack([lax.axis_index("gx"), lax.axis_index("gy")]).astype(jnp.int32)
    below = ring(jnp.stack([right_side[:HALO], shift[:HALO]]), "gx", -1)
    above = ring(jnp.stack([right_side[rows - HALO :], shift[rows - HALO :]]), "gx", 1)
    ext = [(z.ext_rows[l], z.ext_columns[l]) for l in range(3)]
    strip = (z.ext_rows[0], 128)
    to_left, to_right = call(strip_kernel, z, [strip] * 2, [], at, right_side, shift, below, above)
    right = ring(to_left, "gy", -1)
    left = ring(to_right, "gy", 1)
    rc0, rc1 = z.restrict_columns(0), z.restrict_columns(1)
    tiles = (ext[0][1] // 128, ext[0][0], 128)
    g0, d0, w0, v0, c1, d1, w1, v1, d2, w2, packed = call(
        down_kernel, z, [ext[0]] * 4 + [ext[1]] * 4 + [ext[2]] * 2 + [(nx * ny // 2 * 32, z.lanes)], [tiles],
        at, right_side, shift, below, above, left, right, rc0, rc1, z.pack_columns(2, False), z.pack_rows(2, 2))
    y, other = gather_by_core(packed, nx, ny)
    slabs = [level_shape(z, level) for level in (2, 3, 4)]
    d3, d4, w3, w4, e1, c2, e2, packed = call(
        middle_kernel, z, slabs[1:] * 2 + [ext[1], ext[2], ext[2], (nx * ny * 4, z.lanes)],
        [slabs[0]] * 2 + slabs * 3 + [(16, 8 * z.lanes), tiles],
        at, y, other, c1, d1, w1, v1, w2, d2, z.spread_rows(2), z.spread_columns(2),
        rc1, z.pack_columns(3, True), z.pack_rows(3, 1))
    y = gather(packed)
    return call(
        up_kernel, z, [(rows, columns)] * 2, slabs[1:] * 3 + [(8, 4 * z.lanes), tiles],
        at, y, d3, d4, w3, w4, c2, w2, e2, c1, w1, e1, g0, d0, w0, v0,
        z.spread_rows(3), z.spread_columns(3), rc1.T, rc0.T)


def solution(mesh):
    specs = (P("gx", "gy"), P("gx", "gy"))

    def run(right_side, shift):
        out = body(right_side, shift)
        return out[0], out[1]

    return jax.shard_map(run, mesh=mesh, in_specs=specs, out_specs=specs, check_vma=False)
```

```python
import numpy as np
import jax
import jax.numpy as jnp
from jax import lax
from jax.experimental import pallas as pl
from jax.experimental.pallas import tpu as pltpu
from jax.sharding import PartitionSpec as P

LEVELS = 4
COARSE_SWEEPS = 6
DAMPING = 0.8
HALO = 48


def f32dot_right(values, onehot):
    high = values.astype(jnp.bfloat16)
    rest = values - high.astype(jnp.float32)
    middle = rest.astype(jnp.bfloat16)
    low = (rest - middle.astype(jnp.float32)).astype(jnp.bfloat16)
    rows = values.shape[0]
    stacked = jnp.concatenate([high, middle, low], axis=0)
    out = jnp.dot(stacked, onehot, preferred_element_type=jnp.float32)
    return (out[2 * rows :] + out[rows : 2 * rows]) + out[:rows]


def f32dot_left(onehot, values):
    high = values.astype(jnp.bfloat16)
    rest = values - high.astype(jnp.float32)
    middle = rest.astype(jnp.bfloat16)
    low = (rest - middle.astype(jnp.float32)).astype(jnp.bfloat16)
    total = jnp.dot(onehot, low, preferred_element_type=jnp.float32)
    total = total + jnp.dot(onehot, middle, preferred_element_type=jnp.float32)
    return total + jnp.dot(onehot, high, preferred_element_type=jnp.float32)


def around(v):
    rows, columns = v.shape
    up = pltpu.roll(v, 1, 0)
    down = pltpu.roll(v, rows - 1, 0)
    left = pltpu.roll(v, 1, 1)
    right = pltpu.roll(v, columns - 1, 1)
    return (up + down) + (left + right)


def sweep(v, g, w):
    return (1.0 - DAMPING) * v + w * (g + around(v))


class Sizes:
    def __init__(self, rows, columns, nx, ny):
        self.rows, self.columns, self.nx, self.ny = rows, columns, nx, ny
        self.p, self.q = rows // 16, columns // 16
        self.lanes = self.p * self.q
        self.devices = nx * ny

        def up(n):
            return -(-n // 128) * 128

        self.ext_rows = [(rows + 2 * HALO) >> l for l in range(3)]
        self.ext_columns = [up((columns + 2 * HALO) >> l) for l in range(3)]

    def column_at(self, level):
        own, halo, width = self.columns >> level, HALO >> level, self.ext_columns[level]
        lane = np.arange(width)
        inside = (lane < own + halo) | (lane >= width - halo)
        return np.where(lane < own + halo, lane, lane - width), inside

    def row_at(self, level):
        own, halo, height = self.rows >> level, HALO >> level, self.ext_rows[level]
        row = np.arange(height)
        return np.where(row < own + halo, row, row - height)

    def restrict_columns(self, level):
        fine, fine_in = self.column_at(level)
        coarse, coarse_in = self.column_at(level + 1)
        hit = (fine[:, None] // 2 == coarse[None, :]) & fine_in[:, None] & coarse_in[None, :]
        return hit.astype(jnp.bfloat16)

    def pack_columns(self, level, pairs):
        n = 1 << (LEVELS - level)
        own = self.columns >> level
        x = np.arange(self.ext_columns[2])[:, None, None]
        cell = x // 2 if pairs else x
        r = np.arange(n)[None, :, None]
        lane = np.arange(self.lanes)[None, None, :]
        hit = (cell == n * (lane // self.p) + r) & (cell < own)
        return hit.reshape(len(x), n * self.lanes).astype(jnp.bfloat16)

    def pack_rows(self, level, fields):
        n = 1 << (LEVELS - level)
        count = self.rows >> level
        f = np.arange(fields)
        s = np.arange(n)
        k = np.arange(count)
        hit = (f[:, None, None, None] == f[None, None, :, None]) & (k[None, None, None, :] % n == s[None, :, None, None])
        hit = hit.reshape(fields * n, fields * count)
        pad = -hit.shape[0] % 8
        return np.pad(hit, ((0, pad), (0, 0))).astype(jnp.bfloat16)

    def spread_rows(self, level):
        n = 1 << (LEVELS - level)
        k = self.row_at(level - 1) // 2
        count = self.rows >> level
        slot = (k // count + 1) * n + (k % count) % n
        width = 3 * n + (-3 * n) % 8
        return (slot[:, None] == np.arange(width)[None, :]).astype(jnp.bfloat16)

    def spread_columns(self, level):
        n = 1 << (LEVELS - level)
        column, inside = self.column_at(level - 1)
        m = column // 2
        count = self.columns >> level
        block = m // count
        r = (m % count) % n
        q = (m % count) // n
        beside = np.arange(2)[:, None, None, None]
        rr = np.arange(n)[None, :, None, None]
        lane = np.arange(self.lanes)[None, None, :, None]
        hit = ((block != 0) == beside) & (r == rr) & (q == lane // self.p) & inside
        return hit.reshape(2 * n * self.lanes, -1).astype(jnp.bfloat16)


def iota(shape, axis):
    return lax.broadcasted_iota(jnp.int32, shape, axis)


def inside_mask(sizes, level, gx, gy):
    shape = (sizes.ext_rows[level], sizes.ext_columns[level])
    own_r, own_c, halo = sizes.rows >> level, sizes.columns >> level, HALO >> level
    row, column = iota(shape, 0), iota(shape, 1)
    last_row = jnp.where(gx < sizes.nx - 1, own_r + halo, own_r)
    first_row = jnp.where(gx > 0, own_r + halo, shape[0])
    last_column = jnp.where(gy < sizes.ny - 1, own_c + halo, own_c)
    first_column = jnp.where(gy > 0, shape[1] - halo, shape[1])
    return ((row < last_row) | (row >= first_row)) & ((column < last_column) | (column >= first_column))


def pair_rows(scratch, values):
    rows, columns = values.shape
    outs = []
    for t in range(columns // 128):
        scratch[t, :rows, :] = values[:, t * 128 : (t + 1) * 128]
    for t in range(columns // 128):
        outs.append(scratch[t, pl.ds(0, rows // 2, stride=2), :] + scratch[t, pl.ds(1, rows // 2, stride=2), :])
    return jnp.concatenate(outs, axis=1)


def double_rows(scratch, values):
    rows, columns = values.shape
    for t in range(columns // 128):
        part = values[:, t * 128 : (t + 1) * 128]
        scratch[t, pl.ds(0, rows, stride=2), :] = part
        scratch[t, pl.ds(1, rows, stride=2), :] = part
    return jnp.concatenate([scratch[t, : 2 * rows, :] for t in range(columns // 128)], axis=1)


def pack(sizes, level, fields, columns_ref, rows_ref, out_ref):
    n = 1 << (LEVELS - level)
    count = sizes.rows >> level
    spread = f32dot_right(jnp.concatenate(fields, axis=0), columns_ref[...])
    shape = spread.shape
    keep = ((iota(shape, 0) % count) // n) == (iota(shape, 1) % sizes.p)
    out = f32dot_left(rows_ref[...], jnp.where(keep, spread, 0.0))
    height = n * len(fields)
    block = jnp.concatenate([out[:height, r * sizes.lanes : (r + 1) * sizes.lanes] for r in range(n)], axis=0)
    copies = max(1, 8 // block.shape[0])
    block = jnp.concatenate([block] * copies, axis=0)
    for k in range(out_ref.shape[0] // block.shape[0]):
        out_ref[k * block.shape[0] : (k + 1) * block.shape[0], :] = block


def strip_kernel(sizes, at_ref, g_ref, s_ref, below_ref, above_ref, left_ref, right_ref):
    last = sizes.columns - 128
    for rows, sources in ((slice(0, sizes.rows), (g_ref, s_ref)),
                          (slice(sizes.rows, sizes.rows + HALO), (below_ref.at[0], below_ref.at[1])),
                          (slice(sizes.rows + HALO, sizes.rows + 2 * HALO), (above_ref.at[0], above_ref.at[1]))):
        g, s = sources
        first_g, first_s = g[:, :128], s[:, :128]
        last_g, last_s = g[:, last:], s[:, last:]
        lane = iota(first_g.shape, 1)
        left_ref[rows, :] = jnp.where(lane < HALO, first_g, pltpu.roll(first_s, HALO, 1))
        right_ref[rows, :] = jnp.where(lane >= 128 - HALO, last_g, pltpu.roll(last_s, 128 - HALO, 1))


def coefficients(sizes, level, gx, gy, sigma):
    d = 4.0 + sigma
    return d, jnp.where(inside_mask(sizes, level, gx, gy), DAMPING / d, 0.0)


def down_kernel(sizes, at_ref, g_ref, s_ref, below_ref, above_ref, left_ref, right_ref, rc0_ref, rc1_ref, pc_ref, pr_ref,
                g0_ref, d0_ref, w0_ref, v0_ref, c1_ref, d1_ref, w1_ref, v1_ref, d2_ref, w2_ref, out_ref, scratch):
    gx, gy = at_ref[0], at_ref[1]
    rows = sizes.ext_rows[0]
    lane = iota((rows, 128), 1)
    from_left, from_right = left_ref[...], right_ref[...]
    g = jnp.where(lane < HALO, from_right, from_left)
    sigma = jnp.where(lane < HALO, pltpu.roll(from_right, 128 - HALO, 1), pltpu.roll(from_left, HALO, 1))
    g = jnp.concatenate([jnp.concatenate([g_ref[...], below_ref[0], above_ref[0]], axis=0), g], axis=1)
    sigma = jnp.concatenate([jnp.concatenate([s_ref[...], below_ref[1], above_ref[1]], axis=0), sigma], axis=1)
    d, w = coefficients(sizes, 0, gx, gy, sigma)
    v = w * g
    v = sweep(v, g, w)
    r = g - d * v + around(v)
    g0_ref[...] = g
    d0_ref[...] = d
    w0_ref[...] = w
    v0_ref[...] = v
    half = rows // 2
    both = jnp.concatenate([pair_rows(scratch, r), pair_rows(scratch, sigma)], axis=0)
    both = f32dot_right(both, rc0_ref[...])
    g, sigma = both[:half], both[half:]
    d, w = coefficients(sizes, 1, gx, gy, sigma)
    v = w * g
    v = sweep(v, g, w)
    r = g - d * v + around(v)
    c1_ref[...] = g
    d1_ref[...] = d
    w1_ref[...] = w
    v1_ref[...] = v
    half = half // 2
    both = jnp.concatenate([pair_rows(scratch, r), pair_rows(scratch, sigma)], axis=0)
    both = f32dot_right(both, rc1_ref[...])
    g, sigma = both[:half], both[half:]
    d, w = coefficients(sizes, 2, gx, gy, sigma)
    d2_ref[...] = d
    w2_ref[...] = w
    own = sizes.rows // 4
    pack(sizes, 2, [g[:own], sigma[:own]], pc_ref, pr_ref, out_ref)


class Coarse:
    def __init__(self, sizes, first, d_refs, w_refs, g_refs, v_refs, t_refs):
        self.z = sizes
        self.first = first
        self.d, self.w, self.g, self.v, self.t = d_refs, w_refs, g_refs, v_refs, t_refs
        shape = (sizes.ny, sizes.lanes)
        lane, row = iota(shape, 1), iota(shape, 0)
        p, q = lane % sizes.p, lane // sizes.p
        self.first_p, self.last_p = p == 0, p == sizes.p - 1
        self.first_q, self.last_q = q == 0, q == sizes.q - 1
        self.first_row, self.last_row = row == 0, row == sizes.ny - 1

    def blocks(self, body):
        if self.z.nx <= 4:
            for gx in range(self.z.nx):
                body((gx + 1) * self.z.ny)
        else:
            def step(gx, carry):
                body(pl.multiple_of((gx + 1) * self.z.ny, 8))
                return carry

            lax.fori_loop(0, self.z.nx, step, 0)

    def at(self, ref, s, r, base):
        return ref[s, r, pl.ds(base, self.z.ny), :]

    def put(self, ref, s, r, base, value):
        ref[s, r, pl.ds(base, self.z.ny), :] = value

    def neighbours(self, ref, s, r, n, base):
        z = self.z
        if r < n - 1:
            right = self.at(ref, s, r + 1, base)
        else:
            x = self.at(ref, s, 0, base)
            moved = jnp.where(self.last_row, 0.0, pltpu.roll(x, z.ny - 1, 0))
            right = pltpu.roll(jnp.where(self.first_q, moved, x), z.lanes - z.p, 1)
        if r > 0:
            left = self.at(ref, s, r - 1, base)
        else:
            x = self.at(ref, s, n - 1, base)
            moved = jnp.where(self.first_row, 0.0, pltpu.roll(x, 1, 0))
            left = pltpu.roll(jnp.where(self.last_q, moved, x), z.p, 1)
        if s < n - 1:
            down = self.at(ref, s + 1, r, base)
        else:
            here = pltpu.roll(self.at(ref, 0, r, base), z.lanes - 1, 1)
            there = pltpu.roll(self.at(ref, 0, r, base + z.ny), z.p - 1, 1)
            down = jnp.where(self.last_p, there, here)
        if s > 0:
            up = self.at(ref, s - 1, r, base)
        else:
            here = pltpu.roll(self.at(ref, n - 1, r, base), 1, 1)
            there = pltpu.roll(self.at(ref, n - 1, r, base - z.ny), z.lanes - z.p + 1, 1)
            up = jnp.where(self.first_p, there, here)
        return (up + down) + (left + right)

    def each(self, level, body):
        n = 1 << (LEVELS - level)

        def block(base):
            for s in range(n):
                for r in range(n):
                    body(s, r, n, base)

        self.blocks(block)

    def first_sweep(self, level):
        l = level - self.first

        def body(s, r, n, base):
            self.put(self.v[l], s, r, base, self.at(self.w[l], s, r, base) * self.at(self.g[l], s, r, base))

        self.each(level, body)

    def sweep(self, level, source, target):
        l = level - self.first

        def body(s, r, n, base):
            v = self.at(source, s, r, base)
            total = self.at(self.g[l], s, r, base) + self.neighbours(source, s, r, n, base)
            self.put(target, s, r, base, (1.0 - DAMPING) * v + self.at(self.w[l], s, r, base) * total)

        self.each(level, body)

    def two_sweeps(self, level):
        l = level - self.first
        self.sweep(level, self.v[l], self.t[l])
        self.sweep(level, self.t[l], self.v[l])

    def start(self, level):
        l = level - self.first
        self.first_sweep(level)
        self.sweep(level, self.v[l], self.t[l])
        self.v[l], self.t[l] = self.t[l], self.v[l]

    def residual(self, level, s, r, n, base):
        l = level - self.first
        v = self.at(self.v[l], s, r, base)
        g = self.at(self.g[l], s, r, base)
        return (g - self.at(self.d[l], s, r, base) * v) + self.neighbours(self.v[l], s, r, n, base)

    def restrict(self, level):
        l = level - self.first
        n = 1 << (LEVELS - level)

        def block(base):
            for s in range(n // 2):
                for r in range(n // 2):
                    parts = [self.residual(level, 2 * s + a, 2 * r + b, n, base) for a in (0, 1) for b in (0, 1)]
                    self.put(self.g[l + 1], s, r, base, (parts[0] + parts[1]) + (parts[2] + parts[3]))

        self.blocks(block)

    def prolong(self, level):
        l = level - self.first

        def body(s, r, n, base):
            e = self.at(self.v[l + 1], s // 2, r // 2, base)
            self.put(self.v[l], s, r, base, self.at(self.v[l], s, r, base) + e)

        self.each(level, body)

    def total(self, of):
        z = self.z
        if z.nx <= 4:
            parts = [of((gx + 1) * z.ny) for gx in range(z.nx)]
            value = parts[0]
            for part in parts[1:]:
                value = value + part
        else:
            value = lax.fori_loop(
                0, z.nx, lambda gx, acc: acc + of(pl.multiple_of((gx + 1) * z.ny, 8)),
                jnp.zeros((z.ny, z.lanes), jnp.float32))
        return jnp.sum(jnp.sum(value, axis=0, keepdims=True), axis=1, keepdims=True)

    def unit(self):
        z = self.z
        top = LEVELS - self.first
        missing = 2.0 * (z.nx * z.p + z.ny * z.q) - 0.0
        cells = 4.0
        total = self.total(lambda base: self.at(self.d[top], 0, 0, base) - cells)
        return total + missing

    def coarse(self, fresh, unit):
        top = LEVELS - self.first
        v, t, g = self.v[top], self.t[top], self.g[top]
        if fresh:
            left = self.total(lambda base: self.at(g, 0, 0, base)) / unit

            def body(base):
                self.put(v, 0, 0, base, jnp.broadcast_to(left, (self.z.ny, self.z.lanes)))
        else:
            left = self.total(lambda base: self.residual(LEVELS, 0, 0, 1, base)) / unit

            def body(base):
                self.put(v, 0, 0, base, self.at(v, 0, 0, base) + left)

        self.blocks(body)
        for turn in range(COARSE_SWEEPS // 2):
            self.sweep(LEVELS, v, t)
            self.sweep(LEVELS, t, v)

    def vcycle(self, level, fresh, unit):
        if level == LEVELS:
            self.coarse(fresh, unit)
            return
        if fresh:
            self.start(level)
        else:
            self.two_sweeps(level)
        self.restrict(level)
        self.vcycle(level + 1, True, unit)
        self.prolong(level)
        self.two_sweeps(level)

    def fcycle(self, level, unit):
        if level == LEVELS:
            self.coarse(True, unit)
            return
        self.start(level)
        self.restrict(level)
        self.fcycle(level + 1, unit)
        self.vcycle(level + 1, False, unit)
        self.prolong(level)
        self.two_sweeps(level)

    def clear_ends(self):
        z = self.z
        zero = jnp.zeros((z.ny, z.lanes), jnp.float32)
        for refs in (self.v, self.t):
            for ref in refs:
                n = ref.shape[0]
                for s in range(n):
                    for r in range(n):
                        ref[s, r, : z.ny, :] = zero
                        ref[s, r, (z.nx + 1) * z.ny :, :] = zero

    def take(self, y_ref, target, offset, height):
        z = self.z
        n = target.shape[0]

        def block(base):
            for s in range(n):
                for r in range(n):
                    first = (base - z.ny) * n * height + r * height + offset + s
                    self.put(target, s, r, base, y_ref[pl.ds(first, z.ny, stride=n * height), :])

        self.blocks(block)

    def take_cores(self, even_ref, odd_ref, target, offset, height, add):
        z = self.z
        n = target.shape[0]
        half = z.ny // 2

        def block(base):
            for s in range(n):
                for r in range(n):
                    first = (base - z.ny) // 2 * n * height + r * height + offset + s
                    for core, ref in ((0, even_ref), (1, odd_ref)):
                        value = ref[pl.ds(first, half, stride=n * height), :]
                        target[s, r, pl.ds(base + core, half, stride=2), :] = value + add if add else value

        self.blocks(block)

    def spread(self, gx, gy, rows_ref, columns_ref, e_ref):
        z = self.z
        n = 1 << (LEVELS - self.first)
        row = (gx + 1) * z.ny + gy
        lane = iota((1, z.lanes), 1)
        low_half = lane // z.p < z.q // 2
        has_left, has_right = gy > 0, gy < z.ny - 1
        e_ref[...] = jnp.zeros(e_ref.shape, jnp.float32)
        ref = self.v[0]
        for dx in range(3):
            base = row + (dx - 1) * z.ny
            for s in range(n):
                for r in range(n):
                    own = ref[s, r, pl.ds(base, 1), :]
                    left = ref[s, r, pl.ds(jnp.where(has_left, base - 1, 0), 1), :]
                    right = ref[s, r, pl.ds(jnp.where(has_right, base + 1, 0), 1), :]
                    k = dx * n + s
                    e_ref[k : k + 1, r * z.lanes : (r + 1) * z.lanes] = own
                    e_ref[k : k + 1, (n + r) * z.lanes : (n + r + 1) * z.lanes] = jnp.where(low_half, right, left)
        spread = f32dot_left(rows_ref[...], e_ref[...])
        shape = spread.shape
        index = iota(shape, 0)
        above = self.first - 1
        own_r, halo = z.rows >> above, HALO >> above
        cell = jnp.where(index < own_r + halo, index, index - shape[0]) + 2 * z.rows
        keep = ((cell // (2 * n)) % z.p) == (iota(shape, 1) % z.p)
        return f32dot_right(jnp.where(keep, spread, 0.0), columns_ref[...])


def level_shape(sizes, level):
    n = 1 << (LEVELS - level)
    return (n, n, (sizes.nx + 2) * sizes.ny, sizes.lanes)


def middle_kernel(sizes, at_ref, y_ref, other_ref, c1_ref, d1_ref, w1_ref, v1_ref, w2l_ref, d2l_ref, sr_ref, sc_ref,
                  rc1_ref, pc_ref, pr_ref,
                  d3_ref, d4_ref, w3_ref, w4_ref, e1_ref, c2_ref, e2_ref, out_ref,
                  d2, w2, g2, g3, g4, v2, v3, v4, t2, t3, t4, e_ref, scratch):
    gx, gy = at_ref[0], at_ref[1]
    m = Coarse(sizes, 2, [d2, d3_ref, d4_ref], [w2, w3_ref, w4_ref], [g2, g3, g4], [v2, v3, v4], [t2, t3, t4])
    m.clear_ends()
    core = lax.rem(gy, 2)

    @pl.when(core == 0)
    def _():
        m.take_cores(y_ref, other_ref, g2, 0, 8, 0.0)
        m.take_cores(y_ref, other_ref, d2, 4, 8, 4.0)

    @pl.when(core == 1)
    def _():
        m.take_cores(other_ref, y_ref, g2, 0, 8, 0.0)
        m.take_cores(other_ref, y_ref, d2, 4, 8, 4.0)

    for l in range(2):
        n = 2 >> l

        def block(base):
            for s in range(n):
                for r in range(n):
                    parts = [m.at(m.d[l], 2 * s + a, 2 * r + b, base) for a in (0, 1) for b in (0, 1)]
                    m.put(m.d[l + 1], s, r, base, ((parts[0] + parts[1]) + (parts[2] + parts[3])) - 12.0)

        m.blocks(block)
    for l in range(3):
        def body(s, r, n, base):
            m.put(m.w[l], s, r, base, DAMPING / m.at(m.d[l], s, r, base))

        m.each(l + 2, body)
    unit = m.unit()
    m.fcycle(2, unit)
    m.vcycle(2, False, unit)
    g, d, w = c1_ref[...], d1_ref[...], w1_ref[...]
    v = v1_ref[...] + jnp.where(w > 0.0, m.spread(gx, gy, sr_ref, sc_ref, e_ref), 0.0)
    for turn in range(4):
        v = sweep(v, g, w)
    e1_ref[...] = v
    r = g - d * v + around(v)
    g = f32dot_right(pair_rows(scratch, r), rc1_ref[...])
    d, w = d2l_ref[...], w2l_ref[...]
    v = w * g
    v = sweep(v, g, w)
    r = g - d * v + around(v)
    c2_ref[...] = g
    e2_ref[...] = v
    pack(sizes, 3, [pair_rows(scratch, r[: sizes.rows // 4])], pc_ref, pr_ref, out_ref)


def up_kernel(sizes, at_ref, y_ref, d3_ref, d4_ref, w3_ref, w4_ref, c2_ref, w2_ref, e2_ref, c1_ref, w1_ref, e1_ref,
              g0_ref, d0_ref, w0_ref, v0_ref, sr_ref, sc_ref, pc1_ref, pc0_ref,
              solution_ref, residual_ref, g3, g4, v3, v4, t3, t4, e_ref, scratch):
    gx, gy = at_ref[0], at_ref[1]
    m = Coarse(sizes, 3, [d3_ref, d4_ref], [w3_ref, w4_ref], [g3, g4], [v3, v4], [t3, t4])
    m.clear_ends()
    m.take(y_ref, g3, 0, 2)
    m.vcycle(3, True, m.unit())
    g, w = c2_ref[...], w2_ref[...]
    v = e2_ref[...] + jnp.where(w > 0.0, m.spread(gx, gy, sr_ref, sc_ref, e_ref), 0.0)
    for turn in range(2):
        v = sweep(v, g, w)
    g, w = c1_ref[...], w1_ref[...]
    v = e1_ref[...] + double_rows(scratch, f32dot_right(v, pc1_ref[...]))
    for turn in range(2):
        v = sweep(v, g, w)
    g, d, w = g0_ref[...], d0_ref[...], w0_ref[...]
    v = v0_ref[...] + double_rows(scratch, f32dot_right(v, pc0_ref[...]))
    for turn in range(2):
        v = sweep(v, g, w)
    r = g - d * v + around(v)
    solution_ref[...] = v[: sizes.rows, : sizes.columns]
    residual_ref[...] = r[: sizes.rows, : sizes.columns]


def vmem(count):
    return [pl.BlockSpec(memory_space=pltpu.VMEM)] * count


def call(kernel, sizes, outs, scratch, *operands):
    shapes = [jax.ShapeDtypeStruct(shape, jnp.float32) for shape in outs]
    used = sum(4 * int(np.prod(shape)) for shape in list(outs) + list(scratch))
    used += sum(x.size * x.dtype.itemsize for x in operands)
    return pl.pallas_call(
        lambda *refs: kernel(sizes, *refs),
        name=kernel.__name__,
        out_shape=shapes,
        in_specs=[pl.BlockSpec(memory_space=pltpu.SMEM)] + vmem(len(operands) - 1),
        out_specs=vmem(len(outs)),
        scratch_shapes=[pltpu.VMEM(shape, jnp.float32) for shape in scratch],
        compiler_params=pltpu.CompilerParams(vmem_limit_bytes=used + used // 4 + (4 << 20)),
    )(*operands)


def ring(values, axis, step):
    count = lax.axis_size(axis)
    return lax.ppermute(values, axis, [(i, (i + step) % count) for i in range(count)])


def gather(copies):
    return lax.all_to_all(copies, ("gx", "gy"), 0, 0, tiled=True)


def gather_by_core(copies, nx, ny):
    index = np.arange(nx * ny)
    groups = [index[core::2].tolist() for core in range(2)]
    own = lax.all_to_all(copies, ("gx", "gy"), 0, 0, tiled=True, axis_index_groups=groups)
    return own, lax.ppermute(own, "gy", [(j, j ^ 1) for j in range(ny)])


def body(right_side, shift):
    nx, ny = lax.axis_size("gx"), lax.axis_size("gy")
    rows, columns = right_side.shape
    z = Sizes(rows, columns, nx, ny)
    at = jnp.stack([lax.axis_index("gx"), lax.axis_index("gy")]).astype(jnp.int32)
    below = ring(jnp.stack([right_side[:HALO], shift[:HALO]]), "gx", -1)
    above = ring(jnp.stack([right_side[rows - HALO :], shift[rows - HALO :]]), "gx", 1)
    ext = [(z.ext_rows[l], z.ext_columns[l]) for l in range(3)]
    strip = (z.ext_rows[0], 128)
    to_left, to_right = call(strip_kernel, z, [strip] * 2, [], at, right_side, shift, below, above)
    right = ring(to_left, "gy", -1)
    left = ring(to_right, "gy", 1)
    rc0, rc1 = z.restrict_columns(0), z.restrict_columns(1)
    tiles = (ext[0][1] // 128, ext[0][0], 128)
    g0, d0, w0, v0, c1, d1, w1, v1, d2, w2, packed = call(
        down_kernel, z, [ext[0]] * 4 + [ext[1]] * 4 + [ext[2]] * 2 + [(nx * ny // 2 * 32, z.lanes)], [tiles],
        at, right_side, shift, below, above, left, right, rc0, rc1, z.pack_columns(2, False), z.pack_rows(2, 2))
    y, other = gather_by_core(packed, nx, ny)
    slabs = [level_shape(z, level) for level in (2, 3, 4)]
    d3, d4, w3, w4, e1, c2, e2, packed = call(
        middle_kernel, z, slabs[1:] * 2 + [ext[1], ext[2], ext[2], (nx * ny * 4, z.lanes)],
        [slabs[0]] * 2 + slabs * 3 + [(16, 8 * z.lanes), tiles],
        at, y, other, c1, d1, w1, v1, w2, d2, z.spread_rows(2), z.spread_columns(2),
        rc1, z.pack_columns(3, True), z.pack_rows(3, 1))
    y = gather(packed)
    return call(
        up_kernel, z, [(rows, columns)] * 2, slabs[1:] * 3 + [(8, 4 * z.lanes), tiles],
        at, y, d3, d4, w3, w4, c2, w2, e2, c1, w1, e1, g0, d0, w0, v0,
        z.spread_rows(3), z.spread_columns(3), rc1.T, rc0.T)


def solution(mesh):
    specs = (P("gx", "gy"), P("gx", "gy"))

    def run(right_side, shift):
        out = body(right_side, shift)
        return out[0], out[1]

    return jax.shard_map(run, mesh=mesh, in_specs=specs, out_specs=specs, check_vma=False)
```

```python
import numpy as np
import jax
import jax.numpy as jnp
from jax import lax
from jax.experimental import pallas as pl
from jax.experimental.pallas import tpu as pltpu
from jax.sharding import PartitionSpec as P

LEVELS = 4
COARSE_SWEEPS = 6
DAMPING = 0.8
HALO = 48


def f32dot_right(values, onehot):
    high = values.astype(jnp.bfloat16)
    rest = values - high.astype(jnp.float32)
    middle = rest.astype(jnp.bfloat16)
    low = (rest - middle.astype(jnp.float32)).astype(jnp.bfloat16)
    rows = values.shape[0]
    stacked = jnp.concatenate([high, middle, low], axis=0)
    out = jnp.dot(stacked, onehot, preferred_element_type=jnp.float32)
    return (out[2 * rows :] + out[rows : 2 * rows]) + out[:rows]


def f32dot_left(onehot, values):
    high = values.astype(jnp.bfloat16)
    rest = values - high.astype(jnp.float32)
    middle = rest.astype(jnp.bfloat16)
    low = (rest - middle.astype(jnp.float32)).astype(jnp.bfloat16)
    total = jnp.dot(onehot, low, preferred_element_type=jnp.float32)
    total = total + jnp.dot(onehot, middle, preferred_element_type=jnp.float32)
    return total + jnp.dot(onehot, high, preferred_element_type=jnp.float32)


def around(v):
    rows, columns = v.shape
    up = pltpu.roll(v, 1, 0)
    down = pltpu.roll(v, rows - 1, 0)
    left = pltpu.roll(v, 1, 1)
    right = pltpu.roll(v, columns - 1, 1)
    return (up + down) + (left + right)


def sweep(v, g, w):
    return (1.0 - DAMPING) * v + w * (g + around(v))


class Sizes:
    def __init__(self, rows, columns, nx, ny):
        self.rows, self.columns, self.nx, self.ny = rows, columns, nx, ny
        self.p, self.q = rows // 16, columns // 16
        self.coarse_rows, self.coarse_columns = nx * self.p, ny * self.q
        assert self.p == 8 and 8 * self.q == 128, "block shape"

        def up(n):
            return -(-n // 128) * 128

        self.ext_rows = [(rows + 2 * HALO) >> l for l in range(3)]
        self.ext_columns = [up((columns + 2 * HALO) >> l) for l in range(3)]

    def column_at(self, level):
        own, halo, width = self.columns >> level, HALO >> level, self.ext_columns[level]
        lane = np.arange(width)
        inside = (lane < own + halo) | (lane >= width - halo)
        return np.where(lane < own + halo, lane, lane - width), inside

    def row_at(self, level):
        own, halo, height = self.rows >> level, HALO >> level, self.ext_rows[level]
        row = np.arange(height)
        return np.where(row < own + halo, row, row - height)

    def restrict_columns(self, level):
        fine, fine_in = self.column_at(level)
        coarse, coarse_in = self.column_at(level + 1)
        hit = (fine[:, None] // 2 == coarse[None, :]) & fine_in[:, None] & coarse_in[None, :]
        return hit.astype(jnp.bfloat16)

    def pack_pair(self):
        own = self.columns >> 2
        x = np.arange(2 * own)
        target = (x // own) * own + (x % own % 4) * self.q + x % own // 4
        return (target[:, None] == np.arange(2 * own)[None, :]).astype(jnp.bfloat16)

    def pack_single(self):
        x = np.arange(self.ext_columns[2])[:, None]
        lane = np.arange(128)[None, :]
        hit = (x // 2 == 2 * (lane % self.q) + (lane // self.q) % 2) & (x < self.columns >> 2)
        return hit.astype(jnp.bfloat16)

    def spread_columns(self, level):
        n = 1 << (LEVELS - level)
        column, inside = self.column_at(level - 1)
        m = column // 2
        r = np.arange(n)[:, None, None]
        lane = np.arange(128)[None, :, None]
        hit = (m % n == r) & (m // n + self.q == lane) & inside
        return hit.reshape(n * 128, -1).astype(jnp.bfloat16)


def iota(shape, axis):
    return lax.broadcasted_iota(jnp.int32, shape, axis)


def inside_mask(sizes, level, gx, gy):
    shape = (sizes.ext_rows[level], sizes.ext_columns[level])
    own_r, own_c, halo = sizes.rows >> level, sizes.columns >> level, HALO >> level
    row, column = iota(shape, 0), iota(shape, 1)
    last_row = jnp.where(gx < sizes.nx - 1, own_r + halo, own_r)
    first_row = jnp.where(gx > 0, own_r + halo, shape[0])
    last_column = jnp.where(gy < sizes.ny - 1, own_c + halo, own_c)
    first_column = jnp.where(gy > 0, shape[1] - halo, shape[1])
    return ((row < last_row) | (row >= first_row)) & ((column < last_column) | (column >= first_column))


def pair_rows(scratch, values):
    rows, columns = values.shape
    outs = []
    for t in range(columns // 128):
        scratch[t, :rows, :] = values[:, t * 128 : (t + 1) * 128]
    for t in range(columns // 128):
        outs.append(scratch[t, pl.ds(0, rows // 2, stride=2), :] + scratch[t, pl.ds(1, rows // 2, stride=2), :])
    return jnp.concatenate(outs, axis=1)


def double_rows(scratch, values):
    rows, columns = values.shape
    for t in range(columns // 128):
        part = values[:, t * 128 : (t + 1) * 128]
        scratch[t, pl.ds(0, rows, stride=2), :] = part
        scratch[t, pl.ds(1, rows, stride=2), :] = part
    return jnp.concatenate([scratch[t, : 2 * rows, :] for t in range(columns // 128)], axis=1)


def repeat(block, out_ref):
    height = block.shape[0]
    for k in range(out_ref.shape[0] // height):
        out_ref[k * height : (k + 1) * height, :] = block


def pack_two(sizes, gy, first, second, scratch, columns_ref, out_ref):
    own = sizes.columns >> 2
    both = jnp.where(iota(first.shape, 1) < own, first, pltpu.roll(second, own, 1))
    rows = both.shape[0]
    scratch[0, :rows, :] = f32dot_right(both, columns_ref[...])
    block = jnp.concatenate([scratch[0, pl.ds(s, sizes.p, stride=4), :] for s in range(4)], axis=0)
    repeat(pltpu.roll(block, lax.rem(gy, 8) * sizes.q, 1), out_ref)


def pack_one(sizes, gy, values, scratch, columns_ref, out_ref):
    rows = values.shape[0]
    scratch[0, :rows, :] = f32dot_right(values, columns_ref[...])
    part = iota((4, 128), 1) // (2 * sizes.q)
    block = scratch[0, pl.ds(0, 4, stride=2), :]
    for k in range(1, 4):
        block = jnp.where(part == k, scratch[0, pl.ds(8 * (k // 2) + k % 2, 4, stride=2), :], block)
    block = jnp.concatenate([block, block], axis=0)
    repeat(pltpu.roll(block, lax.rem(gy, 8) * sizes.q, 1), out_ref)


def strip_kernel(sizes, at_ref, g_ref, s_ref, below_ref, above_ref, left_ref, right_ref):
    last = sizes.columns - 128
    for rows, sources in ((slice(0, sizes.rows), (g_ref, s_ref)),
                          (slice(sizes.rows, sizes.rows + HALO), (below_ref.at[0], below_ref.at[1])),
                          (slice(sizes.rows + HALO, sizes.rows + 2 * HALO), (above_ref.at[0], above_ref.at[1]))):
        g, s = sources
        first_g, first_s = g[:, :128], s[:, :128]
        last_g, last_s = g[:, last:], s[:, last:]
        lane = iota(first_g.shape, 1)
        left_ref[rows, :] = jnp.where(lane < HALO, first_g, pltpu.roll(first_s, HALO, 1))
        right_ref[rows, :] = jnp.where(lane >= 128 - HALO, last_g, pltpu.roll(last_s, 128 - HALO, 1))


def coefficients(sizes, level, gx, gy, sigma):
    d = 4.0 + sigma
    return d, jnp.where(inside_mask(sizes, level, gx, gy), DAMPING / d, 0.0)


def down_kernel(sizes, at_ref, g_ref, s_ref, below_ref, above_ref, left_ref, right_ref, rc0_ref, rc1_ref, pc_ref,
                g0_ref, d0_ref, w0_ref, v0_ref, c1_ref, d1_ref, w1_ref, v1_ref, d2_ref, w2_ref, out_ref, scratch):
    gx, gy = at_ref[0], at_ref[1]
    rows = sizes.ext_rows[0]
    lane = iota((rows, 128), 1)
    from_left, from_right = left_ref[...], right_ref[...]
    g = jnp.where(lane < HALO, from_right, from_left)
    sigma = jnp.where(lane < HALO, pltpu.roll(from_right, 128 - HALO, 1), pltpu.roll(from_left, HALO, 1))
    g = jnp.concatenate([jnp.concatenate([g_ref[...], below_ref[0], above_ref[0]], axis=0), g], axis=1)
    sigma = jnp.concatenate([jnp.concatenate([s_ref[...], below_ref[1], above_ref[1]], axis=0), sigma], axis=1)
    d, w = coefficients(sizes, 0, gx, gy, sigma)
    v = w * g
    v = sweep(v, g, w)
    r = g - d * v + around(v)
    g0_ref[...] = g
    d0_ref[...] = d
    w0_ref[...] = w
    v0_ref[...] = v
    half = rows // 2
    both = jnp.concatenate([pair_rows(scratch, r), pair_rows(scratch, sigma)], axis=0)
    both = f32dot_right(both, rc0_ref[...])
    g, sigma = both[:half], both[half:]
    d, w = coefficients(sizes, 1, gx, gy, sigma)
    v = w * g
    v = sweep(v, g, w)
    r = g - d * v + around(v)
    c1_ref[...] = g
    d1_ref[...] = d
    w1_ref[...] = w
    v1_ref[...] = v
    half = half // 2
    both = jnp.concatenate([pair_rows(scratch, r), pair_rows(scratch, sigma)], axis=0)
    both = f32dot_right(both, rc1_ref[...])
    g, sigma = both[:half], both[half:]
    d, w = coefficients(sizes, 2, gx, gy, sigma)
    d2_ref[...] = d
    w2_ref[...] = w
    own = sizes.rows // 4
    pack_two(sizes, gy, g[:own], sigma[:own], scratch, pc_ref, out_ref)


class Coarse:
    def __init__(self, sizes, first, d_refs, w_refs, g_refs, v_refs, t_refs):
        self.z = sizes
        self.first = first
        self.d, self.w, self.g, self.v, self.t = d_refs, w_refs, g_refs, v_refs, t_refs
        lane = iota((sizes.p, sizes.coarse_columns), 1)
        self.first_lane, self.last_lane = lane == 0, lane == sizes.coarse_columns - 1

    def blocks(self, body):
        p = self.z.p
        if self.z.nx <= 4:
            for gx in range(self.z.nx):
                body((gx + 1) * p)
        else:
            def step(gx, carry):
                body(pl.multiple_of((gx + 1) * p, 8))
                return carry

            lax.fori_loop(0, self.z.nx, step, 0)

    def at(self, ref, s, r, base):
        return ref[s, r, pl.ds(base, self.z.p), :]

    def put(self, ref, s, r, base, value):
        ref[s, r, pl.ds(base, self.z.p), :] = value

    def beside(self, ref, s, r, base, step):
        p = self.z.p
        if isinstance(base, int):
            return ref[s, r, pl.ds(base + step, p), :]
        return ref[s, r, pl.ds(base - p, 3 * p), :][p + step : 2 * p + step]

    def neighbours(self, ref, s, r, n, base):
        columns = self.z.coarse_columns
        if r < n - 1:
            right = self.at(ref, s, r + 1, base)
        else:
            right = jnp.where(self.last_lane, 0.0, pltpu.roll(self.at(ref, s, 0, base), columns - 1, 1))
        if r > 0:
            left = self.at(ref, s, r - 1, base)
        else:
            left = jnp.where(self.first_lane, 0.0, pltpu.roll(self.at(ref, s, n - 1, base), 1, 1))
        down = self.at(ref, s + 1, r, base) if s < n - 1 else self.beside(ref, 0, r, base, 1)
        up = self.at(ref, s - 1, r, base) if s > 0 else self.beside(ref, n - 1, r, base, -1)
        return (up + down) + (left + right)

    def each(self, level, body):
        n = 1 << (LEVELS - level)

        def block(base):
            for s in range(n):
                for r in range(n):
                    body(s, r, n, base)

        self.blocks(block)

    def first_sweep(self, level):
        l = level - self.first

        def body(s, r, n, base):
            self.put(self.v[l], s, r, base, self.at(self.w[l], s, r, base) * self.at(self.g[l], s, r, base))

        self.each(level, body)

    def sweep(self, level, source, target):
        l = level - self.first

        def body(s, r, n, base):
            v = self.at(source, s, r, base)
            total = self.at(self.g[l], s, r, base) + self.neighbours(source, s, r, n, base)
            self.put(target, s, r, base, (1.0 - DAMPING) * v + self.at(self.w[l], s, r, base) * total)

        self.each(level, body)

    def two_sweeps(self, level):
        l = level - self.first
        self.sweep(level, self.v[l], self.t[l])
        self.sweep(level, self.t[l], self.v[l])

    def start(self, level):
        l = level - self.first
        self.first_sweep(level)
        self.sweep(level, self.v[l], self.t[l])
        self.v[l], self.t[l] = self.t[l], self.v[l]

    def residual(self, level, s, r, n, base):
        l = level - self.first
        v = self.at(self.v[l], s, r, base)
        g = self.at(self.g[l], s, r, base)
        return (g - self.at(self.d[l], s, r, base) * v) + self.neighbours(self.v[l], s, r, n, base)

    def restrict(self, level):
        l = level - self.first
        n = 1 << (LEVELS - level)

        def block(base):
            for s in range(n // 2):
                for r in range(n // 2):
                    parts = [self.residual(level, 2 * s + a, 2 * r + b, n, base) for a in (0, 1) for b in (0, 1)]
                    self.put(self.g[l + 1], s, r, base, (parts[0] + parts[1]) + (parts[2] + parts[3]))

        self.blocks(block)

    def prolong(self, level):
        l = level - self.first

        def body(s, r, n, base):
            e = self.at(self.v[l + 1], s // 2, r // 2, base)
            self.put(self.v[l], s, r, base, self.at(self.v[l], s, r, base) + e)

        self.each(level, body)

    def inner(self, ref):
        p = self.z.p
        return ref[0, 0, p : p + self.z.coarse_rows, :]

    def shifted(self, x, k):
        if k == 0:
            return x
        columns = self.z.coarse_columns
        lane = iota(x.shape, 1)
        keep = lane < columns - k if k > 0 else lane >= -k
        return jnp.where(keep, pltpu.roll(x, -k % columns, 1), 0.0)

    def unit(self):
        z = self.z
        top = LEVELS - self.first
        d, w = self.inner(self.d[top]), self.inner(self.w[top])
        missing = 2.0 * (z.coarse_rows + z.coarse_columns)
        return 1.0 / (jnp.sum(d - 4.0, keepdims=True) + missing), {k: self.shifted(w, k) for k in range(-2, 3)}

    def coarse(self, fresh, unit):
        top = LEVELS - self.first
        one, w = unit
        g = self.inner(self.g[top])
        shape = g.shape
        row, lane = iota(shape, 0), iota(shape, 1)
        first_row, last_row = row == 0, row == shape[0] - 1
        sources = {k: self.shifted(g, k) for k in range(-2, 3)}

        def vertical(x):
            return jnp.where(first_row, 0.0, pltpu.roll(x, 1, 0)) + jnp.where(last_row, 0.0, pltpu.roll(x, shape[0] - 1, 0))

        def three(v):
            for reach in (2, 1, 0):
                v = {
                    k: (1.0 - DAMPING) * v[k] + w[k] * ((sources[k] + vertical(v[k])) + (v[k - 1] + v[k + 1]))
                    for k in range(-reach, reach + 1)
                }
            return v[0]

        if fresh:
            left = jnp.sum(g, keepdims=True) * one
            v = {k: 0.0 for k in range(-3, 4)}
        else:
            v = self.inner(self.v[top])
            v = {k: self.shifted(v, k) for k in range(-3, 4)}
            around_v = vertical(v[0]) + (v[-1] + v[1])
            left = jnp.sum((g - self.inner(self.d[top]) * v[0]) + around_v, keepdims=True) * one
        left = jnp.broadcast_to(left, shape)
        for k in range(-3, 4):
            v[k] = v[k] + jnp.where((lane < shape[1] - k) & (lane >= -k), left, 0.0)
        for turn in range(COARSE_SWEEPS // 3):
            if turn:
                v = {k: self.shifted(v, k) for k in range(-3, 4)}
            v = three(v)
        p = self.z.p
        self.v[top][0, 0, p : p + shape[0], :] = v

    def vcycle(self, level, fresh, unit):
        if level == LEVELS:
            self.coarse(fresh, unit)
            return
        if fresh:
            self.start(level)
        else:
            self.two_sweeps(level)
        self.restrict(level)
        self.vcycle(level + 1, True, unit)
        self.prolong(level)
        self.two_sweeps(level)

    def fcycle(self, level, unit):
        if level == LEVELS:
            self.coarse(True, unit)
            return
        self.start(level)
        self.restrict(level)
        self.fcycle(level + 1, unit)
        self.vcycle(level + 1, False, unit)
        self.prolong(level)
        self.two_sweeps(level)

    def clear_ends(self):
        z = self.z
        zero = jnp.zeros((z.p, z.coarse_columns), jnp.float32)
        for refs in (self.v, self.t):
            for ref in refs:
                n = ref.shape[0]
                for s in range(n):
                    for r in range(n):
                        ref[s, r, : z.p, :] = zero
                        ref[s, r, z.p + z.coarse_rows :, :] = zero

    def turned(self, blocks, k):
        q = self.z.q
        part = iota(blocks[0].shape, 1) // q
        out = blocks[-k % 8]
        for x in range(1, 8):
            out = jnp.where(part == x, blocks[(x - k) % 8], out)
        return pltpu.roll(out, -k * q % 128, 1) if k else out

    def take_two(self, even_ref, odd_ref, targets):
        z = self.z
        for gx in range(z.nx):
            for group in range(z.ny // 8):
                lanes = slice(group * 128, (group + 1) * 128)
                for s in range(4):
                    blocks = []
                    for g in range(8):
                        first = (gx * (z.ny // 2) + group * 4 + g // 2) * 4 * z.p + s * z.p
                        blocks.append((even_ref, odd_ref)[g % 2][first : first + z.p, :])
                    for k in range(8):
                        target, add = targets[k // 4]
                        value = self.turned(blocks, k)
                        target[s, k % 4, (gx + 1) * z.p : (gx + 2) * z.p, lanes] = value + add if add else value

    def take_one(self, y_ref, target):
        z = self.z
        low = iota((8, 128), 0) < 4
        for gx in range(z.nx):
            for group in range(z.ny // 8):
                upper, lower = [], []
                for g in range(0, 8, 2):
                    first = (gx * z.ny + group * 8 + g) * 4
                    pair = y_ref[first : first + 8, :]
                    swapped = pltpu.roll(pair, 4, 0)
                    upper += [pair, swapped]
                    lower += [swapped, pair]
                for k in range(4):
                    value = jnp.where(low, self.turned(upper, k), self.turned(lower, k + 4))
                    target[k // 2, k % 2, (gx + 1) * z.p : (gx + 2) * z.p, group * 128 : (group + 1) * 128] = value

    def spread(self, gx, gy, columns_ref, scratch):
        z = self.z
        n = 1 << (LEVELS - self.first)
        above = self.first - 1
        columns = z.coarse_columns
        turn = lax.rem(columns + z.q - gy * z.q, columns)
        start = pl.multiple_of(gx * z.p, 8)
        parts = []
        for s in range(n):
            line = [pltpu.roll(self.v[0][s, r, pl.ds(start, 3 * z.p), :], turn, 1)[:, :128] for r in range(n)]
            parts.append(jnp.concatenate(line, axis=1))
        wide = f32dot_right(jnp.concatenate(parts, axis=0), columns_ref[...])
        own, halo = z.rows >> above, HALO >> above
        inner, outer = (own + halo) // (2 * n), halo // (2 * n)
        tiles = wide.shape[1] // 128
        for t in range(tiles):
            for s in range(n):
                part = wide[s * 3 * z.p : (s + 1) * 3 * z.p, t * 128 : (t + 1) * 128]
                for a in range(2):
                    scratch[t, pl.ds(2 * s + a, inner, stride=2 * n), :] = part[z.p : z.p + inner]
                    scratch[t, pl.ds(own + halo + 2 * s + a, outer, stride=2 * n), :] = part[z.p - outer : z.p]
        return jnp.concatenate([scratch[t, : own + 2 * halo, :] for t in range(tiles)], axis=1)


def level_shape(sizes, level):
    n = 1 << (LEVELS - level)
    return (n, n, sizes.coarse_rows + 2 * sizes.p, sizes.coarse_columns)


def middle_kernel(sizes, at_ref, y_ref, other_ref, c1_ref, d1_ref, w1_ref, v1_ref, w2l_ref, d2l_ref, sc_ref,
                  rc1_ref, pc_ref,
                  d3_ref, d4_ref, w3_ref, w4_ref, e1_ref, c2_ref, e2_ref, out_ref,
                  d2, w2, g2, g3, g4, v2, v3, v4, t2, t3, t4, scratch):
    gx, gy = at_ref[0], at_ref[1]
    m = Coarse(sizes, 2, [d2, d3_ref, d4_ref], [w2, w3_ref, w4_ref], [g2, g3, g4], [v2, v3, v4], [t2, t3, t4])
    m.clear_ends()
    core = lax.rem(gy, 2)

    @pl.when(core == 0)
    def _():
        m.take_two(y_ref, other_ref, ((g2, 0.0), (d2, 4.0)))

    @pl.when(core == 1)
    def _():
        m.take_two(other_ref, y_ref, ((g2, 0.0), (d2, 4.0)))

    for l in range(2):
        n = 2 >> l

        def block(base):
            for s in range(n):
                for r in range(n):
                    parts = [m.at(m.d[l], 2 * s + a, 2 * r + b, base) for a in (0, 1) for b in (0, 1)]
                    m.put(m.d[l + 1], s, r, base, ((parts[0] + parts[1]) + (parts[2] + parts[3])) - 12.0)

        m.blocks(block)
    for l in range(3):
        def body(s, r, n, base):
            m.put(m.w[l], s, r, base, DAMPING / m.at(m.d[l], s, r, base))

        m.each(l + 2, body)
    unit = m.unit()
    m.fcycle(2, unit)
    m.vcycle(2, False, unit)
    g, d, w = c1_ref[...], d1_ref[...], w1_ref[...]
    v = v1_ref[...] + jnp.where(w > 0.0, m.spread(gx, gy, sc_ref, scratch), 0.0)
    for turn in range(4):
        v = sweep(v, g, w)
    e1_ref[...] = v
    r = g - d * v + around(v)
    g = f32dot_right(pair_rows(scratch, r), rc1_ref[...])
    d, w = d2l_ref[...], w2l_ref[...]
    v = w * g
    v = sweep(v, g, w)
    r = g - d * v + around(v)
    c2_ref[...] = g
    e2_ref[...] = v
    pack_one(sizes, gy, pair_rows(scratch, r[: sizes.rows // 4]), scratch, pc_ref, out_ref)


def up_kernel(sizes, at_ref, y_ref, d3_ref, d4_ref, w3_ref, w4_ref, c2_ref, w2_ref, e2_ref, c1_ref, w1_ref, e1_ref,
              g0_ref, d0_ref, w0_ref, v0_ref, sc_ref, pc1_ref, pc0_ref,
              solution_ref, residual_ref, g3, g4, v3, v4, t3, t4, scratch):
    gx, gy = at_ref[0], at_ref[1]
    m = Coarse(sizes, 3, [d3_ref, d4_ref], [w3_ref, w4_ref], [g3, g4], [v3, v4], [t3, t4])
    m.clear_ends()
    m.take_one(y_ref, g3)
    m.vcycle(3, True, m.unit())
    g, w = c2_ref[...], w2_ref[...]
    v = e2_ref[...] + jnp.where(w > 0.0, m.spread(gx, gy, sc_ref, scratch), 0.0)
    for turn in range(2):
        v = sweep(v, g, w)
    g, w = c1_ref[...], w1_ref[...]
    v = e1_ref[...] + double_rows(scratch, f32dot_right(v, pc1_ref[...]))
    for turn in range(2):
        v = sweep(v, g, w)
    g, d, w = g0_ref[...], d0_ref[...], w0_ref[...]
    v = v0_ref[...] + double_rows(scratch, f32dot_right(v, pc0_ref[...]))
    for turn in range(2):
        v = sweep(v, g, w)
    r = g - d * v + around(v)
    solution_ref[...] = v[: sizes.rows, : sizes.columns]
    residual_ref[...] = r[: sizes.rows, : sizes.columns]


def vmem(count):
    return [pl.BlockSpec(memory_space=pltpu.VMEM)] * count


def call(kernel, sizes, outs, scratch, *operands):
    shapes = [jax.ShapeDtypeStruct(shape, jnp.float32) for shape in outs]
    used = sum(4 * int(np.prod(shape)) for shape in list(outs) + list(scratch))
    used += sum(x.size * x.dtype.itemsize for x in operands)
    return pl.pallas_call(
        lambda *refs: kernel(sizes, *refs),
        name=kernel.__name__,
        out_shape=shapes,
        in_specs=[pl.BlockSpec(memory_space=pltpu.SMEM)] + vmem(len(operands) - 1),
        out_specs=vmem(len(outs)),
        scratch_shapes=[pltpu.VMEM(shape, jnp.float32) for shape in scratch],
        compiler_params=pltpu.CompilerParams(vmem_limit_bytes=used + used // 4 + (4 << 20)),
    )(*operands)


def ring(values, axis, step):
    count = lax.axis_size(axis)
    return lax.ppermute(values, axis, [(i, (i + step) % count) for i in range(count)])


def gather(copies):
    return lax.all_to_all(copies, ("gx", "gy"), 0, 0, tiled=True)


def gather_by_core(copies, nx, ny):
    index = np.arange(nx * ny)
    groups = [index[core::2].tolist() for core in range(2)]
    own = lax.all_to_all(copies, ("gx", "gy"), 0, 0, tiled=True, axis_index_groups=groups)
    return own, lax.ppermute(own, "gy", [(j, j ^ 1) for j in range(ny)])


def body(right_side, shift):
    nx, ny = lax.axis_size("gx"), lax.axis_size("gy")
    rows, columns = right_side.shape
    z = Sizes(rows, columns, nx, ny)
    at = jnp.stack([lax.axis_index("gx"), lax.axis_index("gy")]).astype(jnp.int32)
    below = ring(jnp.stack([right_side[:HALO], shift[:HALO]]), "gx", -1)
    above = ring(jnp.stack([right_side[rows - HALO :], shift[rows - HALO :]]), "gx", 1)
    ext = [(z.ext_rows[l], z.ext_columns[l]) for l in range(3)]
    strip = (z.ext_rows[0], 128)
    to_left, to_right = call(strip_kernel, z, [strip] * 2, [], at, right_side, shift, below, above)
    right = ring(to_left, "gy", -1)
    left = ring(to_right, "gy", 1)
    rc0, rc1 = z.restrict_columns(0), z.restrict_columns(1)
    tiles = (ext[0][1] // 128, ext[0][0], 128)
    g0, d0, w0, v0, c1, d1, w1, v1, d2, w2, packed = call(
        down_kernel, z, [ext[0]] * 4 + [ext[1]] * 4 + [ext[2]] * 2 + [(nx * ny // 2 * 4 * z.p, 128)], [tiles],
        at, right_side, shift, below, above, left, right, rc0, rc1, z.pack_pair())
    y, other = gather_by_core(packed, nx, ny)
    slabs = [level_shape(z, level) for level in (2, 3, 4)]
    d3, d4, w3, w4, e1, c2, e2, packed = call(
        middle_kernel, z, slabs[1:] * 2 + [ext[1], ext[2], ext[2], (nx * ny * 4, 128)],
        [slabs[0]] * 2 + slabs * 3 + [tiles],
        at, y, other, c1, d1, w1, v1, w2, d2, z.spread_columns(2),
        rc1, z.pack_single())
    y = gather(packed)
    return call(
        up_kernel, z, [(rows, columns)] * 2, slabs[1:] * 3 + [tiles],
        at, y, d3, d4, w3, w4, c2, w2, e2, c1, w1, e1, g0, d0, w0, v0,
        z.spread_columns(3), rc1.T, rc0.T)


def solution(mesh):
    specs = (P("gx", "gy"), P("gx", "gy"))

    def run(right_side, shift):
        out = body(right_side, shift)
        return out[0], out[1]

    return jax.shard_map(run, mesh=mesh, in_specs=specs, out_specs=specs, check_vma=False)
```

```python
import numpy as np
import jax
import jax.numpy as jnp
from jax import lax
from jax.experimental import pallas as pl
from jax.experimental.pallas import tpu as pltpu
from jax.sharding import PartitionSpec as P

LEVELS = 4
COARSE_SWEEPS = 6
DAMPING = 0.8
HALOS = (40, 16, 8)
HALO = HALOS[0]
NEAR = 8


def f32dot_right(values, onehot):
    high = values.astype(jnp.bfloat16)
    rest = values - high.astype(jnp.float32)
    middle = rest.astype(jnp.bfloat16)
    low = (rest - middle.astype(jnp.float32)).astype(jnp.bfloat16)
    rows = values.shape[0]
    stacked = jnp.concatenate([high, middle, low], axis=0)
    out = jnp.dot(stacked, onehot, preferred_element_type=jnp.float32)
    return (out[2 * rows :] + out[rows : 2 * rows]) + out[:rows]


def around(v):
    rows, columns = v.shape
    up = pltpu.roll(v, 1, 0)
    down = pltpu.roll(v, rows - 1, 0)
    left = pltpu.roll(v, 1, 1)
    right = pltpu.roll(v, columns - 1, 1)
    return (up + down) + (left + right)


def sweep(v, g, w):
    return (1.0 - DAMPING) * v + w * (g + around(v))


class Sizes:
    def __init__(self, rows, columns, nx, ny):
        self.rows, self.columns, self.nx, self.ny = rows, columns, nx, ny
        self.p, self.q = rows // 16, columns // 16
        self.coarse_rows, self.coarse_columns = nx * self.p, ny * self.q
        assert self.p == 8 and 8 * self.q == 128, "block shape"

        def up(n):
            return -(-n // 128) * 128

        self.ext_rows = [(rows >> l) + 2 * HALOS[l] for l in range(3)]
        self.ext_columns = [up((columns >> l) + 2 * HALOS[l]) for l in range(3)]

    def column_at(self, level):
        own, halo, width = self.columns >> level, HALOS[level], self.ext_columns[level]
        lane = np.arange(width)
        inside = (lane < own + halo) | (lane >= width - halo)
        return np.where(lane < own + halo, lane, lane - width), inside

    def restrict_columns(self, level):
        fine, fine_in = self.column_at(level)
        coarse, coarse_in = self.column_at(level + 1)
        hit = (fine[:, None] // 2 == coarse[None, :]) & fine_in[:, None] & coarse_in[None, :]
        return hit.astype(jnp.bfloat16)

    def pack_pair(self):
        own = self.columns >> 2
        x = np.arange(2 * own)
        target = (x // own) * own + (x % own % 4) * self.q + x % own // 4
        return (target[:, None] == np.arange(2 * own)[None, :]).astype(jnp.bfloat16)

    def pack_single(self):
        x = np.arange(self.ext_columns[2])[:, None]
        lane = np.arange(128)[None, :]
        hit = (x // 2 == 2 * (lane % self.q) + (lane // self.q) % 2) & (x < self.columns >> 2)
        return hit.astype(jnp.bfloat16)

    def spread_columns(self, level):
        n = 1 << (LEVELS - level)
        column, inside = self.column_at(level - 1)
        m = column // 2
        r = np.arange(n)[:, None, None]
        lane = np.arange(128)[None, :, None]
        hit = (m % n == r) & (m // n + self.q == lane) & inside
        return hit.reshape(n * 128, -1).astype(jnp.bfloat16)


def iota(shape, axis):
    return lax.broadcasted_iota(jnp.int32, shape, axis)


def inside_mask(sizes, level, gx, gy):
    shape = (sizes.ext_rows[level], sizes.ext_columns[level])
    own_r, own_c, halo = sizes.rows >> level, sizes.columns >> level, HALOS[level]
    row, column = iota(shape, 0), iota(shape, 1)
    last_row = jnp.where(gx < sizes.nx - 1, own_r + halo, own_r)
    first_row = jnp.where(gx > 0, own_r + halo, shape[0])
    last_column = jnp.where(gy < sizes.ny - 1, own_c + halo, own_c)
    first_column = jnp.where(gy > 0, shape[1] - halo, shape[1])
    return ((row < last_row) | (row >= first_row)) & ((column < last_column) | (column >= first_column))


def pair_rows(scratch, values):
    rows, columns = values.shape
    outs = []
    for t in range(columns // 128):
        scratch[t, :rows, :] = values[:, t * 128 : (t + 1) * 128]
    for t in range(columns // 128):
        outs.append(scratch[t, pl.ds(0, rows // 2, stride=2), :] + scratch[t, pl.ds(1, rows // 2, stride=2), :])
    return jnp.concatenate(outs, axis=1)


def double_rows(scratch, values):
    rows, columns = values.shape
    for t in range(columns // 128):
        part = values[:, t * 128 : (t + 1) * 128]
        scratch[t, pl.ds(0, rows, stride=2), :] = part
        scratch[t, pl.ds(1, rows, stride=2), :] = part
    return jnp.concatenate([scratch[t, : 2 * rows, :] for t in range(columns // 128)], axis=1)


def repeat(block, out_ref):
    height = block.shape[0]
    for k in range(out_ref.shape[0] // height):
        out_ref[k * height : (k + 1) * height, :] = block


def pack_two(sizes, gy, first, second, scratch, columns_ref, out_ref):
    own = sizes.columns >> 2
    both = jnp.where(iota(first.shape, 1) < own, first, pltpu.roll(second, own, 1))
    rows = both.shape[0]
    scratch[0, :rows, :] = f32dot_right(both, columns_ref[...])
    block = jnp.concatenate([scratch[0, pl.ds(s, sizes.p, stride=4), :] for s in range(4)], axis=0)
    repeat(pltpu.roll(block, lax.rem(gy, 8) * sizes.q, 1), out_ref)


def pack_one(sizes, gy, values, scratch, columns_ref, out_ref):
    rows = values.shape[0]
    scratch[0, :rows, :] = f32dot_right(values, columns_ref[...])
    part = iota((4, 128), 1) // (2 * sizes.q)
    block = scratch[0, pl.ds(0, 4, stride=2), :]
    for k in range(1, 4):
        block = jnp.where(part == k, scratch[0, pl.ds(8 * (k // 2) + k % 2, 4, stride=2), :], block)
    block = jnp.concatenate([block, block], axis=0)
    repeat(pltpu.roll(block, lax.rem(gy, 8) * sizes.q, 1), out_ref)


def near(values, own):
    return jnp.concatenate([values[: own + NEAR], values[values.shape[0] - NEAR :]], axis=0)


def sides(at, first_ref, second_ref):
    even = lax.rem(at, 2) == 0
    first, second = first_ref[...], second_ref[...]
    return jnp.where(even, first, second), jnp.where(even, second, first)


def strip_kernel(sizes, at_ref, g_ref, s_ref, rows_a_ref, rows_b_ref, first_ref, second_ref):
    last = sizes.columns - 128
    even = lax.rem(at_ref[1], 2) == 0
    below, above = sides(at_ref[0], rows_a_ref, rows_b_ref)
    start = 0
    for g, s in ((g_ref[...], s_ref[...]), (below[0], below[1]), (above[0], above[1])):
        rows = slice(start, start + g.shape[0])
        start += g.shape[0]
        lane = iota((g.shape[0], 128), 1)
        left = jnp.where(lane < HALO, g[:, :128], pltpu.roll(s[:, :128], HALO, 1))
        right = jnp.where(lane >= 128 - HALO, g[:, last:], pltpu.roll(s[:, last:], 128 - HALO, 1))
        first_ref[rows, :] = jnp.where(even, right, left)
        second_ref[rows, :] = jnp.where(even, left, right)


def coefficients(sizes, level, gx, gy, sigma):
    d = 4.0 + sigma
    return d, jnp.where(inside_mask(sizes, level, gx, gy), DAMPING / d, 0.0)


def down_kernel(sizes, at_ref, g_ref, s_ref, rows_a_ref, rows_b_ref, columns_a_ref, columns_b_ref,
                rc0_ref, rc1_ref, pc_ref,
                g0_ref, d0_ref, w0_ref, v0_ref, c1_ref, d1_ref, w1_ref, v1_ref, d2_ref, w2_ref, out_ref, scratch):
    gx, gy = at_ref[0], at_ref[1]
    rows = sizes.ext_rows[0]
    lane = iota((rows, 128), 1)
    below, above = sides(gx, rows_a_ref, rows_b_ref)
    from_right, from_left = sides(gy, columns_a_ref, columns_b_ref)
    g = jnp.where(lane < HALO, from_right, from_left)
    sigma = jnp.where(lane < HALO, pltpu.roll(from_right, 128 - HALO, 1), pltpu.roll(from_left, HALO, 1))
    g = jnp.concatenate([jnp.concatenate([g_ref[...], below[0], above[0]], axis=0), g], axis=1)
    sigma = jnp.concatenate([jnp.concatenate([s_ref[...], below[1], above[1]], axis=0), sigma], axis=1)
    d, w = coefficients(sizes, 0, gx, gy, sigma)
    v = w * g
    v = sweep(v, g, w)
    r = g - d * v + around(v)
    for ref, values in ((g0_ref, g), (d0_ref, d), (w0_ref, w), (v0_ref, v)):
        ref[...] = near(values, sizes.rows)
    both = []
    own, halo = sizes.rows // 2, HALOS[1]
    for values in (r, sigma):
        pairs = pair_rows(scratch, values)
        both += [pairs[: own + halo], pairs[pairs.shape[0] - halo :]]
    both = f32dot_right(jnp.concatenate(both, axis=0), rc0_ref[...])
    half = own + 2 * halo
    g, sigma = both[:half], both[half:]
    d, w = coefficients(sizes, 1, gx, gy, sigma)
    v = w * g
    v = sweep(v, g, w)
    r = g - d * v + around(v)
    c1_ref[...] = g
    d1_ref[...] = d
    w1_ref[...] = w
    v1_ref[...] = v
    half = half // 2
    both = jnp.concatenate([pair_rows(scratch, r), pair_rows(scratch, sigma)], axis=0)
    both = f32dot_right(both, rc1_ref[...])
    g, sigma = both[:half], both[half:]
    d, w = coefficients(sizes, 2, gx, gy, sigma)
    d2_ref[...] = d
    w2_ref[...] = w
    own = sizes.rows // 4
    pack_two(sizes, gy, g[:own], sigma[:own], scratch, pc_ref, out_ref)


class Coarse:
    def __init__(self, sizes, first, d_refs, w_refs, g_refs, v_refs, t_refs):
        self.z = sizes
        self.first = first
        self.d, self.w, self.g, self.v, self.t = d_refs, w_refs, g_refs, v_refs, t_refs
        lane = iota((sizes.p, sizes.coarse_columns), 1)
        self.first_lane, self.last_lane = lane == 0, lane == sizes.coarse_columns - 1

    def blocks(self, body):
        p = self.z.p
        if self.z.nx <= 4:
            for gx in range(self.z.nx):
                body((gx + 1) * p)
        else:
            def step(gx, carry):
                body(pl.multiple_of((gx + 1) * p, 8))
                return carry

            lax.fori_loop(0, self.z.nx, step, 0)

    def at(self, ref, s, r, base):
        return ref[s, r, pl.ds(base, self.z.p), :]

    def put(self, ref, s, r, base, value):
        ref[s, r, pl.ds(base, self.z.p), :] = value

    def beside(self, ref, s, r, base, step):
        p = self.z.p
        if isinstance(base, int):
            return ref[s, r, pl.ds(base + step, p), :]
        return ref[s, r, pl.ds(base - p, 3 * p), :][p + step : 2 * p + step]

    def neighbours(self, ref, s, r, n, base):
        columns = self.z.coarse_columns
        if r < n - 1:
            right = self.at(ref, s, r + 1, base)
        else:
            right = jnp.where(self.last_lane, 0.0, pltpu.roll(self.at(ref, s, 0, base), columns - 1, 1))
        if r > 0:
            left = self.at(ref, s, r - 1, base)
        else:
            left = jnp.where(self.first_lane, 0.0, pltpu.roll(self.at(ref, s, n - 1, base), 1, 1))
        down = self.at(ref, s + 1, r, base) if s < n - 1 else self.beside(ref, 0, r, base, 1)
        up = self.at(ref, s - 1, r, base) if s > 0 else self.beside(ref, n - 1, r, base, -1)
        return (up + down) + (left + right)

    def each(self, level, body):
        n = 1 << (LEVELS - level)

        def block(base):
            for s in range(n):
                for r in range(n):
                    body(s, r, n, base)

        self.blocks(block)

    def first_sweep(self, level):
        l = level - self.first

        def body(s, r, n, base):
            self.put(self.v[l], s, r, base, self.at(self.w[l], s, r, base) * self.at(self.g[l], s, r, base))

        self.each(level, body)

    def sweep(self, level, source, target):
        l = level - self.first

        def body(s, r, n, base):
            v = self.at(source, s, r, base)
            total = self.at(self.g[l], s, r, base) + self.neighbours(source, s, r, n, base)
            self.put(target, s, r, base, (1.0 - DAMPING) * v + self.at(self.w[l], s, r, base) * total)

        self.each(level, body)

    def two_sweeps(self, level):
        l = level - self.first
        self.sweep(level, self.v[l], self.t[l])
        self.sweep(level, self.t[l], self.v[l])

    def start(self, level):
        l = level - self.first
        self.first_sweep(level)
        self.sweep(level, self.v[l], self.t[l])
        self.v[l], self.t[l] = self.t[l], self.v[l]

    def residual(self, level, s, r, n, base):
        l = level - self.first
        v = self.at(self.v[l], s, r, base)
        g = self.at(self.g[l], s, r, base)
        return (g - self.at(self.d[l], s, r, base) * v) + self.neighbours(self.v[l], s, r, n, base)

    def restrict(self, level):
        l = level - self.first
        n = 1 << (LEVELS - level)

        def block(base):
            for s in range(n // 2):
                for r in range(n // 2):
                    parts = [self.residual(level, 2 * s + a, 2 * r + b, n, base) for a in (0, 1) for b in (0, 1)]
                    self.put(self.g[l + 1], s, r, base, (parts[0] + parts[1]) + (parts[2] + parts[3]))

        self.blocks(block)

    def prolong(self, level):
        l = level - self.first

        def body(s, r, n, base):
            e = self.at(self.v[l + 1], s // 2, r // 2, base)
            self.put(self.v[l], s, r, base, self.at(self.v[l], s, r, base) + e)

        self.each(level, body)

    def inner(self, ref):
        p = self.z.p
        return ref[0, 0, p : p + self.z.coarse_rows, :]

    def shifted(self, x, k):
        if k == 0:
            return x
        columns = self.z.coarse_columns
        lane = iota(x.shape, 1)
        keep = lane < columns - k if k > 0 else lane >= -k
        return jnp.where(keep, pltpu.roll(x, -k % columns, 1), 0.0)

    def unit(self):
        z = self.z
        top = LEVELS - self.first
        d, w = self.inner(self.d[top]), self.inner(self.w[top])
        missing = 2.0 * (z.coarse_rows + z.coarse_columns)
        return 1.0 / (jnp.sum(d - 4.0, keepdims=True) + missing), {k: self.shifted(w, k) for k in range(-2, 3)}

    def coarse(self, fresh, unit):
        top = LEVELS - self.first
        one, w = unit
        g = self.inner(self.g[top])
        shape = g.shape
        row, lane = iota(shape, 0), iota(shape, 1)
        first_row, last_row = row == 0, row == shape[0] - 1
        sources = {k: self.shifted(g, k) for k in range(-2, 3)}

        def vertical(x):
            return jnp.where(first_row, 0.0, pltpu.roll(x, 1, 0)) + jnp.where(last_row, 0.0, pltpu.roll(x, shape[0] - 1, 0))

        def three(v):
            for reach in (2, 1, 0):
                v = {
                    k: (1.0 - DAMPING) * v[k] + w[k] * ((sources[k] + vertical(v[k])) + (v[k - 1] + v[k + 1]))
                    for k in range(-reach, reach + 1)
                }
            return v[0]

        if fresh:
            left = jnp.sum(g, keepdims=True) * one
            v = {k: 0.0 for k in range(-3, 4)}
        else:
            v = self.inner(self.v[top])
            v = {k: self.shifted(v, k) for k in range(-3, 4)}
            around_v = vertical(v[0]) + (v[-1] + v[1])
            left = jnp.sum((g - self.inner(self.d[top]) * v[0]) + around_v, keepdims=True) * one
        left = jnp.broadcast_to(left, shape)
        for k in range(-3, 4):
            v[k] = v[k] + jnp.where((lane < shape[1] - k) & (lane >= -k), left, 0.0)
        for turn in range(COARSE_SWEEPS // 3):
            if turn:
                v = {k: self.shifted(v, k) for k in range(-3, 4)}
            v = three(v)
        p = self.z.p
        self.v[top][0, 0, p : p + shape[0], :] = v

    def vcycle(self, level, fresh, unit):
        if level == LEVELS:
            self.coarse(fresh, unit)
            return
        if fresh:
            self.start(level)
        else:
            self.two_sweeps(level)
        self.restrict(level)
        self.vcycle(level + 1, True, unit)
        self.prolong(level)
        self.two_sweeps(level)

    def fcycle(self, level, unit):
        if level == LEVELS:
            self.coarse(True, unit)
            return
        self.start(level)
        self.restrict(level)
        self.fcycle(level + 1, unit)
        self.vcycle(level + 1, False, unit)
        self.prolong(level)
        self.two_sweeps(level)

    def clear_ends(self):
        z = self.z
        zero = jnp.zeros((z.p, z.coarse_columns), jnp.float32)
        for refs in (self.v, self.t):
            for ref in refs:
                n = ref.shape[0]
                for s in range(n):
                    for r in range(n):
                        ref[s, r, : z.p, :] = zero
                        ref[s, r, z.p + z.coarse_rows :, :] = zero

    def turned(self, blocks, k):
        q = self.z.q
        part = iota(blocks[0].shape, 1) // q
        out = blocks[-k % 8]
        for x in range(1, 8):
            out = jnp.where(part == x, blocks[(x - k) % 8], out)
        return pltpu.roll(out, -k * q % 128, 1) if k else out

    def take_two(self, even_ref, odd_ref, targets):
        z = self.z
        for gx in range(z.nx):
            for group in range(z.ny // 8):
                lanes = slice(group * 128, (group + 1) * 128)
                for s in range(4):
                    blocks = []
                    for g in range(8):
                        first = (gx * (z.ny // 2) + group * 4 + g // 2) * 4 * z.p + s * z.p
                        blocks.append((even_ref, odd_ref)[g % 2][first : first + z.p, :])
                    for k in range(8):
                        target, add = targets[k // 4]
                        value = self.turned(blocks, k)
                        target[s, k % 4, (gx + 1) * z.p : (gx + 2) * z.p, lanes] = value + add if add else value

    def take_one(self, y_ref, target):
        z = self.z
        low = iota((8, 128), 0) < 4
        for gx in range(z.nx):
            for group in range(z.ny // 8):
                upper, lower = [], []
                for g in range(0, 8, 2):
                    first = (gx * z.ny + group * 8 + g) * 4
                    pair = y_ref[first : first + 8, :]
                    swapped = pltpu.roll(pair, 4, 0)
                    upper += [pair, swapped]
                    lower += [swapped, pair]
                for k in range(4):
                    value = jnp.where(low, self.turned(upper, k), self.turned(lower, k + 4))
                    target[k // 2, k % 2, (gx + 1) * z.p : (gx + 2) * z.p, group * 128 : (group + 1) * 128] = value

    def spread(self, gx, gy, columns_ref, scratch):
        z = self.z
        n = 1 << (LEVELS - self.first)
        above = self.first - 1
        columns = z.coarse_columns
        turn = lax.rem(columns + z.q - gy * z.q, columns)
        start = pl.multiple_of(gx * z.p, 8)
        parts = []
        for s in range(n):
            line = [pltpu.roll(self.v[0][s, r, pl.ds(start, 3 * z.p), :], turn, 1)[:, :128] for r in range(n)]
            parts.append(jnp.concatenate(line, axis=1))
        wide = f32dot_right(jnp.concatenate(parts, axis=0), columns_ref[...])
        own, halo = z.rows >> above, HALOS[above]
        inner, outer = (own + halo) // (2 * n), halo // (2 * n)
        tiles = wide.shape[1] // 128
        for t in range(tiles):
            for s in range(n):
                part = wide[s * 3 * z.p : (s + 1) * 3 * z.p, t * 128 : (t + 1) * 128]
                for a in range(2):
                    scratch[t, pl.ds(2 * s + a, inner, stride=2 * n), :] = part[z.p : z.p + inner]
                    scratch[t, pl.ds(own + halo + 2 * s + a, outer, stride=2 * n), :] = part[z.p - outer : z.p]
        return jnp.concatenate([scratch[t, : own + 2 * halo, :] for t in range(tiles)], axis=1)


def level_shape(sizes, level):
    n = 1 << (LEVELS - level)
    return (n, n, sizes.coarse_rows + 2 * sizes.p, sizes.coarse_columns)


def middle_kernel(sizes, at_ref, y_ref, other_ref, c1_ref, d1_ref, w1_ref, v1_ref, w2l_ref, d2l_ref, sc_ref,
                  rc1_ref, pc_ref,
                  d3_ref, d4_ref, w3_ref, w4_ref, e1_ref, c2_ref, e2_ref, out_ref,
                  d2, w2, g2, g3, g4, v2, v3, v4, t2, t3, t4, scratch):
    gx, gy = at_ref[0], at_ref[1]
    m = Coarse(sizes, 2, [d2, d3_ref, d4_ref], [w2, w3_ref, w4_ref], [g2, g3, g4], [v2, v3, v4], [t2, t3, t4])
    m.clear_ends()
    core = lax.rem(gy, 2)

    @pl.when(core == 0)
    def _():
        m.take_two(y_ref, other_ref, ((g2, 0.0), (d2, 4.0)))

    @pl.when(core == 1)
    def _():
        m.take_two(other_ref, y_ref, ((g2, 0.0), (d2, 4.0)))

    for l in range(2):
        n = 2 >> l

        def block(base):
            for s in range(n):
                for r in range(n):
                    parts = [m.at(m.d[l], 2 * s + a, 2 * r + b, base) for a in (0, 1) for b in (0, 1)]
                    m.put(m.d[l + 1], s, r, base, ((parts[0] + parts[1]) + (parts[2] + parts[3])) - 12.0)

        m.blocks(block)
    for l in range(3):
        def body(s, r, n, base):
            m.put(m.w[l], s, r, base, DAMPING / m.at(m.d[l], s, r, base))

        m.each(l + 2, body)
    unit = m.unit()
    m.fcycle(2, unit)
    m.vcycle(2, False, unit)
    g, d, w = c1_ref[...], d1_ref[...], w1_ref[...]
    v = v1_ref[...] + jnp.where(w > 0.0, m.spread(gx, gy, sc_ref, scratch), 0.0)
    for turn in range(4):
        v = sweep(v, g, w)
    e1_ref[...] = v
    r = g - d * v + around(v)
    g = f32dot_right(pair_rows(scratch, r), rc1_ref[...])
    d, w = d2l_ref[...], w2l_ref[...]
    v = w * g
    v = sweep(v, g, w)
    r = g - d * v + around(v)
    c2_ref[...] = g
    e2_ref[...] = v
    pack_one(sizes, gy, pair_rows(scratch, r[: sizes.rows // 4]), scratch, pc_ref, out_ref)


def up_kernel(sizes, at_ref, y_ref, d3_ref, d4_ref, w3_ref, w4_ref, c2_ref, w2_ref, e2_ref, c1_ref, w1_ref, e1_ref,
              g0_ref, d0_ref, w0_ref, v0_ref, sc_ref, pc1_ref, pc0_ref,
              solution_ref, residual_ref, g3, g4, v3, v4, t3, t4, scratch):
    gx, gy = at_ref[0], at_ref[1]
    m = Coarse(sizes, 3, [d3_ref, d4_ref], [w3_ref, w4_ref], [g3, g4], [v3, v4], [t3, t4])
    m.clear_ends()
    m.take_one(y_ref, g3)
    m.vcycle(3, True, m.unit())
    g, w = c2_ref[...], w2_ref[...]
    v = e2_ref[...] + jnp.where(w > 0.0, m.spread(gx, gy, sc_ref, scratch), 0.0)
    for turn in range(2):
        v = sweep(v, g, w)
    own = sizes.rows // 2
    g, w = near(c1_ref, own), near(w1_ref, own)
    v = near(e1_ref, own) + near(double_rows(scratch, f32dot_right(v, pc1_ref[...])), own)
    for turn in range(2):
        v = sweep(v, g, w)
    g, d, w = g0_ref[...], d0_ref[...], w0_ref[...]
    v = v0_ref[...] + near(double_rows(scratch, f32dot_right(v, pc0_ref[...])), sizes.rows)
    for turn in range(2):
        v = sweep(v, g, w)
    r = g - d * v + around(v)
    solution_ref[...] = v[: sizes.rows, : sizes.columns]
    residual_ref[...] = r[: sizes.rows, : sizes.columns]


def vmem(count):
    return [pl.BlockSpec(memory_space=pltpu.VMEM)] * count


def call(kernel, sizes, outs, scratch, *operands):
    shapes = [jax.ShapeDtypeStruct(shape, jnp.float32) for shape in outs]
    used = sum(4 * int(np.prod(shape)) for shape in list(outs) + list(scratch))
    used += sum(x.size * x.dtype.itemsize for x in operands)
    return pl.pallas_call(
        lambda *refs: kernel(sizes, *refs),
        name=kernel.__name__,
        out_shape=shapes,
        in_specs=[pl.BlockSpec(memory_space=pltpu.SMEM)] + vmem(len(operands) - 1),
        out_specs=vmem(len(outs)),
        scratch_shapes=[pltpu.VMEM(shape, jnp.float32) for shape in scratch],
        compiler_params=pltpu.CompilerParams(vmem_limit_bytes=used + used // 4 + (4 << 20)),
    )(*operands)


def swaps(first, second, axis, spare):
    nx, ny = lax.axis_size("gx"), lax.axis_size("gy")
    count = lax.axis_size(axis)

    def target(gx, gy):
        place = gx if axis == "gx" else gy
        if place in (0, count - 1):
            return (gx ^ 1) * ny + gy if spare == "gx" else gx * ny + (gy ^ 1)
        place = place + 1 if place % 2 else place - 1
        return place * ny + gy if axis == "gx" else gx * ny + place

    pairs = [(gx * ny + gy, target(gx, gy)) for gx in range(nx) for gy in range(ny)]
    return lax.ppermute(first, axis, [(i, i ^ 1) for i in range(count)]), lax.ppermute(second, ("gx", "gy"), pairs)


def gather(copies):
    return lax.all_to_all(copies, ("gx", "gy"), 0, 0, tiled=True)


def gather_by_core(copies, nx, ny):
    index = np.arange(nx * ny)
    groups = [index[core::2].tolist() for core in range(2)]
    own = lax.all_to_all(copies, ("gx", "gy"), 0, 0, tiled=True, axis_index_groups=groups)
    return own, lax.ppermute(own, "gy", [(j, j ^ 1) for j in range(ny)])


def body(right_side, shift):
    nx, ny = lax.axis_size("gx"), lax.axis_size("gy")
    rows, columns = right_side.shape
    z = Sizes(rows, columns, nx, ny)
    at = jnp.stack([lax.axis_index("gx"), lax.axis_index("gy")]).astype(jnp.int32)
    even = lax.axis_index("gx") % 2 == 0

    def strips(start):
        return jnp.stack([lax.dynamic_slice(x, (start, 0), (HALO, columns)) for x in (right_side, shift)])

    last = rows - HALO
    rows_a, rows_b = swaps(strips(jnp.where(even, last, 0)), strips(jnp.where(even, 0, last)), "gx", "gy")
    ext = [(z.ext_rows[l], z.ext_columns[l]) for l in range(3)]
    strip = (z.ext_rows[0], 128)
    first, second = call(strip_kernel, z, [strip] * 2, [], at, right_side, shift, rows_a, rows_b)
    columns_a, columns_b = swaps(first, second, "gy", "gx")
    rc0, rc1 = z.restrict_columns(0), z.restrict_columns(1)
    tiles = (ext[0][1] // 128, ext[0][0], 128)
    g0, d0, w0, v0, c1, d1, w1, v1, d2, w2, packed = call(
        down_kernel, z, [(rows + 2 * NEAR, ext[0][1])] * 4 + [ext[1]] * 4 + [ext[2]] * 2 + [(nx * ny // 2 * 4 * z.p, 128)], [tiles],
        at, right_side, shift, rows_a, rows_b, columns_a, columns_b, rc0, rc1, z.pack_pair())
    y, other = gather_by_core(packed, nx, ny)
    slabs = [level_shape(z, level) for level in (2, 3, 4)]
    d3, d4, w3, w4, e1, c2, e2, packed = call(
        middle_kernel, z, slabs[1:] * 2 + [ext[1], ext[2], ext[2], (nx * ny * 4, 128)],
        [slabs[0]] * 2 + slabs * 3 + [tiles],
        at, y, other, c1, d1, w1, v1, w2, d2, z.spread_columns(2),
        rc1, z.pack_single())
    y = gather(packed)
    return call(
        up_kernel, z, [(rows, columns)] * 2, slabs[1:] * 3 + [tiles],
        at, y, d3, d4, w3, w4, c2, w2, e2, c1, w1, e1, g0, d0, w0, v0,
        z.spread_columns(3), rc1.T, rc0.T)


def solution(mesh):
    specs = (P("gx", "gy"), P("gx", "gy"))

    def run(right_side, shift):
        out = body(right_side, shift)
        return out[0], out[1]

    return jax.shard_map(run, mesh=mesh, in_specs=specs, out_specs=specs, check_vma=False)
```

```python
import numpy as np
import jax
import jax.numpy as jnp
from jax import lax
from jax.experimental import pallas as pl
from jax.experimental.pallas import tpu as pltpu
from jax.sharding import PartitionSpec as P

LEVELS = 4
COARSE_SWEEPS = 6
DAMPING = 0.8
HALOS = (40, 16, 8)
HALO = HALOS[0]
NEAR = 8


def f32dot_right(values, onehot):
    high = values.astype(jnp.bfloat16)
    rest = values - high.astype(jnp.float32)
    middle = rest.astype(jnp.bfloat16)
    low = (rest - middle.astype(jnp.float32)).astype(jnp.bfloat16)
    rows = values.shape[0]
    stacked = jnp.concatenate([high, middle, low], axis=0)
    out = jnp.dot(stacked, onehot, preferred_element_type=jnp.float32)
    return (out[2 * rows :] + out[rows : 2 * rows]) + out[:rows]


def around(v):
    rows, columns = v.shape
    up = pltpu.roll(v, 1, 0)
    down = pltpu.roll(v, rows - 1, 0)
    left = pltpu.roll(v, 1, 1)
    right = pltpu.roll(v, columns - 1, 1)
    return (up + down) + (left + right)


def sweep(v, g, w):
    return (1.0 - DAMPING) * v + w * (g + around(v))


class Sizes:
    def __init__(self, rows, columns, nx, ny):
        self.rows, self.columns, self.nx, self.ny = rows, columns, nx, ny
        self.p, self.q = rows // 16, columns // 16
        self.coarse_rows, self.coarse_columns = nx * self.p, ny * self.q
        assert self.p == 8 and 8 * self.q == 128, "block shape"

        def up(n):
            return -(-n // 128) * 128

        self.ext_rows = [(rows >> l) + 2 * HALOS[l] for l in range(3)]
        self.ext_columns = [up((columns >> l) + 2 * HALOS[l]) for l in range(3)]

    def column_at(self, level):
        own, halo, width = self.columns >> level, HALOS[level], self.ext_columns[level]
        lane = np.arange(width)
        inside = (lane < own + halo) | (lane >= width - halo)
        return np.where(lane < own + halo, lane, lane - width), inside

    def restrict_columns(self, level):
        fine, fine_in = self.column_at(level)
        coarse, coarse_in = self.column_at(level + 1)
        hit = (fine[:, None] // 2 == coarse[None, :]) & fine_in[:, None] & coarse_in[None, :]
        return hit.astype(jnp.bfloat16)

    def pack_pair(self):
        own = self.columns >> 2
        x = np.arange(2 * own)
        target = (x // own) * own + (x % own % 4) * self.q + x % own // 4
        return (target[:, None] == np.arange(2 * own)[None, :]).astype(jnp.bfloat16)

    def pack_single(self):
        x = np.arange(self.ext_columns[2])[:, None]
        lane = np.arange(128)[None, :]
        hit = (x // 2 == 2 * (lane % self.q) + (lane // self.q) % 2) & (x < self.columns >> 2)
        return hit.astype(jnp.bfloat16)

    def spread_columns(self, level):
        n = 1 << (LEVELS - level)
        column, inside = self.column_at(level - 1)
        m = column // 2
        r = np.arange(n)[:, None, None]
        lane = np.arange(128)[None, :, None]
        hit = (m % n == r) & (m // n + self.q == lane) & inside
        return hit.reshape(n * 128, -1).astype(jnp.bfloat16)


def iota(shape, axis):
    return lax.broadcasted_iota(jnp.int32, shape, axis)


def inside_mask(sizes, level, gx, gy):
    shape = (sizes.ext_rows[level], sizes.ext_columns[level])
    own_r, own_c, halo = sizes.rows >> level, sizes.columns >> level, HALOS[level]
    row, column = iota(shape, 0), iota(shape, 1)
    last_row = jnp.where(gx < sizes.nx - 1, own_r + halo, own_r)
    first_row = jnp.where(gx > 0, own_r + halo, shape[0])
    last_column = jnp.where(gy < sizes.ny - 1, own_c + halo, own_c)
    first_column = jnp.where(gy > 0, shape[1] - halo, shape[1])
    return ((row < last_row) | (row >= first_row)) & ((column < last_column) | (column >= first_column))


def pair_rows(scratch, values):
    rows, columns = values.shape
    outs = []
    for t in range(columns // 128):
        scratch[t, :rows, :] = values[:, t * 128 : (t + 1) * 128]
    for t in range(columns // 128):
        outs.append(scratch[t, pl.ds(0, rows // 2, stride=2), :] + scratch[t, pl.ds(1, rows // 2, stride=2), :])
    return jnp.concatenate(outs, axis=1)


def double_rows(scratch, values):
    rows, columns = values.shape
    for t in range(columns // 128):
        part = values[:, t * 128 : (t + 1) * 128]
        scratch[t, pl.ds(0, rows, stride=2), :] = part
        scratch[t, pl.ds(1, rows, stride=2), :] = part
    return jnp.concatenate([scratch[t, : 2 * rows, :] for t in range(columns // 128)], axis=1)


def repeat(block, out_ref):
    height = block.shape[0]
    for k in range(out_ref.shape[0] // height):
        out_ref[k * height : (k + 1) * height, :] = block


def pack_two(sizes, gy, first, second, scratch, columns_ref, out_ref):
    own = sizes.columns >> 2
    both = jnp.where(iota(first.shape, 1) < own, first, pltpu.roll(second, own, 1))
    rows = both.shape[0]
    scratch[0, :rows, :] = f32dot_right(both, columns_ref[...])
    block = jnp.concatenate([scratch[0, pl.ds(s, sizes.p, stride=4), :] for s in range(4)], axis=0)
    repeat(pltpu.roll(block, lax.rem(gy, 8) * sizes.q, 1), out_ref)


def pack_one(sizes, gy, values, scratch, columns_ref, out_ref):
    rows = values.shape[0]
    scratch[0, :rows, :] = f32dot_right(values, columns_ref[...])
    part = iota((4, 128), 1) // (2 * sizes.q)
    block = scratch[0, pl.ds(0, 4, stride=2), :]
    for k in range(1, 4):
        block = jnp.where(part == k, scratch[0, pl.ds(8 * (k // 2) + k % 2, 4, stride=2), :], block)
    block = jnp.concatenate([block, block], axis=0)
    repeat(pltpu.roll(block, lax.rem(gy, 8) * sizes.q, 1), out_ref)


def near(values, own):
    return jnp.concatenate([values[: own + NEAR], values[values.shape[0] - NEAR :]], axis=0)


def sides(at, first_ref, second_ref):
    even = lax.rem(at, 2) == 0
    first, second = first_ref[...], second_ref[...]
    return jnp.where(even, first, second), jnp.where(even, second, first)


def rows_kernel(sizes, g_ref, s_ref, first_ref, second_ref, semaphores):
    even = lax.rem(lax.axis_index("gx"), 2) == 0
    last = sizes.rows - HALO
    copies = []
    for k, (out, start) in enumerate(((first_ref, jnp.where(even, last, 0)), (second_ref, jnp.where(even, 0, last)))):
        for f, ref in enumerate((g_ref, s_ref)):
            rows = pl.ds(pl.multiple_of(start, 8), HALO)
            copies.append(pltpu.make_async_copy(ref.at[rows, :], out.at[f], semaphores.at[2 * k + f]))
    for copy in copies:
        copy.start()
    for copy in copies:
        copy.wait()


def strip_kernel(sizes, g_ref, s_ref, rows_a_ref, rows_b_ref, first_ref, second_ref):
    last = sizes.columns - 128
    even = lax.rem(lax.axis_index("gy"), 2) == 0
    below, above = sides(lax.axis_index("gx"), rows_a_ref, rows_b_ref)
    start = 0
    for g, s in ((g_ref[...], s_ref[...]), (below[0], below[1]), (above[0], above[1])):
        rows = slice(start, start + g.shape[0])
        start += g.shape[0]
        lane = iota((g.shape[0], 128), 1)
        left = jnp.where(lane < HALO, g[:, :128], pltpu.roll(s[:, :128], HALO, 1))
        right = jnp.where(lane >= 128 - HALO, g[:, last:], pltpu.roll(s[:, last:], 128 - HALO, 1))
        first_ref[rows, :] = jnp.where(even, right, left)
        second_ref[rows, :] = jnp.where(even, left, right)


def coefficients(sizes, level, gx, gy, sigma):
    d = 4.0 + sigma
    return d, jnp.where(inside_mask(sizes, level, gx, gy), DAMPING / d, 0.0)


def down_kernel(sizes, g_ref, s_ref, rows_a_ref, rows_b_ref, columns_a_ref, columns_b_ref,
                rc0_ref, rc1_ref, pc_ref,
                g0_ref, d0_ref, w0_ref, v0_ref, c1_ref, d1_ref, w1_ref, v1_ref, d2_ref, w2_ref, out_ref, scratch):
    gx, gy = lax.axis_index("gx"), lax.axis_index("gy")
    rows = sizes.ext_rows[0]
    lane = iota((rows, 128), 1)
    below, above = sides(gx, rows_a_ref, rows_b_ref)
    from_right, from_left = sides(gy, columns_a_ref, columns_b_ref)
    g = jnp.where(lane < HALO, from_right, from_left)
    sigma = jnp.where(lane < HALO, pltpu.roll(from_right, 128 - HALO, 1), pltpu.roll(from_left, HALO, 1))
    g = jnp.concatenate([jnp.concatenate([g_ref[...], below[0], above[0]], axis=0), g], axis=1)
    sigma = jnp.concatenate([jnp.concatenate([s_ref[...], below[1], above[1]], axis=0), sigma], axis=1)
    d, w = coefficients(sizes, 0, gx, gy, sigma)
    v = w * g
    v = sweep(v, g, w)
    r = g - d * v + around(v)
    for ref, values in ((g0_ref, g), (d0_ref, d), (w0_ref, w), (v0_ref, v)):
        ref[...] = near(values, sizes.rows)
    both = []
    own, halo = sizes.rows // 2, HALOS[1]
    for values in (r, sigma):
        pairs = pair_rows(scratch, values)
        both += [pairs[: own + halo], pairs[pairs.shape[0] - halo :]]
    both = f32dot_right(jnp.concatenate(both, axis=0), rc0_ref[...])
    half = own + 2 * halo
    g, sigma = both[:half], both[half:]
    d, w = coefficients(sizes, 1, gx, gy, sigma)
    v = w * g
    v = sweep(v, g, w)
    r = g - d * v + around(v)
    c1_ref[...] = g
    d1_ref[...] = d
    w1_ref[...] = w
    v1_ref[...] = v
    half = half // 2
    both = jnp.concatenate([pair_rows(scratch, r), pair_rows(scratch, sigma)], axis=0)
    both = f32dot_right(both, rc1_ref[...])
    g, sigma = both[:half], both[half:]
    d, w = coefficients(sizes, 2, gx, gy, sigma)
    d2_ref[...] = d
    w2_ref[...] = w
    own = sizes.rows // 4
    pack_two(sizes, gy, g[:own], sigma[:own], scratch, pc_ref, out_ref)


class Coarse:
    def __init__(self, sizes, first, d_refs, w_refs, g_refs, v_refs, t_refs, coarsest):
        self.z = sizes
        self.first = first
        self.d, self.w, self.g, self.v, self.t = d_refs, w_refs, g_refs, v_refs, t_refs
        self.va, self.vb, self.wk, self.gk = coarsest
        lane = iota((sizes.p, sizes.coarse_columns), 1)
        self.first_lane, self.last_lane = lane == 0, lane == sizes.coarse_columns - 1

    def blocks(self, body):
        p = self.z.p
        if self.z.nx <= 4:
            for gx in range(self.z.nx):
                body((gx + 1) * p)
        else:
            def step(gx, carry):
                body(pl.multiple_of((gx + 1) * p, 8))
                return carry

            lax.fori_loop(0, self.z.nx, step, 0)

    def at(self, ref, s, r, base):
        return ref[s, r, pl.ds(base, self.z.p), :]

    def put(self, ref, s, r, base, value):
        ref[s, r, pl.ds(base, self.z.p), :] = value

    def beside(self, ref, s, r, base, step):
        p = self.z.p
        if isinstance(base, int):
            return ref[s, r, pl.ds(base + step, p), :]
        return ref[s, r, pl.ds(base - p, 3 * p), :][p + step : 2 * p + step]

    def neighbours(self, ref, s, r, n, base):
        columns = self.z.coarse_columns
        if r < n - 1:
            right = self.at(ref, s, r + 1, base)
        else:
            right = jnp.where(self.last_lane, 0.0, pltpu.roll(self.at(ref, s, 0, base), columns - 1, 1))
        if r > 0:
            left = self.at(ref, s, r - 1, base)
        else:
            left = jnp.where(self.first_lane, 0.0, pltpu.roll(self.at(ref, s, n - 1, base), 1, 1))
        down = self.at(ref, s + 1, r, base) if s < n - 1 else self.beside(ref, 0, r, base, 1)
        up = self.at(ref, s - 1, r, base) if s > 0 else self.beside(ref, n - 1, r, base, -1)
        return (up + down) + (left + right)

    def each(self, level, body):
        n = 1 << (LEVELS - level)

        def block(base):
            for s in range(n):
                for r in range(n):
                    body(s, r, n, base)

        self.blocks(block)

    def first_sweep(self, level):
        l = level - self.first

        def body(s, r, n, base):
            self.put(self.v[l], s, r, base, self.at(self.w[l], s, r, base) * self.at(self.g[l], s, r, base))

        self.each(level, body)

    def sweep(self, level, source, target):
        l = level - self.first

        def body(s, r, n, base):
            v = self.at(source, s, r, base)
            total = self.at(self.g[l], s, r, base) + self.neighbours(source, s, r, n, base)
            self.put(target, s, r, base, (1.0 - DAMPING) * v + self.at(self.w[l], s, r, base) * total)

        self.each(level, body)

    def two_sweeps(self, level):
        l = level - self.first
        self.sweep(level, self.v[l], self.t[l])
        self.sweep(level, self.t[l], self.v[l])

    def start(self, level):
        l = level - self.first
        self.first_sweep(level)
        self.sweep(level, self.v[l], self.t[l])
        self.v[l], self.t[l] = self.t[l], self.v[l]

    def residual(self, level, s, r, n, base):
        l = level - self.first
        v = self.at(self.v[l], s, r, base)
        g = self.at(self.g[l], s, r, base)
        return (g - self.at(self.d[l], s, r, base) * v) + self.neighbours(self.v[l], s, r, n, base)

    def restrict(self, level):
        l = level - self.first
        n = 1 << (LEVELS - level)

        def block(base):
            for s in range(n // 2):
                for r in range(n // 2):
                    parts = [self.residual(level, 2 * s + a, 2 * r + b, n, base) for a in (0, 1) for b in (0, 1)]
                    self.put(self.g[l + 1], s, r, base, (parts[0] + parts[1]) + (parts[2] + parts[3]))

        self.blocks(block)

    def prolong(self, level):
        l = level - self.first

        def body(s, r, n, base):
            e = self.at(self.v[l + 1], s // 2, r // 2, base)
            self.put(self.v[l], s, r, base, self.at(self.v[l], s, r, base) + e)

        self.each(level, body)

    def inner(self, ref):
        p = self.z.p
        return ref[0, 0, p : p + self.z.coarse_rows, :]

    def shifted(self, x, k):
        if k == 0:
            return x
        columns = self.z.coarse_columns
        lane = iota(x.shape, 1)
        keep = lane < columns - k if k > 0 else lane >= -k
        return jnp.where(keep, pltpu.roll(x, -k % columns, 1), 0.0)

    def unit(self):
        z = self.z
        top = LEVELS - self.first
        d, w = self.inner(self.d[top]), self.inner(self.w[top])
        missing = 2.0 * (z.coarse_rows + z.coarse_columns)
        for k in range(-2, 3):
            self.wk[k + 2] = self.shifted(w, k)
        return 1.0 / (jnp.sum(d - 4.0, keepdims=True) + missing)

    def coarse(self, fresh, unit):
        top = LEVELS - self.first
        p, height = self.z.p, self.z.coarse_rows
        g = self.inner(self.g[top])
        for k in range(-2, 3):
            self.gk[k + 2] = self.shifted(g, k)
        lane = iota(g.shape, 1)

        def at(ref, k, step=0):
            return ref[k + 3, p + step : p + step + height, :]

        def put(ref, k, value):
            ref[k + 3, p : p + height, :] = value

        if fresh:
            left = jnp.broadcast_to(jnp.sum(g, keepdims=True) * unit, g.shape)
            v = {k: 0.0 for k in range(-3, 4)}
        else:
            v = self.inner(self.v[top])
            v = {k: self.shifted(v, k) for k in range(-3, 4)}
            put(self.va, 0, v[0])
            around_v = (at(self.va, 0, -1) + at(self.va, 0, 1)) + (v[-1] + v[1])
            left = jnp.sum((g - self.inner(self.d[top]) * v[0]) + around_v, keepdims=True) * unit
            left = jnp.broadcast_to(left, g.shape)
        for k in range(-3, 4):
            inside = (lane < g.shape[1] - k) & (lane >= -k)
            put(self.va, k, v[k] + jnp.where(inside, left, 0.0) if k else v[k] + left)
        for turn in range(COARSE_SWEEPS // 3):
            if turn:
                v = self.inner(self.v[top])
                for k in range(-3, 4):
                    put(self.va, k, self.shifted(v, k))
            source, target = self.va, self.vb
            for reach in (2, 1, 0):
                for k in range(-reach, reach + 1):
                    total = self.gk[k + 2] + (at(source, k, -1) + at(source, k, 1))
                    total = total + (at(source, k - 1) + at(source, k + 1))
                    value = (1.0 - DAMPING) * at(source, k) + self.wk[k + 2] * total
                    if reach:
                        put(target, k, value)
                    else:
                        self.v[top][0, 0, p : p + height, :] = value
                source, target = target, source

    def vcycle(self, level, fresh, unit):
        if level == LEVELS:
            self.coarse(fresh, unit)
            return
        if fresh:
            self.start(level)
        else:
            self.two_sweeps(level)
        self.restrict(level)
        self.vcycle(level + 1, True, unit)
        self.prolong(level)
        self.two_sweeps(level)

    def fcycle(self, level, unit):
        if level == LEVELS:
            self.coarse(True, unit)
            return
        self.start(level)
        self.restrict(level)
        self.fcycle(level + 1, unit)
        self.vcycle(level + 1, False, unit)
        self.prolong(level)
        self.two_sweeps(level)

    def clear_ends(self):
        z = self.z
        zero = jnp.zeros((z.p, z.coarse_columns), jnp.float32)
        for refs in (self.v, self.t):
            for ref in refs:
                n = ref.shape[0]
                for s in range(n):
                    for r in range(n):
                        ref[s, r, : z.p, :] = zero
                        ref[s, r, z.p + z.coarse_rows :, :] = zero
        for ref in (self.va, self.vb):
            for k in range(7):
                ref[k, : z.p, :] = zero
                ref[k, z.p + z.coarse_rows :, :] = zero

    def turned(self, blocks, k):
        q = self.z.q
        part = iota(blocks[0].shape, 1) // q
        out = blocks[-k % 8]
        for x in range(1, 8):
            out = jnp.where(part == x, blocks[(x - k) % 8], out)
        return pltpu.roll(out, -k * q % 128, 1) if k else out

    def take_two(self, even_ref, odd_ref, targets):
        z = self.z
        for gx in range(z.nx):
            for group in range(z.ny // 8):
                lanes = slice(group * 128, (group + 1) * 128)
                for s in range(4):
                    blocks = []
                    for g in range(8):
                        first = (gx * (z.ny // 2) + group * 4 + g // 2) * 4 * z.p + s * z.p
                        blocks.append((even_ref, odd_ref)[g % 2][first : first + z.p, :])
                    for k in range(8):
                        target, add = targets[k // 4]
                        value = self.turned(blocks, k)
                        target[s, k % 4, (gx + 1) * z.p : (gx + 2) * z.p, lanes] = value + add if add else value

    def take_one(self, y_ref, target):
        z = self.z
        low = iota((8, 128), 0) < 4
        for gx in range(z.nx):
            for group in range(z.ny // 8):
                upper, lower = [], []
                for g in range(0, 8, 2):
                    first = (gx * z.ny + group * 8 + g) * 4
                    pair = y_ref[first : first + 8, :]
                    swapped = pltpu.roll(pair, 4, 0)
                    upper += [pair, swapped]
                    lower += [swapped, pair]
                for k in range(4):
                    value = jnp.where(low, self.turned(upper, k), self.turned(lower, k + 4))
                    target[k // 2, k % 2, (gx + 1) * z.p : (gx + 2) * z.p, group * 128 : (group + 1) * 128] = value

    def spread(self, gx, gy, columns_ref, scratch, lines):
        z = self.z
        n = 1 << (LEVELS - self.first)
        above = self.first - 1
        columns = z.coarse_columns
        turn = lax.rem(columns + z.q - gy * z.q, columns)
        start = pl.multiple_of(gx * z.p, 8)
        for s in range(n):
            for r in range(n):
                part = pltpu.roll(self.v[0][s, r, pl.ds(start, 3 * z.p), :], turn, 1)[:, :128]
                lines[r, pl.ds(s, 3 * z.p, stride=n), :] = part
        own, halo = z.rows >> self.first, HALOS[above]
        window = slice(n * z.p - 8, n * z.p + own + 8)
        wide = f32dot_right(jnp.concatenate([lines[r, window, :] for r in range(n)], axis=1), columns_ref[...])
        doubled = double_rows(scratch, jnp.concatenate([wide[8:], wide[:8]], axis=0))
        height = doubled.shape[0]
        return jnp.concatenate([doubled[: 2 * own + halo], doubled[height - halo :]], axis=0)


def level_shape(sizes, level):
    n = 1 << (LEVELS - level)
    return (n, n, sizes.coarse_rows + 2 * sizes.p, sizes.coarse_columns)


def middle_kernel(sizes, y_ref, other_ref, c1_ref, d1_ref, w1_ref, v1_ref, w2l_ref, d2l_ref, sc_ref,
                  rc1_ref, pc_ref,
                  d3_ref, d4_ref, w3_ref, w4_ref, e1_ref, c2_ref, e2_ref, out_ref,
                  d2, w2, g2, g3, g4, v2, v3, v4, t2, t3, t4, scratch, lines, *coarsest):
    gx, gy = lax.axis_index("gx"), lax.axis_index("gy")
    m = Coarse(sizes, 2, [d2, d3_ref, d4_ref], [w2, w3_ref, w4_ref], [g2, g3, g4], [v2, v3, v4], [t2, t3, t4], coarsest)
    m.clear_ends()
    core = lax.rem(gy, 2)

    @pl.when(core == 0)
    def _():
        m.take_two(y_ref, other_ref, ((g2, 0.0), (d2, 4.0)))

    @pl.when(core == 1)
    def _():
        m.take_two(other_ref, y_ref, ((g2, 0.0), (d2, 4.0)))

    for l in range(2):
        n = 2 >> l

        def block(base):
            for s in range(n):
                for r in range(n):
                    parts = [m.at(m.d[l], 2 * s + a, 2 * r + b, base) for a in (0, 1) for b in (0, 1)]
                    m.put(m.d[l + 1], s, r, base, ((parts[0] + parts[1]) + (parts[2] + parts[3])) - 12.0)

        m.blocks(block)
    for l in range(3):
        def body(s, r, n, base):
            m.put(m.w[l], s, r, base, DAMPING / m.at(m.d[l], s, r, base))

        m.each(l + 2, body)
    unit = m.unit()
    m.fcycle(2, unit)
    m.vcycle(2, False, unit)
    g, d, w = c1_ref[...], d1_ref[...], w1_ref[...]
    v = v1_ref[...] + jnp.where(w > 0.0, m.spread(gx, gy, sc_ref, scratch, lines), 0.0)
    for turn in range(4):
        v = sweep(v, g, w)
    e1_ref[...] = v
    r = g - d * v + around(v)
    g = f32dot_right(pair_rows(scratch, r), rc1_ref[...])
    d, w = d2l_ref[...], w2l_ref[...]
    v = w * g
    v = sweep(v, g, w)
    r = g - d * v + around(v)
    c2_ref[...] = g
    e2_ref[...] = v
    pack_one(sizes, gy, pair_rows(scratch, r[: sizes.rows // 4]), scratch, pc_ref, out_ref)


def up_kernel(sizes, y_ref, d3_ref, d4_ref, w3_ref, w4_ref, c2_ref, w2_ref, e2_ref, c1_ref, w1_ref, e1_ref,
              g0_ref, d0_ref, w0_ref, v0_ref, sc_ref, pc1_ref, pc0_ref,
              solution_ref, residual_ref, g3, g4, v3, v4, t3, t4, scratch, lines, *coarsest):
    gx, gy = lax.axis_index("gx"), lax.axis_index("gy")
    m = Coarse(sizes, 3, [d3_ref, d4_ref], [w3_ref, w4_ref], [g3, g4], [v3, v4], [t3, t4], coarsest)
    m.clear_ends()
    m.take_one(y_ref, g3)
    m.vcycle(3, True, m.unit())
    g, w = c2_ref[...], w2_ref[...]
    v = e2_ref[...] + jnp.where(w > 0.0, m.spread(gx, gy, sc_ref, scratch, lines), 0.0)
    for turn in range(2):
        v = sweep(v, g, w)
    own = sizes.rows // 2
    g, w = near(c1_ref, own), near(w1_ref, own)
    v = near(e1_ref, own) + near(double_rows(scratch, f32dot_right(v, pc1_ref[...])), own)
    for turn in range(2):
        v = sweep(v, g, w)
    g, d, w = g0_ref[...], d0_ref[...], w0_ref[...]
    v = v0_ref[...] + near(double_rows(scratch, f32dot_right(v, pc0_ref[...])), sizes.rows)
    for turn in range(2):
        v = sweep(v, g, w)
    r = g - d * v + around(v)
    solution_ref[...] = v[: sizes.rows, : sizes.columns]
    residual_ref[...] = r[: sizes.rows, : sizes.columns]


def vmem(count):
    return [pl.BlockSpec(memory_space=pltpu.VMEM)] * count


def call(kernel, sizes, outs, scratch, *operands, inputs=None, semaphores=()):
    shapes = [jax.ShapeDtypeStruct(shape, jnp.float32) for shape in outs]
    used = sum(4 * int(np.prod(shape)) for shape in list(outs) + list(scratch))
    used += sum(x.size * x.dtype.itemsize for x in operands)
    return pl.pallas_call(
        lambda *refs: kernel(sizes, *refs),
        name=kernel.__name__,
        out_shape=shapes,
        in_specs=vmem(len(operands)) if inputs is None else inputs,
        out_specs=vmem(len(outs)),
        scratch_shapes=[pltpu.VMEM(shape, jnp.float32) for shape in scratch] + list(semaphores),
        compiler_params=pltpu.CompilerParams(vmem_limit_bytes=used + used // 4 + (4 << 20)),
    )(*operands)


def swaps(first, second, axis, spare):
    nx, ny = lax.axis_size("gx"), lax.axis_size("gy")
    count = lax.axis_size(axis)

    def target(gx, gy):
        place = gx if axis == "gx" else gy
        if place in (0, count - 1):
            return (gx ^ 1) * ny + gy if spare == "gx" else gx * ny + (gy ^ 1)
        place = place + 1 if place % 2 else place - 1
        return place * ny + gy if axis == "gx" else gx * ny + place

    pairs = [(gx * ny + gy, target(gx, gy)) for gx in range(nx) for gy in range(ny)]
    return lax.ppermute(first, axis, [(i, i ^ 1) for i in range(count)]), lax.ppermute(second, ("gx", "gy"), pairs)


def gather(copies):
    return lax.all_to_all(copies, ("gx", "gy"), 0, 0, tiled=True)


def gather_by_core(copies, nx, ny):
    index = np.arange(nx * ny)
    groups = [index[core::2].tolist() for core in range(2)]
    own = lax.all_to_all(copies, ("gx", "gy"), 0, 0, tiled=True, axis_index_groups=groups)
    return own, lax.ppermute(own, "gy", [(j, j ^ 1) for j in range(ny)])


def body(right_side, shift):
    nx, ny = lax.axis_size("gx"), lax.axis_size("gy")
    rows, columns = right_side.shape
    z = Sizes(rows, columns, nx, ny)
    first, second = call(
        rows_kernel, z, [(2, HALO, columns)] * 2, [], right_side, shift,
        inputs=[pl.BlockSpec(memory_space=pl.ANY)] * 2, semaphores=[pltpu.SemaphoreType.DMA((4,))])
    rows_a, rows_b = swaps(first, second, "gx", "gy")
    ext = [(z.ext_rows[l], z.ext_columns[l]) for l in range(3)]
    strip = (z.ext_rows[0], 128)
    first, second = call(strip_kernel, z, [strip] * 2, [], right_side, shift, rows_a, rows_b)
    columns_a, columns_b = swaps(first, second, "gy", "gx")
    rc0, rc1 = z.restrict_columns(0), z.restrict_columns(1)
    tiles = (ext[0][1] // 128, ext[0][0], 128)
    g0, d0, w0, v0, c1, d1, w1, v1, d2, w2, packed = call(
        down_kernel, z, [(rows + 2 * NEAR, ext[0][1])] * 4 + [ext[1]] * 4 + [ext[2]] * 2 + [(nx * ny // 2 * 4 * z.p, 128)], [tiles],
        right_side, shift, rows_a, rows_b, columns_a, columns_b, rc0, rc1, z.pack_pair())
    y, other = gather_by_core(packed, nx, ny)
    slabs = [level_shape(z, level) for level in (2, 3, 4)]
    coarsest = [(7,) + slabs[2][2:]] * 2 + [(5, z.coarse_rows, z.coarse_columns)] * 2
    d3, d4, w3, w4, e1, c2, e2, packed = call(
        middle_kernel, z, slabs[1:] * 2 + [ext[1], ext[2], ext[2], (nx * ny * 4, 128)],
        [slabs[0]] * 2 + slabs * 3 + [tiles, (4, 12 * z.p, 128)] + coarsest,
        y, other, c1, d1, w1, v1, w2, d2, z.spread_columns(2),
        rc1, z.pack_single())
    y = gather(packed)
    return call(
        up_kernel, z, [(rows, columns)] * 2, slabs[1:] * 3 + [tiles, (2, 6 * z.p, 128)] + coarsest,
        y, d3, d4, w3, w4, c2, w2, e2, c1, w1, e1, g0, d0, w0, v0,
        z.spread_columns(3), rc1.T, rc0.T)


def solution(mesh):
    specs = (P("gx", "gy"), P("gx", "gy"))

    def run(right_side, shift):
        out = body(right_side, shift)
        return out[0], out[1]

    return jax.shard_map(run, mesh=mesh, in_specs=specs, out_specs=specs, check_vma=False)
```

```python
import numpy as np
import jax
import jax.numpy as jnp
from jax import lax
from jax.experimental import pallas as pl
from jax.experimental.pallas import tpu as pltpu
from jax.sharding import PartitionSpec as P

LEVELS = 4
COARSE_SWEEPS = 6
DAMPING = 0.8
HALOS = (40, 16, 8)
HALO = HALOS[0]
NEAR = 8


def f32dot_right(values, onehot):
    high = values.astype(jnp.bfloat16)
    rest = values - high.astype(jnp.float32)
    middle = rest.astype(jnp.bfloat16)
    low = (rest - middle.astype(jnp.float32)).astype(jnp.bfloat16)
    rows = values.shape[0]
    stacked = jnp.concatenate([high, middle, low], axis=0)
    out = jnp.dot(stacked, onehot, preferred_element_type=jnp.float32)
    return (out[2 * rows :] + out[rows : 2 * rows]) + out[:rows]


def around(v):
    rows, columns = v.shape
    up = pltpu.roll(v, 1, 0)
    down = pltpu.roll(v, rows - 1, 0)
    left = pltpu.roll(v, 1, 1)
    right = pltpu.roll(v, columns - 1, 1)
    return (up + down) + (left + right)


def sweep(v, g, w):
    return (1.0 - DAMPING) * v + w * (g + around(v))


class Sizes:
    def __init__(self, rows, columns, nx, ny):
        self.rows, self.columns, self.nx, self.ny = rows, columns, nx, ny
        self.p, self.q = rows // 16, columns // 16
        self.coarse_rows, self.coarse_columns = nx * self.p, ny * self.q
        assert self.p == 8 and 8 * self.q == 128, "block shape"

        def up(n):
            return -(-n // 128) * 128

        self.ext_rows = [(rows >> l) + 2 * HALOS[l] for l in range(3)]
        self.ext_columns = [up((columns >> l) + 2 * HALOS[l]) for l in range(3)]

    def column_at(self, level):
        own, halo, width = self.columns >> level, HALOS[level], self.ext_columns[level]
        lane = np.arange(width)
        inside = (lane < own + halo) | (lane >= width - halo)
        return np.where(lane < own + halo, lane, lane - width), inside

    def restrict_columns(self, level):
        fine, fine_in = self.column_at(level)
        coarse, coarse_in = self.column_at(level + 1)
        hit = (fine[:, None] // 2 == coarse[None, :]) & fine_in[:, None] & coarse_in[None, :]
        return hit.astype(jnp.bfloat16)

    def pack_pair(self):
        own = self.columns >> 2
        x = np.arange(2 * own)
        target = (x // own) * own + (x % own % 4) * self.q + x % own // 4
        return (target[:, None] == np.arange(2 * own)[None, :]).astype(jnp.bfloat16)

    def pack_single(self):
        x = np.arange(self.ext_columns[2])[:, None]
        lane = np.arange(128)[None, :]
        hit = (x // 2 == 2 * (lane % self.q) + (lane // self.q) % 2) & (x < self.columns >> 2)
        return hit.astype(jnp.bfloat16)

    def spread_columns(self, level):
        n = 1 << (LEVELS - level)
        column, inside = self.column_at(level - 1)
        m = column // 2
        r = np.arange(n)[:, None, None]
        lane = np.arange(128)[None, :, None]
        hit = (m % n == r) & (m // n + self.q == lane) & inside
        return hit.reshape(n * 128, -1).astype(jnp.bfloat16)


def iota(shape, axis):
    return lax.broadcasted_iota(jnp.int32, shape, axis)


def inside_mask(sizes, level, gx, gy):
    shape = (sizes.ext_rows[level], sizes.ext_columns[level])
    own_r, own_c, halo = sizes.rows >> level, sizes.columns >> level, HALOS[level]
    row, column = iota(shape, 0), iota(shape, 1)
    last_row = jnp.where(gx < sizes.nx - 1, own_r + halo, own_r)
    first_row = jnp.where(gx > 0, own_r + halo, shape[0])
    last_column = jnp.where(gy < sizes.ny - 1, own_c + halo, own_c)
    first_column = jnp.where(gy > 0, shape[1] - halo, shape[1])
    return ((row < last_row) | (row >= first_row)) & ((column < last_column) | (column >= first_column))


def pair_rows(scratch, values):
    rows, columns = values.shape
    outs = []
    for t in range(columns // 128):
        scratch[t, :rows, :] = values[:, t * 128 : (t + 1) * 128]
    for t in range(columns // 128):
        outs.append(scratch[t, pl.ds(0, rows // 2, stride=2), :] + scratch[t, pl.ds(1, rows // 2, stride=2), :])
    return jnp.concatenate(outs, axis=1)


def double_rows(scratch, values):
    rows, columns = values.shape
    for t in range(columns // 128):
        part = values[:, t * 128 : (t + 1) * 128]
        scratch[t, pl.ds(0, rows, stride=2), :] = part
        scratch[t, pl.ds(1, rows, stride=2), :] = part
    return jnp.concatenate([scratch[t, : 2 * rows, :] for t in range(columns // 128)], axis=1)


def repeat(block, out_ref):
    height = block.shape[0]
    for k in range(out_ref.shape[0] // height):
        out_ref[k * height : (k + 1) * height, :] = block


def pack_two(sizes, gy, first, second, scratch, columns_ref, out_ref):
    own = sizes.columns >> 2
    both = jnp.where(iota(first.shape, 1) < own, first, pltpu.roll(second, own, 1))
    rows = both.shape[0]
    scratch[0, :rows, :] = f32dot_right(both, columns_ref[...])
    block = jnp.concatenate([scratch[0, pl.ds(s, sizes.p, stride=4), :] for s in range(4)], axis=0)
    repeat(pltpu.roll(block, lax.rem(gy, 8) * sizes.q, 1), out_ref)


def pack_one(sizes, gy, values, scratch, columns_ref, out_ref):
    rows = values.shape[0]
    scratch[0, :rows, :] = f32dot_right(values, columns_ref[...])
    part = iota((4, 128), 1) // (2 * sizes.q)
    block = scratch[0, pl.ds(0, 4, stride=2), :]
    for k in range(1, 4):
        block = jnp.where(part == k, scratch[0, pl.ds(8 * (k // 2) + k % 2, 4, stride=2), :], block)
    block = jnp.concatenate([block, block], axis=0)
    repeat(pltpu.roll(block, lax.rem(gy, 8) * sizes.q, 1), out_ref)


def near(values, own):
    return jnp.concatenate([values[: own + NEAR], values[values.shape[0] - NEAR :]], axis=0)


def sides(at, first_ref, second_ref):
    even = lax.rem(at, 2) == 0
    first, second = first_ref[...], second_ref[...]
    return jnp.where(even, first, second), jnp.where(even, second, first)


def rows_kernel(sizes, g_ref, s_ref, first_ref, second_ref, semaphores):
    even = lax.rem(lax.axis_index("gx"), 2) == 0
    last = sizes.rows - HALO
    copies = []
    for k, (out, start) in enumerate(((first_ref, jnp.where(even, last, 0)), (second_ref, jnp.where(even, 0, last)))):
        for f, ref in enumerate((g_ref, s_ref)):
            rows = pl.ds(pl.multiple_of(start, 8), HALO)
            copies.append(pltpu.make_async_copy(ref.at[rows, :], out.at[f], semaphores.at[2 * k + f]))
    for copy in copies:
        copy.start()
    for copy in copies:
        copy.wait()


def strip_rows(sizes):
    groups = 128 // HALO
    return groups, -(-2 * sizes.ext_rows[0] // (8 * groups)) * 8


def fold(sizes, strip, step):
    groups, height = strip_rows(sizes)
    lane = iota((height, 128), 1)
    lane = lane if step > 0 else 127 - lane
    out = strip[:height]
    for k in range(1, groups):
        part = strip[k * height : (k + 1) * height]
        part = pltpu.roll(part, k * step % 128, 1)
        if part.shape[0] < height:
            part = jnp.concatenate([part, jnp.zeros((height - part.shape[0], 128), jnp.float32)], axis=0)
        out = jnp.where(lane >= k * HALO, part, out)
    return out


def unfold(sizes, packed, step):
    groups, _ = strip_rows(sizes)
    parts = [packed] + [pltpu.roll(packed, -k * step % 128, 1) for k in range(1, groups)]
    rows = sizes.ext_rows[0]
    out = jnp.concatenate(parts, axis=0)
    return out[:rows], out[rows : 2 * rows]


def strip_kernel(sizes, g_ref, s_ref, rows_a_ref, rows_b_ref, first_ref, second_ref):
    last = sizes.columns - 128
    even = lax.rem(lax.axis_index("gy"), 2) == 0
    below, above = sides(lax.axis_index("gx"), rows_a_ref, rows_b_ref)
    fields = (g_ref[...], below[0], above[0], s_ref[...], below[1], above[1])
    left = fold(sizes, jnp.concatenate([x[:, :128] for x in fields], axis=0), HALO)
    right = fold(sizes, jnp.concatenate([x[:, last:] for x in fields], axis=0), -HALO)
    first_ref[...] = jnp.where(even, right, left)
    second_ref[...] = jnp.where(even, left, right)


def coefficients(sizes, level, gx, gy, sigma):
    d = 4.0 + sigma
    return d, jnp.where(inside_mask(sizes, level, gx, gy), DAMPING / d, 0.0)


def down_kernel(sizes, g_ref, s_ref, rows_a_ref, rows_b_ref, columns_a_ref, columns_b_ref,
                rc0_ref, rc1_ref, pc_ref,
                g0_ref, d0_ref, w0_ref, v0_ref, c1_ref, d1_ref, w1_ref, v1_ref, d2_ref, w2_ref, out_ref, scratch):
    gx, gy = lax.axis_index("gx"), lax.axis_index("gy")
    rows = sizes.ext_rows[0]
    lane = iota((rows, 128), 1)
    below, above = sides(gx, rows_a_ref, rows_b_ref)
    from_right, from_left = sides(gy, columns_a_ref, columns_b_ref)
    from_right, from_left = unfold(sizes, from_right, HALO), unfold(sizes, from_left, -HALO)
    g = jnp.where(lane < HALO, from_right[0], from_left[0])
    sigma = jnp.where(lane < HALO, from_right[1], from_left[1])
    g = jnp.concatenate([jnp.concatenate([g_ref[...], below[0], above[0]], axis=0), g], axis=1)
    sigma = jnp.concatenate([jnp.concatenate([s_ref[...], below[1], above[1]], axis=0), sigma], axis=1)
    d, w = coefficients(sizes, 0, gx, gy, sigma)
    v = w * g
    v = sweep(v, g, w)
    r = g - d * v + around(v)
    for ref, values in ((g0_ref, g), (d0_ref, d), (w0_ref, w), (v0_ref, v)):
        ref[...] = near(values, sizes.rows)
    both = []
    own, halo = sizes.rows // 2, HALOS[1]
    for values in (r, sigma):
        pairs = pair_rows(scratch, values)
        both += [pairs[: own + halo], pairs[pairs.shape[0] - halo :]]
    both = f32dot_right(jnp.concatenate(both, axis=0), rc0_ref[...])
    half = own + 2 * halo
    g, sigma = both[:half], both[half:]
    d, w = coefficients(sizes, 1, gx, gy, sigma)
    v = w * g
    v = sweep(v, g, w)
    r = g - d * v + around(v)
    c1_ref[...] = g
    d1_ref[...] = d
    w1_ref[...] = w
    v1_ref[...] = v
    half = half // 2
    both = jnp.concatenate([pair_rows(scratch, r), pair_rows(scratch, sigma)], axis=0)
    both = f32dot_right(both, rc1_ref[...])
    g, sigma = both[:half], both[half:]
    d, w = coefficients(sizes, 2, gx, gy, sigma)
    d2_ref[...] = d
    w2_ref[...] = w
    own = sizes.rows // 4
    pack_two(sizes, gy, g[:own], sigma[:own], scratch, pc_ref, out_ref)


class Coarse:
    def __init__(self, sizes, first, d_refs, w_refs, g_refs, v_refs, t_refs, coarsest):
        self.z = sizes
        self.first = first
        self.d, self.w, self.g, self.v, self.t = d_refs, w_refs, g_refs, v_refs, t_refs
        self.va, self.vb, self.wk, self.gk = coarsest
        lane = iota((sizes.p, sizes.coarse_columns), 1)
        self.first_lane, self.last_lane = lane == 0, lane == sizes.coarse_columns - 1

    def blocks(self, body):
        p = self.z.p
        if self.z.nx <= 4:
            for gx in range(self.z.nx):
                body((gx + 1) * p)
        else:
            def step(gx, carry):
                body(pl.multiple_of((gx + 1) * p, 8))
                return carry

            lax.fori_loop(0, self.z.nx, step, 0)

    def at(self, ref, s, r, base):
        return ref[s, r, pl.ds(base, self.z.p), :]

    def put(self, ref, s, r, base, value):
        ref[s, r, pl.ds(base, self.z.p), :] = value

    def beside(self, ref, s, r, base, step):
        p = self.z.p
        if isinstance(base, int):
            return ref[s, r, pl.ds(base + step, p), :]
        return ref[s, r, pl.ds(base - p, 3 * p), :][p + step : 2 * p + step]

    def neighbours(self, ref, s, r, n, base):
        columns = self.z.coarse_columns
        if r < n - 1:
            right = self.at(ref, s, r + 1, base)
        else:
            right = jnp.where(self.last_lane, 0.0, pltpu.roll(self.at(ref, s, 0, base), columns - 1, 1))
        if r > 0:
            left = self.at(ref, s, r - 1, base)
        else:
            left = jnp.where(self.first_lane, 0.0, pltpu.roll(self.at(ref, s, n - 1, base), 1, 1))
        down = self.at(ref, s + 1, r, base) if s < n - 1 else self.beside(ref, 0, r, base, 1)
        up = self.at(ref, s - 1, r, base) if s > 0 else self.beside(ref, n - 1, r, base, -1)
        return (up + down) + (left + right)

    def each(self, level, body):
        n = 1 << (LEVELS - level)

        def block(base):
            for s in range(n):
                for r in range(n):
                    body(s, r, n, base)

        self.blocks(block)

    def first_sweep(self, level):
        l = level - self.first

        def body(s, r, n, base):
            self.put(self.v[l], s, r, base, self.at(self.w[l], s, r, base) * self.at(self.g[l], s, r, base))

        self.each(level, body)

    def sweep(self, level, source, target):
        l = level - self.first

        def body(s, r, n, base):
            v = self.at(source, s, r, base)
            total = self.at(self.g[l], s, r, base) + self.neighbours(source, s, r, n, base)
            self.put(target, s, r, base, (1.0 - DAMPING) * v + self.at(self.w[l], s, r, base) * total)

        self.each(level, body)

    def two_sweeps(self, level):
        l = level - self.first
        self.sweep(level, self.v[l], self.t[l])
        self.sweep(level, self.t[l], self.v[l])

    def start(self, level):
        l = level - self.first
        self.first_sweep(level)
        self.sweep(level, self.v[l], self.t[l])
        self.v[l], self.t[l] = self.t[l], self.v[l]

    def residual(self, level, s, r, n, base):
        l = level - self.first
        v = self.at(self.v[l], s, r, base)
        g = self.at(self.g[l], s, r, base)
        return (g - self.at(self.d[l], s, r, base) * v) + self.neighbours(self.v[l], s, r, n, base)

    def restrict(self, level):
        l = level - self.first
        n = 1 << (LEVELS - level)

        def block(base):
            for s in range(n // 2):
                for r in range(n // 2):
                    parts = [self.residual(level, 2 * s + a, 2 * r + b, n, base) for a in (0, 1) for b in (0, 1)]
                    self.put(self.g[l + 1], s, r, base, (parts[0] + parts[1]) + (parts[2] + parts[3]))

        self.blocks(block)

    def prolong(self, level):
        l = level - self.first

        def body(s, r, n, base):
            e = self.at(self.v[l + 1], s // 2, r // 2, base)
            self.put(self.v[l], s, r, base, self.at(self.v[l], s, r, base) + e)

        self.each(level, body)

    def inner(self, ref):
        p = self.z.p
        return ref[0, 0, p : p + self.z.coarse_rows, :]

    def shifted(self, x, k):
        if k == 0:
            return x
        columns = self.z.coarse_columns
        lane = iota(x.shape, 1)
        keep = lane < columns - k if k > 0 else lane >= -k
        return jnp.where(keep, pltpu.roll(x, -k % columns, 1), 0.0)

    def unit(self):
        z = self.z
        top = LEVELS - self.first
        d, w = self.inner(self.d[top]), self.inner(self.w[top])
        missing = 2.0 * (z.coarse_rows + z.coarse_columns)
        for k in range(-2, 3):
            self.wk[k + 2] = self.shifted(w, k)
        return 1.0 / (jnp.sum(d - 4.0, keepdims=True) + missing)

    def coarse(self, fresh, unit):
        top = LEVELS - self.first
        p, height = self.z.p, self.z.coarse_rows
        g = self.inner(self.g[top])
        for k in range(-2, 3):
            self.gk[k + 2] = self.shifted(g, k)
        lane = iota(g.shape, 1)

        def at(ref, k, step=0):
            return ref[k + 3, p + step : p + step + height, :]

        def put(ref, k, value):
            ref[k + 3, p : p + height, :] = value

        if fresh:
            left = jnp.broadcast_to(jnp.sum(g, keepdims=True) * unit, g.shape)
            v = {k: 0.0 for k in range(-3, 4)}
        else:
            v = self.inner(self.v[top])
            v = {k: self.shifted(v, k) for k in range(-3, 4)}
            put(self.va, 0, v[0])
            around_v = (at(self.va, 0, -1) + at(self.va, 0, 1)) + (v[-1] + v[1])
            left = jnp.sum((g - self.inner(self.d[top]) * v[0]) + around_v, keepdims=True) * unit
            left = jnp.broadcast_to(left, g.shape)
        for k in range(-3, 4):
            inside = (lane < g.shape[1] - k) & (lane >= -k)
            put(self.va, k, v[k] + jnp.where(inside, left, 0.0) if k else v[k] + left)
        for turn in range(COARSE_SWEEPS // 3):
            if turn:
                v = self.inner(self.v[top])
                for k in range(-3, 4):
                    put(self.va, k, self.shifted(v, k))
            source, target = self.va, self.vb
            for reach in (2, 1, 0):
                for k in range(-reach, reach + 1):
                    total = self.gk[k + 2] + (at(source, k, -1) + at(source, k, 1))
                    total = total + (at(source, k - 1) + at(source, k + 1))
                    value = (1.0 - DAMPING) * at(source, k) + self.wk[k + 2] * total
                    if reach:
                        put(target, k, value)
                    else:
                        self.v[top][0, 0, p : p + height, :] = value
                source, target = target, source

    def vcycle(self, level, fresh, unit):
        if level == LEVELS:
            self.coarse(fresh, unit)
            return
        if fresh:
            self.start(level)
        else:
            self.two_sweeps(level)
        self.restrict(level)
        self.vcycle(level + 1, True, unit)
        self.prolong(level)
        self.two_sweeps(level)

    def fcycle(self, level, unit):
        if level == LEVELS:
            self.coarse(True, unit)
            return
        self.start(level)
        self.restrict(level)
        self.fcycle(level + 1, unit)
        self.vcycle(level + 1, False, unit)
        self.prolong(level)
        self.two_sweeps(level)

    def clear_ends(self):
        z = self.z
        zero = jnp.zeros((z.p, z.coarse_columns), jnp.float32)
        for refs in (self.v, self.t):
            for ref in refs:
                n = ref.shape[0]
                for s in range(n):
                    for r in range(n):
                        ref[s, r, : z.p, :] = zero
                        ref[s, r, z.p + z.coarse_rows :, :] = zero
        for ref in (self.va, self.vb):
            for k in range(7):
                ref[k, : z.p, :] = zero
                ref[k, z.p + z.coarse_rows :, :] = zero

    def turned(self, blocks, k):
        q = self.z.q
        part = iota(blocks[0].shape, 1) // q
        out = blocks[-k % 8]
        for x in range(1, 8):
            out = jnp.where(part == x, blocks[(x - k) % 8], out)
        return pltpu.roll(out, -k * q % 128, 1) if k else out

    def take_two(self, even_ref, odd_ref, targets):
        z = self.z
        for gx in range(z.nx):
            for group in range(z.ny // 8):
                lanes = slice(group * 128, (group + 1) * 128)
                for s in range(4):
                    blocks = []
                    for g in range(8):
                        first = (gx * (z.ny // 2) + group * 4 + g // 2) * 4 * z.p + s * z.p
                        blocks.append((even_ref, odd_ref)[g % 2][first : first + z.p, :])
                    for k in range(8):
                        target, add = targets[k // 4]
                        value = self.turned(blocks, k)
                        target[s, k % 4, (gx + 1) * z.p : (gx + 2) * z.p, lanes] = value + add if add else value

    def take_one(self, y_ref, target):
        z = self.z
        low = iota((8, 128), 0) < 4
        for gx in range(z.nx):
            for group in range(z.ny // 8):
                upper, lower = [], []
                for g in range(0, 8, 2):
                    first = (gx * z.ny + group * 8 + g) * 4
                    pair = y_ref[first : first + 8, :]
                    swapped = pltpu.roll(pair, 4, 0)
                    upper += [pair, swapped]
                    lower += [swapped, pair]
                for k in range(4):
                    value = jnp.where(low, self.turned(upper, k), self.turned(lower, k + 4))
                    target[k // 2, k % 2, (gx + 1) * z.p : (gx + 2) * z.p, group * 128 : (group + 1) * 128] = value

    def spread(self, gx, gy, columns_ref, scratch, lines):
        z = self.z
        n = 1 << (LEVELS - self.first)
        above = self.first - 1
        columns = z.coarse_columns
        turn = lax.rem(columns + z.q - gy * z.q, columns)
        start = pl.multiple_of(gx * z.p, 8)
        for s in range(n):
            for r in range(n):
                part = pltpu.roll(self.v[0][s, r, pl.ds(start, 3 * z.p), :], turn, 1)[:, :128]
                lines[r, pl.ds(s, 3 * z.p, stride=n), :] = part
        own, halo = z.rows >> self.first, HALOS[above]
        window = slice(n * z.p - 8, n * z.p + own + 8)
        wide = f32dot_right(jnp.concatenate([lines[r, window, :] for r in range(n)], axis=1), columns_ref[...])
        doubled = double_rows(scratch, jnp.concatenate([wide[8:], wide[:8]], axis=0))
        height = doubled.shape[0]
        return jnp.concatenate([doubled[: 2 * own + halo], doubled[height - halo :]], axis=0)


def level_shape(sizes, level):
    n = 1 << (LEVELS - level)
    return (n, n, sizes.coarse_rows + 2 * sizes.p, sizes.coarse_columns)


def middle_kernel(sizes, y_ref, other_ref, c1_ref, d1_ref, w1_ref, v1_ref, w2l_ref, d2l_ref, sc_ref,
                  rc1_ref, pc_ref,
                  d3_ref, d4_ref, w3_ref, w4_ref, e1_ref, c2_ref, e2_ref, out_ref,
                  d2, w2, g2, g3, g4, v2, v3, v4, t2, t3, t4, scratch, lines, *coarsest):
    gx, gy = lax.axis_index("gx"), lax.axis_index("gy")
    m = Coarse(sizes, 2, [d2, d3_ref, d4_ref], [w2, w3_ref, w4_ref], [g2, g3, g4], [v2, v3, v4], [t2, t3, t4], coarsest)
    m.clear_ends()
    core = lax.rem(gy, 2)

    @pl.when(core == 0)
    def _():
        m.take_two(y_ref, other_ref, ((g2, 0.0), (d2, 4.0)))

    @pl.when(core == 1)
    def _():
        m.take_two(other_ref, y_ref, ((g2, 0.0), (d2, 4.0)))

    for l in range(2):
        n = 2 >> l

        def block(base):
            for s in range(n):
                for r in range(n):
                    parts = [m.at(m.d[l], 2 * s + a, 2 * r + b, base) for a in (0, 1) for b in (0, 1)]
                    m.put(m.d[l + 1], s, r, base, ((parts[0] + parts[1]) + (parts[2] + parts[3])) - 12.0)

        m.blocks(block)
    for l in range(3):
        def body(s, r, n, base):
            m.put(m.w[l], s, r, base, DAMPING / m.at(m.d[l], s, r, base))

        m.each(l + 2, body)
    unit = m.unit()
    m.fcycle(2, unit)
    m.vcycle(2, False, unit)
    g, d, w = c1_ref[...], d1_ref[...], w1_ref[...]
    v = v1_ref[...] + jnp.where(w > 0.0, m.spread(gx, gy, sc_ref, scratch, lines), 0.0)
    for turn in range(4):
        v = sweep(v, g, w)
    e1_ref[...] = v
    r = g - d * v + around(v)
    g = f32dot_right(pair_rows(scratch, r), rc1_ref[...])
    d, w = d2l_ref[...], w2l_ref[...]
    v = w * g
    v = sweep(v, g, w)
    r = g - d * v + around(v)
    c2_ref[...] = g
    e2_ref[...] = v
    pack_one(sizes, gy, pair_rows(scratch, r[: sizes.rows // 4]), scratch, pc_ref, out_ref)


def up_kernel(sizes, y_ref, d3_ref, d4_ref, w3_ref, w4_ref, c2_ref, w2_ref, e2_ref, c1_ref, w1_ref, e1_ref,
              g0_ref, d0_ref, w0_ref, v0_ref, sc_ref, pc1_ref, pc0_ref,
              solution_ref, residual_ref, g3, g4, v3, v4, t3, t4, scratch, lines, *coarsest):
    gx, gy = lax.axis_index("gx"), lax.axis_index("gy")
    m = Coarse(sizes, 3, [d3_ref, d4_ref], [w3_ref, w4_ref], [g3, g4], [v3, v4], [t3, t4], coarsest)
    m.clear_ends()
    m.take_one(y_ref, g3)
    m.vcycle(3, True, m.unit())
    g, w = c2_ref[...], w2_ref[...]
    v = e2_ref[...] + jnp.where(w > 0.0, m.spread(gx, gy, sc_ref, scratch, lines), 0.0)
    for turn in range(2):
        v = sweep(v, g, w)
    own = sizes.rows // 2
    g, w = near(c1_ref, own), near(w1_ref, own)
    v = near(e1_ref, own) + near(double_rows(scratch, f32dot_right(v, pc1_ref[...])), own)
    for turn in range(2):
        v = sweep(v, g, w)
    g, d, w = g0_ref[...], d0_ref[...], w0_ref[...]
    v = v0_ref[...] + near(double_rows(scratch, f32dot_right(v, pc0_ref[...])), sizes.rows)
    for turn in range(2):
        v = sweep(v, g, w)
    r = g - d * v + around(v)
    solution_ref[...] = v[: sizes.rows, : sizes.columns]
    residual_ref[...] = r[: sizes.rows, : sizes.columns]


def vmem(count):
    return [pl.BlockSpec(memory_space=pltpu.VMEM)] * count


def call(kernel, sizes, outs, scratch, *operands, inputs=None, semaphores=()):
    shapes = [jax.ShapeDtypeStruct(shape, jnp.float32) for shape in outs]
    used = sum(4 * int(np.prod(shape)) for shape in list(outs) + list(scratch))
    used += sum(x.size * x.dtype.itemsize for x in operands)
    return pl.pallas_call(
        lambda *refs: kernel(sizes, *refs),
        name=kernel.__name__,
        out_shape=shapes,
        in_specs=vmem(len(operands)) if inputs is None else inputs,
        out_specs=vmem(len(outs)),
        scratch_shapes=[pltpu.VMEM(shape, jnp.float32) for shape in scratch] + list(semaphores),
        compiler_params=pltpu.CompilerParams(vmem_limit_bytes=used + used // 4 + (4 << 20)),
    )(*operands)


def swaps(first, second, axis, spare):
    nx, ny = lax.axis_size("gx"), lax.axis_size("gy")
    count = lax.axis_size(axis)

    def target(gx, gy):
        place = gx if axis == "gx" else gy
        if place in (0, count - 1):
            return (gx ^ 1) * ny + gy if spare == "gx" else gx * ny + (gy ^ 1)
        place = place + 1 if place % 2 else place - 1
        return place * ny + gy if axis == "gx" else gx * ny + place

    pairs = [(gx * ny + gy, target(gx, gy)) for gx in range(nx) for gy in range(ny)]
    return lax.ppermute(first, axis, [(i, i ^ 1) for i in range(count)]), lax.ppermute(second, ("gx", "gy"), pairs)


def gather(copies):
    return lax.all_to_all(copies, ("gx", "gy"), 0, 0, tiled=True)


def gather_by_core(copies, nx, ny):
    index = np.arange(nx * ny)
    groups = [index[core::2].tolist() for core in range(2)]
    own = lax.all_to_all(copies, ("gx", "gy"), 0, 0, tiled=True, axis_index_groups=groups)
    return own, lax.ppermute(own, "gy", [(j, j ^ 1) for j in range(ny)])


def body(right_side, shift):
    nx, ny = lax.axis_size("gx"), lax.axis_size("gy")
    rows, columns = right_side.shape
    z = Sizes(rows, columns, nx, ny)
    first, second = call(
        rows_kernel, z, [(2, HALO, columns)] * 2, [], right_side, shift,
        inputs=[pl.BlockSpec(memory_space=pltpu.HBM)] * 2, semaphores=[pltpu.SemaphoreType.DMA((4,))])
    rows_a, rows_b = swaps(first, second, "gx", "gy")
    ext = [(z.ext_rows[l], z.ext_columns[l]) for l in range(3)]
    strip = (strip_rows(z)[1], 128)
    first, second = call(strip_kernel, z, [strip] * 2, [], right_side, shift, rows_a, rows_b)
    columns_a, columns_b = swaps(first, second, "gy", "gx")
    rc0, rc1 = z.restrict_columns(0), z.restrict_columns(1)
    tiles = (ext[0][1] // 128, ext[0][0], 128)
    g0, d0, w0, v0, c1, d1, w1, v1, d2, w2, packed = call(
        down_kernel, z, [(rows + 2 * NEAR, ext[0][1])] * 4 + [ext[1]] * 4 + [ext[2]] * 2 + [(nx * ny // 2 * 4 * z.p, 128)], [tiles],
        right_side, shift, rows_a, rows_b, columns_a, columns_b, rc0, rc1, z.pack_pair())
    y, other = gather_by_core(packed, nx, ny)
    slabs = [level_shape(z, level) for level in (2, 3, 4)]
    coarsest = [(7,) + slabs[2][2:]] * 2 + [(5, z.coarse_rows, z.coarse_columns)] * 2
    d3, d4, w3, w4, e1, c2, e2, packed = call(
        middle_kernel, z, slabs[1:] * 2 + [ext[1], ext[2], ext[2], (nx * ny * 4, 128)],
        [slabs[0]] * 2 + slabs * 3 + [tiles, (4, 12 * z.p, 128)] + coarsest,
        y, other, c1, d1, w1, v1, w2, d2, z.spread_columns(2),
        rc1, z.pack_single())
    y = gather(packed)
    return call(
        up_kernel, z, [(rows, columns)] * 2, slabs[1:] * 3 + [tiles, (2, 6 * z.p, 128)] + coarsest,
        y, d3, d4, w3, w4, c2, w2, e2, c1, w1, e1, g0, d0, w0, v0,
        z.spread_columns(3), rc1.T, rc0.T)


def solution(mesh):
    specs = (P("gx", "gy"), P("gx", "gy"))

    def run(right_side, shift):
        out = body(right_side, shift)
        return out[0], out[1]

    return jax.shard_map(run, mesh=mesh, in_specs=specs, out_specs=specs, check_vma=False)
```

```python
import numpy as np
import jax
import jax.numpy as jnp
from jax import lax
from jax.experimental import pallas as pl
from jax.experimental.pallas import tpu as pltpu
from jax.sharding import PartitionSpec as P

LEVELS = 4
COARSE_SWEEPS = 6
DAMPING = 0.8
HALOS = (40, 16, 8)
HALO = HALOS[0]
NEAR = 8


def f32dot_right(values, onehot):
    high = values.astype(jnp.bfloat16)
    rest = values - high.astype(jnp.float32)
    middle = rest.astype(jnp.bfloat16)
    low = (rest - middle.astype(jnp.float32)).astype(jnp.bfloat16)
    rows = values.shape[0]
    stacked = jnp.concatenate([high, middle, low], axis=0)
    out = jnp.dot(stacked, onehot, preferred_element_type=jnp.float32)
    return (out[2 * rows :] + out[rows : 2 * rows]) + out[:rows]


def around(v):
    rows, columns = v.shape
    up = pltpu.roll(v, 1, 0)
    down = pltpu.roll(v, rows - 1, 0)
    left = pltpu.roll(v, 1, 1)
    right = pltpu.roll(v, columns - 1, 1)
    return (up + down) + (left + right)


def sweep(v, g, w):
    return (1.0 - DAMPING) * v + w * (g + around(v))


class Sizes:
    def __init__(self, rows, columns, nx, ny):
        self.rows, self.columns, self.nx, self.ny = rows, columns, nx, ny
        self.p, self.q = rows // 16, columns // 16
        self.coarse_rows, self.coarse_columns = nx * self.p, ny * self.q
        assert self.p == 8 and 8 * self.q == 128, "block shape"

        def up(n):
            return -(-n // 128) * 128

        self.ext_rows = [(rows >> l) + 2 * HALOS[l] for l in range(3)]
        self.ext_columns = [up((columns >> l) + 2 * HALOS[l]) for l in range(3)]

    def column_at(self, level):
        own, halo, width = self.columns >> level, HALOS[level], self.ext_columns[level]
        lane = np.arange(width)
        inside = (lane < own + halo) | (lane >= width - halo)
        return np.where(lane < own + halo, lane, lane - width), inside

    def restrict_columns(self, level):
        fine, fine_in = self.column_at(level)
        coarse, coarse_in = self.column_at(level + 1)
        hit = (fine[:, None] // 2 == coarse[None, :]) & fine_in[:, None] & coarse_in[None, :]
        return hit.astype(jnp.bfloat16)

    def pack_pair(self):
        own = self.columns >> 2
        x = np.arange(2 * own)
        target = (x // own) * own + (x % own % 4) * self.q + x % own // 4
        return (target[:, None] == np.arange(2 * own)[None, :]).astype(jnp.bfloat16)

    def pack_single(self):
        x = np.arange(self.ext_columns[2])[:, None]
        lane = np.arange(128)[None, :]
        hit = (x // 2 == 2 * (lane % self.q) + (lane // self.q) % 2) & (x < self.columns >> 2)
        return hit.astype(jnp.bfloat16)

    def spread_columns(self, level):
        n = 1 << (LEVELS - level)
        column, inside = self.column_at(level - 1)
        m = column // 2
        r = np.arange(n)[:, None, None]
        lane = np.arange(128)[None, :, None]
        hit = (m % n == r) & (m // n + self.q == lane) & inside
        return hit.reshape(n * 128, -1).astype(jnp.bfloat16)


def iota(shape, axis):
    return lax.broadcasted_iota(jnp.int32, shape, axis)


def inside_mask(sizes, level, gx, gy):
    shape = (sizes.ext_rows[level], sizes.ext_columns[level])
    own_r, own_c, halo = sizes.rows >> level, sizes.columns >> level, HALOS[level]
    row, column = iota(shape, 0), iota(shape, 1)
    last_row = jnp.where(gx < sizes.nx - 1, own_r + halo, own_r)
    first_row = jnp.where(gx > 0, own_r + halo, shape[0])
    last_column = jnp.where(gy < sizes.ny - 1, own_c + halo, own_c)
    first_column = jnp.where(gy > 0, shape[1] - halo, shape[1])
    return ((row < last_row) | (row >= first_row)) & ((column < last_column) | (column >= first_column))


def pair_rows(scratch, values):
    rows, columns = values.shape
    outs = []
    for t in range(columns // 128):
        scratch[t, :rows, :] = values[:, t * 128 : (t + 1) * 128]
    for t in range(columns // 128):
        outs.append(scratch[t, pl.ds(0, rows // 2, stride=2), :] + scratch[t, pl.ds(1, rows // 2, stride=2), :])
    return jnp.concatenate(outs, axis=1)


def double_rows(scratch, values):
    rows, columns = values.shape
    for t in range(columns // 128):
        part = values[:, t * 128 : (t + 1) * 128]
        scratch[t, pl.ds(0, rows, stride=2), :] = part
        scratch[t, pl.ds(1, rows, stride=2), :] = part
    return jnp.concatenate([scratch[t, : 2 * rows, :] for t in range(columns // 128)], axis=1)


def repeat(block, out_ref):
    height = block.shape[0]
    for k in range(out_ref.shape[0] // height):
        out_ref[k * height : (k + 1) * height, :] = block


def pack_two(sizes, gy, first, second, scratch, columns_ref, out_ref):
    own = sizes.columns >> 2
    both = jnp.where(iota(first.shape, 1) < own, first, pltpu.roll(second, own, 1))
    rows = both.shape[0]
    scratch[0, :rows, :] = f32dot_right(both, columns_ref[...])
    block = jnp.concatenate([scratch[0, pl.ds(s, sizes.p, stride=4), :] for s in range(4)], axis=0)
    repeat(pltpu.roll(block, lax.rem(gy, 8) * sizes.q, 1), out_ref)


def pack_one(sizes, gy, values, scratch, columns_ref, out_ref):
    rows = values.shape[0]
    scratch[0, :rows, :] = f32dot_right(values, columns_ref[...])
    part = iota((4, 128), 1) // (2 * sizes.q)
    block = scratch[0, pl.ds(0, 4, stride=2), :]
    for k in range(1, 4):
        block = jnp.where(part == k, scratch[0, pl.ds(8 * (k // 2) + k % 2, 4, stride=2), :], block)
    block = jnp.concatenate([block, block], axis=0)
    repeat(pltpu.roll(block, lax.rem(gy, 8) * sizes.q, 1), out_ref)


def near(values, own):
    return jnp.concatenate([values[: own + NEAR], values[values.shape[0] - NEAR :]], axis=0)


def sides(at, first_ref, second_ref):
    even = lax.rem(at, 2) == 0
    first, second = first_ref[...], second_ref[...]
    return jnp.where(even, first, second), jnp.where(even, second, first)


def strip_rows(sizes):
    groups = 128 // HALO
    return groups, -(-2 * sizes.ext_rows[0] // (8 * groups)) * 8


def fold(sizes, strip, step):
    groups, height = strip_rows(sizes)
    lane = iota((height, 128), 1)
    lane = lane if step > 0 else 127 - lane
    out = strip[:height]
    for k in range(1, groups):
        part = strip[k * height : (k + 1) * height]
        part = pltpu.roll(part, k * step % 128, 1)
        if part.shape[0] < height:
            part = jnp.concatenate([part, jnp.zeros((height - part.shape[0], 128), jnp.float32)], axis=0)
        out = jnp.where(lane >= k * HALO, part, out)
    return out


def unfold(sizes, packed, step):
    groups, _ = strip_rows(sizes)
    parts = [packed] + [pltpu.roll(packed, -k * step % 128, 1) for k in range(1, groups)]
    rows = sizes.ext_rows[0]
    out = jnp.concatenate(parts, axis=0)
    return out[:rows], out[rows : 2 * rows]


def strip_kernel(sizes, g_ref, s_ref, rows_a_ref, rows_b_ref, first_ref, second_ref):
    last = sizes.columns - 128
    even = lax.rem(lax.axis_index("gy"), 2) == 0
    below, above = sides(lax.axis_index("gx"), rows_a_ref, rows_b_ref)
    fields = (g_ref[...], below[0], above[0], s_ref[...], below[1], above[1])
    left = fold(sizes, jnp.concatenate([x[:, :128] for x in fields], axis=0), HALO)
    right = fold(sizes, jnp.concatenate([x[:, last:] for x in fields], axis=0), -HALO)
    first_ref[...] = jnp.where(even, right, left)
    second_ref[...] = jnp.where(even, left, right)


def coefficients(sizes, level, gx, gy, sigma):
    d = 4.0 + sigma
    return d, jnp.where(inside_mask(sizes, level, gx, gy), DAMPING / d, 0.0)


def down_kernel(sizes, g_ref, s_ref, rows_a_ref, rows_b_ref, columns_a_ref, columns_b_ref,
                rc0_ref, rc1_ref, pc_ref,
                g0_ref, d0_ref, w0_ref, v0_ref, c1_ref, d1_ref, w1_ref, v1_ref, d2_ref, w2_ref, out_ref, scratch):
    gx, gy = lax.axis_index("gx"), lax.axis_index("gy")
    rows = sizes.ext_rows[0]
    lane = iota((rows, 128), 1)
    below, above = sides(gx, rows_a_ref, rows_b_ref)
    from_right, from_left = sides(gy, columns_a_ref, columns_b_ref)
    from_right, from_left = unfold(sizes, from_right, HALO), unfold(sizes, from_left, -HALO)
    g = jnp.where(lane < HALO, from_right[0], from_left[0])
    sigma = jnp.where(lane < HALO, from_right[1], from_left[1])
    g = jnp.concatenate([jnp.concatenate([g_ref[...], below[0], above[0]], axis=0), g], axis=1)
    sigma = jnp.concatenate([jnp.concatenate([s_ref[...], below[1], above[1]], axis=0), sigma], axis=1)
    d, w = coefficients(sizes, 0, gx, gy, sigma)
    v = w * g
    v = sweep(v, g, w)
    r = g - d * v + around(v)
    for ref, values in ((g0_ref, g), (d0_ref, d), (w0_ref, w), (v0_ref, v)):
        ref[...] = near(values, sizes.rows)
    both = []
    own, halo = sizes.rows // 2, HALOS[1]
    for values in (r, sigma):
        pairs = pair_rows(scratch, values)
        both += [pairs[: own + halo], pairs[pairs.shape[0] - halo :]]
    both = f32dot_right(jnp.concatenate(both, axis=0), rc0_ref[...])
    half = own + 2 * halo
    g, sigma = both[:half], both[half:]
    d, w = coefficients(sizes, 1, gx, gy, sigma)
    v = w * g
    v = sweep(v, g, w)
    r = g - d * v + around(v)
    c1_ref[...] = g
    d1_ref[...] = d
    w1_ref[...] = w
    v1_ref[...] = v
    half = half // 2
    both = jnp.concatenate([pair_rows(scratch, r), pair_rows(scratch, sigma)], axis=0)
    both = f32dot_right(both, rc1_ref[...])
    g, sigma = both[:half], both[half:]
    d, w = coefficients(sizes, 2, gx, gy, sigma)
    d2_ref[...] = d
    w2_ref[...] = w
    own = sizes.rows // 4
    pack_two(sizes, gy, g[:own], sigma[:own], scratch, pc_ref, out_ref)


class Coarse:
    def __init__(self, sizes, first, d_refs, w_refs, g_refs, v_refs, t_refs, coarsest):
        self.z = sizes
        self.first = first
        self.d, self.w, self.g, self.v, self.t = d_refs, w_refs, g_refs, v_refs, t_refs
        self.va, self.vb, self.wk, self.gk, self.wide_v, self.wide_t, self.wide_w, self.wide_g = coarsest
        lane = iota((sizes.p, sizes.coarse_columns), 1)
        self.first_lane, self.last_lane = lane == 0, lane == sizes.coarse_columns - 1

    def blocks(self, body):
        p = self.z.p
        if self.z.nx <= 4:
            for gx in range(self.z.nx):
                body((gx + 1) * p)
        else:
            def step(gx, carry):
                body(pl.multiple_of((gx + 1) * p, 8))
                return carry

            lax.fori_loop(0, self.z.nx, step, 0)

    def at(self, ref, s, r, base):
        return ref[s, r, pl.ds(base, self.z.p), :]

    def put(self, ref, s, r, base, value):
        ref[s, r, pl.ds(base, self.z.p), :] = value

    def beside(self, ref, s, r, base, step):
        p = self.z.p
        if isinstance(base, int):
            return ref[s, r, pl.ds(base + step, p), :]
        return ref[s, r, pl.ds(base - p, 3 * p), :][p + step : 2 * p + step]

    def neighbours(self, ref, s, r, n, base):
        columns = self.z.coarse_columns
        if r < n - 1:
            right = self.at(ref, s, r + 1, base)
        else:
            right = jnp.where(self.last_lane, 0.0, pltpu.roll(self.at(ref, s, 0, base), columns - 1, 1))
        if r > 0:
            left = self.at(ref, s, r - 1, base)
        else:
            left = jnp.where(self.first_lane, 0.0, pltpu.roll(self.at(ref, s, n - 1, base), 1, 1))
        down = self.at(ref, s + 1, r, base) if s < n - 1 else self.beside(ref, 0, r, base, 1)
        up = self.at(ref, s - 1, r, base) if s > 0 else self.beside(ref, n - 1, r, base, -1)
        return (up + down) + (left + right)

    def each(self, level, body):
        n = 1 << (LEVELS - level)

        def block(base):
            for s in range(n):
                for r in range(n):
                    body(s, r, n, base)

        self.blocks(block)

    def first_sweep(self, level):
        l = level - self.first

        def body(s, r, n, base):
            self.put(self.v[l], s, r, base, self.at(self.w[l], s, r, base) * self.at(self.g[l], s, r, base))

        self.each(level, body)

    def sweep(self, level, source, target):
        l = level - self.first

        def body(s, r, n, base):
            v = self.at(source, s, r, base)
            total = self.at(self.g[l], s, r, base) + self.neighbours(source, s, r, n, base)
            self.put(target, s, r, base, (1.0 - DAMPING) * v + self.at(self.w[l], s, r, base) * total)

        self.each(level, body)

    def two_sweeps(self, level):
        l = level - self.first
        self.sweep(level, self.v[l], self.t[l])
        self.sweep(level, self.t[l], self.v[l])

    def start(self, level):
        l = level - self.first
        self.first_sweep(level)
        self.sweep(level, self.v[l], self.t[l])
        self.v[l], self.t[l] = self.t[l], self.v[l]

    def residual(self, level, s, r, n, base):
        l = level - self.first
        v = self.at(self.v[l], s, r, base)
        g = self.at(self.g[l], s, r, base)
        return (g - self.at(self.d[l], s, r, base) * v) + self.neighbours(self.v[l], s, r, n, base)

    def restrict(self, level):
        l = level - self.first
        n = 1 << (LEVELS - level)

        def block(base):
            for s in range(n // 2):
                for r in range(n // 2):
                    parts = [self.residual(level, 2 * s + a, 2 * r + b, n, base) for a in (0, 1) for b in (0, 1)]
                    self.put(self.g[l + 1], s, r, base, (parts[0] + parts[1]) + (parts[2] + parts[3]))

        self.blocks(block)

    def prolong(self, level):
        l = level - self.first

        def body(s, r, n, base):
            e = self.at(self.v[l + 1], s // 2, r // 2, base)
            self.put(self.v[l], s, r, base, self.at(self.v[l], s, r, base) + e)

        self.each(level, body)

    def inner(self, ref, s=0, r=0):
        p = self.z.p
        return ref[s, r, p : p + self.z.coarse_rows, :]

    def shifted(self, x, k):
        if k == 0:
            return x
        columns = self.z.coarse_columns
        lane = iota(x.shape, 1)
        keep = lane < columns - k if k > 0 else lane >= -k
        return jnp.where(keep, pltpu.roll(x, -k % columns, 1), 0.0)

    def unit(self):
        z = self.z
        top = LEVELS - self.first
        d, w = self.inner(self.d[top]), self.inner(self.w[top])
        missing = 2.0 * (z.coarse_rows + z.coarse_columns)
        for k in range(-2, 3):
            self.wk[k + 2] = self.shifted(w, k)
        self.widen(self.w[top - 1], self.wide_w, 1, False)
        return 1.0 / (jnp.sum(d - 4.0, keepdims=True) + missing)

    def coarse(self, fresh, unit):
        top = LEVELS - self.first
        p, height = self.z.p, self.z.coarse_rows
        g = self.inner(self.g[top])
        for k in range(-2, 3):
            self.gk[k + 2] = self.shifted(g, k)
        lane = iota(g.shape, 1)

        def at(ref, k, step=0):
            return ref[k + 3, p + step : p + step + height, :]

        def put(ref, k, value):
            ref[k + 3, p : p + height, :] = value

        if fresh:
            left = jnp.broadcast_to(jnp.sum(g, keepdims=True) * unit, g.shape)
            v = {k: 0.0 for k in range(-3, 4)}
        else:
            v = self.inner(self.v[top])
            v = {k: self.shifted(v, k) for k in range(-3, 4)}
            put(self.va, 0, v[0])
            around_v = (at(self.va, 0, -1) + at(self.va, 0, 1)) + (v[-1] + v[1])
            left = jnp.sum((g - self.inner(self.d[top]) * v[0]) + around_v, keepdims=True) * unit
            left = jnp.broadcast_to(left, g.shape)
        for k in range(-3, 4):
            inside = (lane < g.shape[1] - k) & (lane >= -k)
            put(self.va, k, v[k] + jnp.where(inside, left, 0.0) if k else v[k] + left)
        for turn in range(COARSE_SWEEPS // 3):
            if turn:
                v = self.inner(self.v[top])
                for k in range(-3, 4):
                    put(self.va, k, self.shifted(v, k))
            source, target = self.va, self.vb
            for reach in (2, 1, 0):
                for k in range(-reach, reach + 1):
                    total = self.gk[k + 2] + (at(source, k, -1) + at(source, k, 1))
                    total = total + (at(source, k - 1) + at(source, k + 1))
                    value = (1.0 - DAMPING) * at(source, k) + self.wk[k + 2] * total
                    if reach:
                        put(target, k, value)
                    else:
                        self.v[top][0, 0, p : p + height, :] = value
                source, target = target, source

    def widen(self, source, target, reach, padded):
        rows = slice(self.z.p, self.z.p + self.z.coarse_rows) if padded else slice(None)
        for s in range(2):
            for k in range(-reach, 2 + reach):
                target[s, k + reach, rows, :] = self.shifted(self.inner(source, s, k % 2), k // 2)

    def twice(self, restricting):
        l = LEVELS - 1 - self.first
        p, height = self.z.p, self.z.coarse_rows
        rows = slice(p, p + height)

        def at(ref, s, k, step=0):
            return ref[s, k + 2, p + step : p + step + height, :]

        def beside(ref, s, k):
            up = at(ref, 0, k) if s else at(ref, 1, k, -1)
            down = at(ref, 0, k, 1) if s else at(ref, 1, k)
            return (up + down) + (at(ref, s, k - 1) + at(ref, s, k + 1))

        def swept(ref, s, k):
            total = self.wide_g[s, k + 1] + beside(ref, s, k)
            return (1.0 - DAMPING) * at(ref, s, k) + self.wide_w[s, k + 1] * total

        self.widen(self.v[l], self.wide_v, 2, True)
        for s in range(2):
            for k in range(-1, 3):
                self.wide_t[s, k + 2, rows, :] = swept(self.wide_v, s, k)
        parts = []
        for s in range(2):
            for k in range(2):
                if restricting:
                    v = at(self.wide_t, s, k)
                    self.v[l][s, k, rows, :] = v
                    left = self.wide_g[s, k + 1] - self.inner(self.d[l], s, k) * v
                    parts.append(left + beside(self.wide_t, s, k))
                else:
                    self.v[l][s, k, rows, :] = swept(self.wide_t, s, k)
        if restricting:
            self.g[l + 1][0, 0, rows, :] = (parts[0] + parts[1]) + (parts[2] + parts[3])

    def before(self, level, fresh, new_source):
        l = level - self.first
        if level < LEVELS - 1:
            if fresh:
                self.start(level)
            else:
                self.two_sweeps(level)
            self.restrict(level)
            return
        if new_source:
            self.widen(self.g[l], self.wide_g, 1, False)
        if fresh:
            self.first_sweep(level)
        else:
            self.sweep(level, self.v[l], self.t[l])
            self.v[l], self.t[l] = self.t[l], self.v[l]
        self.twice(True)

    def after(self, level):
        self.prolong(level)
        if level < LEVELS - 1:
            self.two_sweeps(level)
        else:
            self.twice(False)

    def vcycle(self, level, fresh, unit):
        if level == LEVELS:
            self.coarse(fresh, unit)
            return
        self.before(level, fresh, fresh)
        self.vcycle(level + 1, True, unit)
        self.after(level)

    def fcycle(self, level, unit):
        if level == LEVELS:
            self.coarse(True, unit)
            return
        self.before(level, True, True)
        self.fcycle(level + 1, unit)
        self.vcycle(level + 1, False, unit)
        self.after(level)

    def clear_ends(self):
        z = self.z
        zero = jnp.zeros((z.p, z.coarse_columns), jnp.float32)
        for refs in (self.v, self.t):
            for ref in refs:
                n = ref.shape[0]
                for s in range(n):
                    for r in range(n):
                        ref[s, r, : z.p, :] = zero
                        ref[s, r, z.p + z.coarse_rows :, :] = zero
        for ref in (self.va, self.vb, self.wide_v.at[0], self.wide_v.at[1], self.wide_t.at[0], self.wide_t.at[1]):
            for k in range(ref.shape[0]):
                ref[k, : z.p, :] = zero
                ref[k, z.p + z.coarse_rows :, :] = zero

    def turned(self, blocks, k):
        q = self.z.q
        part = iota(blocks[0].shape, 1) // q
        out = blocks[-k % 8]
        for x in range(1, 8):
            out = jnp.where(part == x, blocks[(x - k) % 8], out)
        return pltpu.roll(out, -k * q % 128, 1) if k else out

    def take_two(self, even_ref, odd_ref, targets):
        z = self.z
        for gx in range(z.nx):
            for group in range(z.ny // 8):
                lanes = slice(group * 128, (group + 1) * 128)
                for s in range(4):
                    blocks = []
                    for g in range(8):
                        first = (gx * (z.ny // 2) + group * 4 + g // 2) * 4 * z.p + s * z.p
                        blocks.append((even_ref, odd_ref)[g % 2][first : first + z.p, :])
                    for k in range(8):
                        target, add = targets[k // 4]
                        value = self.turned(blocks, k)
                        target[s, k % 4, (gx + 1) * z.p : (gx + 2) * z.p, lanes] = value + add if add else value

    def take_one(self, y_ref, target):
        z = self.z
        low = iota((8, 128), 0) < 4
        for gx in range(z.nx):
            for group in range(z.ny // 8):
                upper, lower = [], []
                for g in range(0, 8, 2):
                    first = (gx * z.ny + group * 8 + g) * 4
                    pair = y_ref[first : first + 8, :]
                    swapped = pltpu.roll(pair, 4, 0)
                    upper += [pair, swapped]
                    lower += [swapped, pair]
                for k in range(4):
                    value = jnp.where(low, self.turned(upper, k), self.turned(lower, k + 4))
                    target[k // 2, k % 2, (gx + 1) * z.p : (gx + 2) * z.p, group * 128 : (group + 1) * 128] = value

    def spread(self, gx, gy, columns_ref, scratch, lines):
        z = self.z
        n = 1 << (LEVELS - self.first)
        above = self.first - 1
        columns = z.coarse_columns
        turn = lax.rem(columns + z.q - gy * z.q, columns)
        start = pl.multiple_of(gx * z.p, 8)
        for s in range(n):
            for r in range(n):
                part = pltpu.roll(self.v[0][s, r, pl.ds(start, 3 * z.p), :], turn, 1)[:, :128]
                lines[r, pl.ds(s, 3 * z.p, stride=n), :] = part
        own, halo = z.rows >> self.first, HALOS[above]
        window = slice(n * z.p - 8, n * z.p + own + 8)
        wide = f32dot_right(jnp.concatenate([lines[r, window, :] for r in range(n)], axis=1), columns_ref[...])
        doubled = double_rows(scratch, jnp.concatenate([wide[8:], wide[:8]], axis=0))
        height = doubled.shape[0]
        return jnp.concatenate([doubled[: 2 * own + halo], doubled[height - halo :]], axis=0)


def level_shape(sizes, level):
    n = 1 << (LEVELS - level)
    return (n, n, sizes.coarse_rows + 2 * sizes.p, sizes.coarse_columns)


def middle_kernel(sizes, y_ref, other_ref, c1_ref, d1_ref, w1_ref, v1_ref, w2l_ref, d2l_ref, sc_ref,
                  rc1_ref, pc_ref,
                  d3_ref, d4_ref, w3_ref, w4_ref, e1_ref, c2_ref, e2_ref, out_ref,
                  d2, w2, g2, g3, g4, v2, v3, v4, t2, t3, t4, scratch, lines, *coarsest):
    gx, gy = lax.axis_index("gx"), lax.axis_index("gy")
    m = Coarse(sizes, 2, [d2, d3_ref, d4_ref], [w2, w3_ref, w4_ref], [g2, g3, g4], [v2, v3, v4], [t2, t3, t4], coarsest)
    m.clear_ends()
    core = lax.rem(gy, 2)

    @pl.when(core == 0)
    def _():
        m.take_two(y_ref, other_ref, ((g2, 0.0), (d2, 4.0)))

    @pl.when(core == 1)
    def _():
        m.take_two(other_ref, y_ref, ((g2, 0.0), (d2, 4.0)))

    for l in range(2):
        n = 2 >> l

        def block(base):
            for s in range(n):
                for r in range(n):
                    parts = [m.at(m.d[l], 2 * s + a, 2 * r + b, base) for a in (0, 1) for b in (0, 1)]
                    m.put(m.d[l + 1], s, r, base, ((parts[0] + parts[1]) + (parts[2] + parts[3])) - 12.0)

        m.blocks(block)
    for l in range(3):
        def body(s, r, n, base):
            m.put(m.w[l], s, r, base, DAMPING / m.at(m.d[l], s, r, base))

        m.each(l + 2, body)
    unit = m.unit()
    m.fcycle(2, unit)
    m.vcycle(2, False, unit)
    g, d, w = c1_ref[...], d1_ref[...], w1_ref[...]
    v = v1_ref[...] + jnp.where(w > 0.0, m.spread(gx, gy, sc_ref, scratch, lines), 0.0)
    for turn in range(4):
        v = sweep(v, g, w)
    e1_ref[...] = v
    r = g - d * v + around(v)
    g = f32dot_right(pair_rows(scratch, r), rc1_ref[...])
    d, w = d2l_ref[...], w2l_ref[...]
    v = w * g
    v = sweep(v, g, w)
    r = g - d * v + around(v)
    c2_ref[...] = g
    e2_ref[...] = v
    pack_one(sizes, gy, pair_rows(scratch, r[: sizes.rows // 4]), scratch, pc_ref, out_ref)


def up_kernel(sizes, y_ref, d3_ref, d4_ref, w3_ref, w4_ref, c2_ref, w2_ref, e2_ref, c1_ref, w1_ref, e1_ref,
              g0_ref, d0_ref, w0_ref, v0_ref, sc_ref, pc1_ref, pc0_ref,
              solution_ref, residual_ref, g3, g4, v3, v4, t3, t4, scratch, lines, *coarsest):
    gx, gy = lax.axis_index("gx"), lax.axis_index("gy")
    m = Coarse(sizes, 3, [d3_ref, d4_ref], [w3_ref, w4_ref], [g3, g4], [v3, v4], [t3, t4], coarsest)
    m.clear_ends()
    m.take_one(y_ref, g3)
    m.vcycle(3, True, m.unit())
    g, w = c2_ref[...], w2_ref[...]
    v = e2_ref[...] + jnp.where(w > 0.0, m.spread(gx, gy, sc_ref, scratch, lines), 0.0)
    for turn in range(2):
        v = sweep(v, g, w)
    own = sizes.rows // 2
    g, w = near(c1_ref, own), near(w1_ref, own)
    v = near(e1_ref, own) + near(double_rows(scratch, f32dot_right(v, pc1_ref[...])), own)
    for turn in range(2):
        v = sweep(v, g, w)
    g, d, w = g0_ref[...], d0_ref[...], w0_ref[...]
    v = v0_ref[...] + near(double_rows(scratch, f32dot_right(v, pc0_ref[...])), sizes.rows)
    for turn in range(2):
        v = sweep(v, g, w)
    r = g - d * v + around(v)
    solution_ref[...] = v[: sizes.rows, : sizes.columns]
    residual_ref[...] = r[: sizes.rows, : sizes.columns]


def vmem(count):
    return [pl.BlockSpec(memory_space=pltpu.VMEM)] * count


def call(kernel, sizes, outs, scratch, *operands):
    shapes = [jax.ShapeDtypeStruct(shape, jnp.float32) for shape in outs]
    used = sum(4 * int(np.prod(shape)) for shape in list(outs) + list(scratch))
    used += sum(x.size * x.dtype.itemsize for x in operands)
    return pl.pallas_call(
        lambda *refs: kernel(sizes, *refs),
        name=kernel.__name__,
        out_shape=shapes,
        in_specs=vmem(len(operands)),
        out_specs=vmem(len(outs)),
        scratch_shapes=[pltpu.VMEM(shape, jnp.float32) for shape in scratch],
        compiler_params=pltpu.CompilerParams(vmem_limit_bytes=used + used // 4 + (4 << 20)),
    )(*operands)


def swaps(first, second, axis, spare):
    nx, ny = lax.axis_size("gx"), lax.axis_size("gy")
    count = lax.axis_size(axis)

    def target(gx, gy):
        place = gx if axis == "gx" else gy
        if place in (0, count - 1):
            return (gx ^ 1) * ny + gy if spare == "gx" else gx * ny + (gy ^ 1)
        place = place + 1 if place % 2 else place - 1
        return place * ny + gy if axis == "gx" else gx * ny + place

    pairs = [(gx * ny + gy, target(gx, gy)) for gx in range(nx) for gy in range(ny)]
    return lax.ppermute(first, axis, [(i, i ^ 1) for i in range(count)]), lax.ppermute(second, ("gx", "gy"), pairs)


def gather(copies):
    return lax.all_to_all(copies, ("gx", "gy"), 0, 0, tiled=True)


def gather_by_core(copies, nx, ny):
    index = np.arange(nx * ny)
    groups = [index[core::2].tolist() for core in range(2)]
    own = lax.all_to_all(copies, ("gx", "gy"), 0, 0, tiled=True, axis_index_groups=groups)
    return own, lax.ppermute(own, "gy", [(j, j ^ 1) for j in range(ny)])


def body(right_side, shift):
    nx, ny = lax.axis_size("gx"), lax.axis_size("gy")
    rows, columns = right_side.shape
    z = Sizes(rows, columns, nx, ny)
    even = lax.axis_index("gx") % 2 == 0
    last = rows - HALO

    def strips(start):
        return jnp.stack([lax.dynamic_slice(x, (start, 0), (HALO, columns)) for x in (right_side, shift)])

    rows_a, rows_b = swaps(strips(jnp.where(even, last, 0)), strips(jnp.where(even, 0, last)), "gx", "gy")
    ext = [(z.ext_rows[l], z.ext_columns[l]) for l in range(3)]
    strip = (strip_rows(z)[1], 128)
    first, second = call(strip_kernel, z, [strip] * 2, [], right_side, shift, rows_a, rows_b)
    columns_a, columns_b = swaps(first, second, "gy", "gx")
    rc0, rc1 = z.restrict_columns(0), z.restrict_columns(1)
    tiles = (ext[0][1] // 128, ext[0][0], 128)
    g0, d0, w0, v0, c1, d1, w1, v1, d2, w2, packed = call(
        down_kernel, z, [(rows + 2 * NEAR, ext[0][1])] * 4 + [ext[1]] * 4 + [ext[2]] * 2 + [(nx * ny // 2 * 4 * z.p, 128)], [tiles],
        right_side, shift, rows_a, rows_b, columns_a, columns_b, rc0, rc1, z.pack_pair())
    y, other = gather_by_core(packed, nx, ny)
    slabs = [level_shape(z, level) for level in (2, 3, 4)]
    padded, plain = slabs[2][2:], (z.coarse_rows, z.coarse_columns)
    coarsest = [(7,) + padded] * 2 + [(5,) + plain] * 2 + [(2, 6) + padded] * 2 + [(2, 4) + plain] * 2
    d3, d4, w3, w4, e1, c2, e2, packed = call(
        middle_kernel, z, slabs[1:] * 2 + [ext[1], ext[2], ext[2], (nx * ny * 4, 128)],
        [slabs[0]] * 2 + slabs * 3 + [tiles, (4, 12 * z.p, 128)] + coarsest,
        y, other, c1, d1, w1, v1, w2, d2, z.spread_columns(2),
        rc1, z.pack_single())
    y = gather(packed)
    return call(
        up_kernel, z, [(rows, columns)] * 2, slabs[1:] * 3 + [tiles, (2, 6 * z.p, 128)] + coarsest,
        y, d3, d4, w3, w4, c2, w2, e2, c1, w1, e1, g0, d0, w0, v0,
        z.spread_columns(3), rc1.T, rc0.T)


def solution(mesh):
    specs = (P("gx", "gy"), P("gx", "gy"))

    def run(right_side, shift):
        out = body(right_side, shift)
        return out[0], out[1]

    return jax.shard_map(run, mesh=mesh, in_specs=specs, out_specs=specs, check_vma=False)
```

```python
import numpy as np
import jax
import jax.numpy as jnp
from jax import lax
from jax.experimental import pallas as pl
from jax.experimental.pallas import tpu as pltpu
from jax.sharding import PartitionSpec as P

LEVELS = 4
COARSE_SWEEPS = 6
DAMPING = 0.8
HALOS = (40, 16, 8)
HALO = HALOS[0]
NEAR = 8


def f32dot_right(values, onehot):
    high = values.astype(jnp.bfloat16)
    rest = values - high.astype(jnp.float32)
    middle = rest.astype(jnp.bfloat16)
    low = (rest - middle.astype(jnp.float32)).astype(jnp.bfloat16)
    rows = values.shape[0]
    stacked = jnp.concatenate([high, middle, low], axis=0)
    out = jnp.dot(stacked, onehot, preferred_element_type=jnp.float32)
    return (out[2 * rows :] + out[rows : 2 * rows]) + out[:rows]


def around(v):
    rows, columns = v.shape
    up = pltpu.roll(v, 1, 0)
    down = pltpu.roll(v, rows - 1, 0)
    left = pltpu.roll(v, 1, 1)
    right = pltpu.roll(v, columns - 1, 1)
    return (up + down) + (left + right)


def sweep(v, g, w):
    return (1.0 - DAMPING) * v + w * (g + around(v))


class Sizes:
    def __init__(self, rows, columns, nx, ny):
        self.rows, self.columns, self.nx, self.ny = rows, columns, nx, ny
        self.p, self.q = rows // 16, columns // 16
        self.coarse_rows, self.coarse_columns = nx * self.p, ny * self.q
        assert self.p == 8 and 8 * self.q == 128, "block shape"

        def up(n):
            return -(-n // 128) * 128

        self.ext_rows = [(rows >> l) + 2 * HALOS[l] for l in range(3)]
        self.ext_columns = [up((columns >> l) + 2 * HALOS[l]) for l in range(3)]

    def column_at(self, level):
        own, halo, width = self.columns >> level, HALOS[level], self.ext_columns[level]
        lane = np.arange(width)
        inside = (lane < own + halo) | (lane >= width - halo)
        return np.where(lane < own + halo, lane, lane - width), inside

    def restrict_columns(self, level):
        fine, fine_in = self.column_at(level)
        coarse, coarse_in = self.column_at(level + 1)
        hit = (fine[:, None] // 2 == coarse[None, :]) & fine_in[:, None] & coarse_in[None, :]
        return hit.astype(jnp.bfloat16)

    def pack_pair(self):
        width, own = self.ext_columns[1], self.columns >> 1
        x = np.arange(2 * width)
        column = x % width // 2
        target = (x // width) * (own // 2) + (column % 4) * self.q + column // 4
        hit = (target[:, None] == np.arange(own)[None, :]) & (x % width < own)[:, None]
        return hit.astype(jnp.bfloat16)

    def pack_single(self):
        x = np.arange(self.ext_columns[2])[:, None]
        lane = np.arange(128)[None, :]
        hit = (x // 2 == 2 * (lane % self.q) + (lane // self.q) % 2) & (x < self.columns >> 2)
        return hit.astype(jnp.bfloat16)

    def spread_columns(self, level):
        n = 1 << (LEVELS - level)
        column, inside = self.column_at(level - 1)
        m = column // 2
        r = np.arange(n)[:, None, None]
        lane = np.arange(128)[None, :, None]
        hit = (m % n == r) & (m // n + self.q == lane) & inside
        return hit.reshape(n * 128, -1).astype(jnp.bfloat16)


def iota(shape, axis):
    return lax.broadcasted_iota(jnp.int32, shape, axis)


def inside_mask(sizes, level, gx, gy):
    shape = (sizes.ext_rows[level], sizes.ext_columns[level])
    own_r, own_c, halo = sizes.rows >> level, sizes.columns >> level, HALOS[level]
    row, column = iota(shape, 0), iota(shape, 1)
    last_row = jnp.where(gx < sizes.nx - 1, own_r + halo, own_r)
    first_row = jnp.where(gx > 0, own_r + halo, shape[0])
    last_column = jnp.where(gy < sizes.ny - 1, own_c + halo, own_c)
    first_column = jnp.where(gy > 0, shape[1] - halo, shape[1])
    return ((row < last_row) | (row >= first_row)) & ((column < last_column) | (column >= first_column))


def pair_rows(scratch, values):
    rows, columns = values.shape
    outs = []
    for t in range(columns // 128):
        scratch[t, :rows, :] = values[:, t * 128 : (t + 1) * 128]
    for t in range(columns // 128):
        outs.append(scratch[t, pl.ds(0, rows // 2, stride=2), :] + scratch[t, pl.ds(1, rows // 2, stride=2), :])
    return jnp.concatenate(outs, axis=1)


def double_rows(scratch, values):
    rows, columns = values.shape
    for t in range(columns // 128):
        part = values[:, t * 128 : (t + 1) * 128]
        scratch[t, pl.ds(0, rows, stride=2), :] = part
        scratch[t, pl.ds(1, rows, stride=2), :] = part
    return jnp.concatenate([scratch[t, : 2 * rows, :] for t in range(columns // 128)], axis=1)


def repeat(block, out_ref):
    height = block.shape[0]
    for k in range(out_ref.shape[0] // height):
        out_ref[k * height : (k + 1) * height, :] = block


def pack_two(sizes, gy, first, second, scratch, columns_ref, out_ref):
    rows = first.shape[0]
    scratch[0, :rows, :] = f32dot_right(jnp.concatenate([first, second], axis=1), columns_ref[...])
    block = jnp.concatenate([scratch[0, pl.ds(s, sizes.p, stride=4), :] for s in range(4)], axis=0)
    repeat(pltpu.roll(block, lax.rem(gy, 8) * sizes.q, 1), out_ref)


def pack_one(sizes, gy, values, scratch, columns_ref, out_ref):
    rows = values.shape[0]
    scratch[0, :rows, :] = f32dot_right(values, columns_ref[...])
    part = iota((4, 128), 1) // (2 * sizes.q)
    block = scratch[0, pl.ds(0, 4, stride=2), :]
    for k in range(1, 4):
        block = jnp.where(part == k, scratch[0, pl.ds(8 * (k // 2) + k % 2, 4, stride=2), :], block)
    block = jnp.concatenate([block, block], axis=0)
    repeat(pltpu.roll(block, lax.rem(gy, 8) * sizes.q, 1), out_ref)


def near(values, own):
    return jnp.concatenate([values[: own + NEAR], values[values.shape[0] - NEAR :]], axis=0)


def sides(at, first_ref, second_ref):
    even = lax.rem(at, 2) == 0
    first, second = first_ref[...], second_ref[...]
    return jnp.where(even, first, second), jnp.where(even, second, first)


def strip_rows(sizes):
    groups = 128 // HALO
    return groups, -(-2 * sizes.ext_rows[0] // (8 * groups)) * 8


def fold(sizes, strip, step):
    groups, height = strip_rows(sizes)
    lane = iota((height, 128), 1)
    lane = lane if step > 0 else 127 - lane
    out = strip[:height]
    for k in range(1, groups):
        part = strip[k * height : (k + 1) * height]
        part = pltpu.roll(part, k * step % 128, 1)
        if part.shape[0] < height:
            part = jnp.concatenate([part, jnp.zeros((height - part.shape[0], 128), jnp.float32)], axis=0)
        out = jnp.where(lane >= k * HALO, part, out)
    return out


def unfold(sizes, packed, step):
    groups, _ = strip_rows(sizes)
    parts = [packed] + [pltpu.roll(packed, -k * step % 128, 1) for k in range(1, groups)]
    rows = sizes.ext_rows[0]
    out = jnp.concatenate(parts, axis=0)
    return out[:rows], out[rows : 2 * rows]


def strip_kernel(sizes, g_ref, s_ref, rows_a_ref, rows_b_ref, first_ref, second_ref):
    last = sizes.columns - 128
    even = lax.rem(lax.axis_index("gy"), 2) == 0
    below, above = sides(lax.axis_index("gx"), rows_a_ref, rows_b_ref)
    fields = (g_ref[...], below[0], above[0], s_ref[...], below[1], above[1])
    left = fold(sizes, jnp.concatenate([x[:, :128] for x in fields], axis=0), HALO)
    right = fold(sizes, jnp.concatenate([x[:, last:] for x in fields], axis=0), -HALO)
    first_ref[...] = jnp.where(even, right, left)
    second_ref[...] = jnp.where(even, left, right)


def coefficients(sizes, level, gx, gy, sigma):
    d = 4.0 + sigma
    return d, jnp.where(inside_mask(sizes, level, gx, gy), DAMPING / d, 0.0)


def down_kernel(sizes, g_ref, s_ref, rows_a_ref, rows_b_ref, columns_a_ref, columns_b_ref,
                rc0_ref, rc1_ref, pc_ref,
                g0_ref, d0_ref, w0_ref, v0_ref, c1_ref, d1_ref, w1_ref, v1_ref, d2_ref, w2_ref, out_ref, scratch):
    gx, gy = lax.axis_index("gx"), lax.axis_index("gy")
    rows = sizes.ext_rows[0]
    lane = iota((rows, 128), 1)
    below, above = sides(gx, rows_a_ref, rows_b_ref)
    from_right, from_left = sides(gy, columns_a_ref, columns_b_ref)
    from_right, from_left = unfold(sizes, from_right, HALO), unfold(sizes, from_left, -HALO)
    g = jnp.where(lane < HALO, from_right[0], from_left[0])
    sigma = jnp.where(lane < HALO, from_right[1], from_left[1])
    g = jnp.concatenate([jnp.concatenate([g_ref[...], below[0], above[0]], axis=0), g], axis=1)
    sigma = jnp.concatenate([jnp.concatenate([s_ref[...], below[1], above[1]], axis=0), sigma], axis=1)
    d, w = coefficients(sizes, 0, gx, gy, sigma)
    v = w * g
    v = sweep(v, g, w)
    r = g - d * v + around(v)
    for ref, values in ((g0_ref, g), (d0_ref, d), (w0_ref, w), (v0_ref, v)):
        ref[...] = near(values, sizes.rows)
    both = []
    own, halo = sizes.rows // 2, HALOS[1]
    for values in (r, sigma):
        pairs = pair_rows(scratch, values)
        both += [pairs[: own + halo], pairs[pairs.shape[0] - halo :]]
    both = f32dot_right(jnp.concatenate(both, axis=0), rc0_ref[...])
    half = own + 2 * halo
    g, sigma = both[:half], both[half:]
    d, w = coefficients(sizes, 1, gx, gy, sigma)
    v = w * g
    v = sweep(v, g, w)
    r = g - d * v + around(v)
    c1_ref[...] = g
    d1_ref[...] = d
    w1_ref[...] = w
    v1_ref[...] = v
    own = sizes.rows // 4
    source, sigma = pair_rows(scratch, r), pair_rows(scratch, sigma)
    pack_two(sizes, gy, source[:own], sigma[:own], scratch, pc_ref, out_ref)
    d, w = coefficients(sizes, 2, gx, gy, f32dot_right(sigma, rc1_ref[...]))
    d2_ref[...] = d
    w2_ref[...] = w


class Coarse:
    def __init__(self, sizes, first, d_refs, w_refs, g_refs, v_refs, t_refs, coarsest):
        self.z = sizes
        self.first = first
        self.d, self.w, self.g, self.v, self.t = d_refs, w_refs, g_refs, v_refs, t_refs
        self.va, self.vb, self.wk, self.gk, self.wide_v, self.wide_t, self.wide_w, self.wide_g, self.ones = coarsest
        lane = iota((sizes.p, sizes.coarse_columns), 1)
        self.first_lane, self.last_lane = lane == 0, lane == sizes.coarse_columns - 1

    def blocks(self, body):
        p = self.z.p
        if self.z.nx <= 4:
            for gx in range(self.z.nx):
                body((gx + 1) * p)
        else:
            def step(gx, carry):
                body(pl.multiple_of((gx + 1) * p, 8))
                return carry

            lax.fori_loop(0, self.z.nx, step, 0)

    def at(self, ref, s, r, base):
        return ref[s, r, pl.ds(base, self.z.p), :]

    def put(self, ref, s, r, base, value):
        ref[s, r, pl.ds(base, self.z.p), :] = value

    def beside(self, ref, s, r, base, step):
        p = self.z.p
        if isinstance(base, int):
            return ref[s, r, pl.ds(base + step, p), :]
        return ref[s, r, pl.ds(base - p, 3 * p), :][p + step : 2 * p + step]

    def neighbours(self, ref, s, r, n, base):
        columns = self.z.coarse_columns
        if r < n - 1:
            right = self.at(ref, s, r + 1, base)
        else:
            right = jnp.where(self.last_lane, 0.0, pltpu.roll(self.at(ref, s, 0, base), columns - 1, 1))
        if r > 0:
            left = self.at(ref, s, r - 1, base)
        else:
            left = jnp.where(self.first_lane, 0.0, pltpu.roll(self.at(ref, s, n - 1, base), 1, 1))
        down = self.at(ref, s + 1, r, base) if s < n - 1 else self.beside(ref, 0, r, base, 1)
        up = self.at(ref, s - 1, r, base) if s > 0 else self.beside(ref, n - 1, r, base, -1)
        return (up + down) + (left + right)

    def each(self, level, body):
        n = 1 << (LEVELS - level)

        def block(base):
            for s in range(n):
                for r in range(n):
                    body(s, r, n, base)

        self.blocks(block)

    def first_sweep(self, level):
        l = level - self.first

        def body(s, r, n, base):
            self.put(self.v[l], s, r, base, self.at(self.w[l], s, r, base) * self.at(self.g[l], s, r, base))

        self.each(level, body)

    def sweep(self, level, source, target):
        l = level - self.first

        def body(s, r, n, base):
            v = self.at(source, s, r, base)
            total = self.at(self.g[l], s, r, base) + self.neighbours(source, s, r, n, base)
            self.put(target, s, r, base, (1.0 - DAMPING) * v + self.at(self.w[l], s, r, base) * total)

        self.each(level, body)

    def two_sweeps(self, level):
        l = level - self.first
        self.sweep(level, self.v[l], self.t[l])
        self.sweep(level, self.t[l], self.v[l])

    def start(self, level):
        l = level - self.first
        self.first_sweep(level)
        self.sweep(level, self.v[l], self.t[l])
        self.v[l], self.t[l] = self.t[l], self.v[l]

    def residual(self, level, s, r, n, base):
        l = level - self.first
        v = self.at(self.v[l], s, r, base)
        g = self.at(self.g[l], s, r, base)
        return (g - self.at(self.d[l], s, r, base) * v) + self.neighbours(self.v[l], s, r, n, base)

    def restrict(self, level):
        l = level - self.first
        n = 1 << (LEVELS - level)

        def block(base):
            for s in range(n // 2):
                for r in range(n // 2):
                    parts = [self.residual(level, 2 * s + a, 2 * r + b, n, base) for a in (0, 1) for b in (0, 1)]
                    self.put(self.g[l + 1], s, r, base, (parts[0] + parts[1]) + (parts[2] + parts[3]))

        self.blocks(block)

    def prolong(self, level):
        l = level - self.first

        def body(s, r, n, base):
            e = self.at(self.v[l + 1], s // 2, r // 2, base)
            self.put(self.v[l], s, r, base, self.at(self.v[l], s, r, base) + e)

        self.each(level, body)

    def inner(self, ref, s=0, r=0):
        p = self.z.p
        return ref[s, r, p : p + self.z.coarse_rows, :]

    def shifted(self, x, k):
        if k == 0:
            return x
        columns = self.z.coarse_columns
        lane = iota(x.shape, 1)
        keep = lane < columns - k if k > 0 else lane >= -k
        return jnp.where(keep, pltpu.roll(x, -k % columns, 1), 0.0)

    def unit(self, build):
        z = self.z
        top = LEVELS - self.first
        d, w = self.inner(self.d[top]), self.inner(self.w[top])
        missing = 2.0 * (z.coarse_rows + z.coarse_columns)
        for k in range(-2, 3):
            self.wk[k + 2] = self.shifted(w, k)
        self.widen(self.w[top - 1], self.wide_w, 1, False)
        if build:
            lane = iota(d.shape, 1)
            for k in range(-3, 4):
                self.put_shifted(self.va, k, jnp.where((lane < d.shape[1] - k) & (lane >= -k), 1.0, 0.0))
            self.ones[...] = self.coarse_sweeps(False, False)
        return 1.0 / (jnp.sum(d - 4.0, keepdims=True) + missing)

    def shifted_at(self, ref, k, step=0):
        p = self.z.p
        return ref[k + 3, p + step : p + step + self.z.coarse_rows, :]

    def put_shifted(self, ref, k, value):
        ref[k + 3, self.z.p : self.z.p + self.z.coarse_rows, :] = value

    def coarse_sweeps(self, from_zero, with_source):
        at = self.shifted_at
        for turn in range(COARSE_SWEEPS // 3):
            if turn:
                for k in range(-3, 4):
                    self.put_shifted(self.va, k, self.shifted(value, k))
            source, target = self.va, self.vb
            for reach in (2, 1, 0):
                for k in range(-reach, reach + 1):
                    if from_zero and not turn and reach == 2:
                        value = self.wk[k + 2] * self.gk[k + 2]
                    else:
                        total = (at(source, k, -1) + at(source, k, 1)) + (at(source, k - 1) + at(source, k + 1))
                        if with_source:
                            total = self.gk[k + 2] + total
                        value = (1.0 - DAMPING) * at(source, k) + self.wk[k + 2] * total
                    if reach:
                        self.put_shifted(target, k, value)
                source, target = target, source
        return value

    def coarse(self, fresh, unit):
        top = LEVELS - self.first
        g = self.inner(self.g[top])
        for k in range(-2, 3):
            self.gk[k + 2] = self.shifted(g, k)
        if fresh:
            left = jnp.sum(g, keepdims=True)
        else:
            v = self.inner(self.v[top])
            for k in range(-3, 4):
                self.put_shifted(self.va, k, self.shifted(v, k))
            at = self.shifted_at
            beside = (at(self.va, 0, -1) + at(self.va, 0, 1)) + (at(self.va, -1) + at(self.va, 1))
            left = jnp.sum((g - self.inner(self.d[top]) * v) + beside, keepdims=True)
        value = self.coarse_sweeps(fresh, True)
        left = jnp.broadcast_to(left * unit, g.shape)
        self.v[top][0, 0, self.z.p : self.z.p + self.z.coarse_rows, :] = value + left * self.ones[...]

    def widen(self, source, target, reach, padded):
        rows = slice(self.z.p, self.z.p + self.z.coarse_rows) if padded else slice(None)
        for s in range(2):
            for k in range(-reach, 2 + reach):
                target[s, k + reach, rows, :] = self.shifted(self.inner(source, s, k % 2), k // 2)

    def twice(self, restricting):
        l = LEVELS - 1 - self.first
        p, height = self.z.p, self.z.coarse_rows
        rows = slice(p, p + height)

        def at(ref, s, k, step=0):
            return ref[s, k + 2, p + step : p + step + height, :]

        def beside(ref, s, k):
            up = at(ref, 0, k) if s else at(ref, 1, k, -1)
            down = at(ref, 0, k, 1) if s else at(ref, 1, k)
            return (up + down) + (at(ref, s, k - 1) + at(ref, s, k + 1))

        def swept(ref, s, k):
            total = self.wide_g[s, k + 1] + beside(ref, s, k)
            return (1.0 - DAMPING) * at(ref, s, k) + self.wide_w[s, k + 1] * total

        self.widen(self.v[l], self.wide_v, 2, True)
        for s in range(2):
            for k in range(-1, 3):
                self.wide_t[s, k + 2, rows, :] = swept(self.wide_v, s, k)
        parts = []
        for s in range(2):
            for k in range(2):
                if restricting:
                    v = at(self.wide_t, s, k)
                    self.v[l][s, k, rows, :] = v
                    left = self.wide_g[s, k + 1] - self.inner(self.d[l], s, k) * v
                    parts.append(left + beside(self.wide_t, s, k))
                else:
                    self.v[l][s, k, rows, :] = swept(self.wide_t, s, k)
        if restricting:
            self.g[l + 1][0, 0, rows, :] = (parts[0] + parts[1]) + (parts[2] + parts[3])

    def before(self, level, fresh, new_source):
        l = level - self.first
        if level < LEVELS - 1:
            if fresh:
                self.start(level)
            else:
                self.two_sweeps(level)
            self.restrict(level)
            return
        if new_source:
            self.widen(self.g[l], self.wide_g, 1, False)
        if fresh:
            self.first_sweep(level)
        else:
            self.sweep(level, self.v[l], self.t[l])
            self.v[l], self.t[l] = self.t[l], self.v[l]
        self.twice(True)

    def after(self, level):
        self.prolong(level)
        if level < LEVELS - 1:
            self.two_sweeps(level)
        else:
            self.twice(False)

    def vcycle(self, level, fresh, unit):
        if level == LEVELS:
            self.coarse(fresh, unit)
            return
        self.before(level, fresh, fresh)
        self.vcycle(level + 1, True, unit)
        self.after(level)

    def fcycle(self, level, unit):
        if level == LEVELS:
            self.coarse(True, unit)
            return
        self.before(level, True, True)
        self.fcycle(level + 1, unit)
        self.vcycle(level + 1, False, unit)
        self.after(level)

    def clear_ends(self):
        z = self.z
        zero = jnp.zeros((z.p, z.coarse_columns), jnp.float32)
        for refs in (self.v, self.t):
            for ref in refs:
                n = ref.shape[0]
                for s in range(n):
                    for r in range(n):
                        ref[s, r, : z.p, :] = zero
                        ref[s, r, z.p + z.coarse_rows :, :] = zero
        for ref in (self.va, self.vb, self.wide_v.at[0], self.wide_v.at[1], self.wide_t.at[0], self.wide_t.at[1]):
            for k in range(ref.shape[0]):
                ref[k, : z.p, :] = zero
                ref[k, z.p + z.coarse_rows :, :] = zero

    def turned(self, blocks, k):
        q = self.z.q
        part = iota(blocks[0].shape, 1) // q
        out = blocks[-k % 8]
        for x in range(1, 8):
            out = jnp.where(part == x, blocks[(x - k) % 8], out)
        return pltpu.roll(out, -k * q % 128, 1) if k else out

    def take_two(self, even_ref, odd_ref, targets):
        z = self.z
        for gx in range(z.nx):
            for group in range(z.ny // 8):
                lanes = slice(group * 128, (group + 1) * 128)
                for s in range(4):
                    blocks = []
                    for g in range(8):
                        first = (gx * (z.ny // 2) + group * 4 + g // 2) * 4 * z.p + s * z.p
                        blocks.append((even_ref, odd_ref)[g % 2][first : first + z.p, :])
                    for k in range(8):
                        target, add = targets[k // 4]
                        value = self.turned(blocks, k)
                        target[s, k % 4, (gx + 1) * z.p : (gx + 2) * z.p, lanes] = value + add if add else value

    def take_one(self, y_ref, target):
        z = self.z
        low = iota((8, 128), 0) < 4
        for gx in range(z.nx):
            for group in range(z.ny // 8):
                upper, lower = [], []
                for g in range(0, 8, 2):
                    first = (gx * z.ny + group * 8 + g) * 4
                    pair = y_ref[first : first + 8, :]
                    swapped = pltpu.roll(pair, 4, 0)
                    upper += [pair, swapped]
                    lower += [swapped, pair]
                for k in range(4):
                    value = jnp.where(low, self.turned(upper, k), self.turned(lower, k + 4))
                    target[k // 2, k % 2, (gx + 1) * z.p : (gx + 2) * z.p, group * 128 : (group + 1) * 128] = value

    def spread(self, gx, gy, columns_ref, scratch, lines):
        z = self.z
        n = 1 << (LEVELS - self.first)
        above = self.first - 1
        columns = z.coarse_columns
        turn = lax.rem(columns + z.q - gy * z.q, columns)
        start = pl.multiple_of(gx * z.p, 8)
        for s in range(n):
            for r in range(n):
                part = pltpu.roll(self.v[0][s, r, pl.ds(start, 3 * z.p), :], turn, 1)[:, :128]
                lines[r, pl.ds(s, 3 * z.p, stride=n), :] = part
        own, halo = z.rows >> self.first, HALOS[above]
        window = slice(n * z.p - 8, n * z.p + own + 8)
        wide = f32dot_right(jnp.concatenate([lines[r, window, :] for r in range(n)], axis=1), columns_ref[...])
        doubled = double_rows(scratch, jnp.concatenate([wide[8:], wide[:8]], axis=0))
        height = doubled.shape[0]
        return jnp.concatenate([doubled[: 2 * own + halo], doubled[height - halo :]], axis=0)


def level_shape(sizes, level):
    n = 1 << (LEVELS - level)
    return (n, n, sizes.coarse_rows + 2 * sizes.p, sizes.coarse_columns)


def middle_kernel(sizes, y_ref, other_ref, c1_ref, d1_ref, w1_ref, v1_ref, w2l_ref, d2l_ref, sc_ref,
                  rc1_ref, pc_ref,
                  d3_ref, d4_ref, w3_ref, w4_ref, ones_ref, e1_ref, c2_ref, e2_ref, out_ref,
                  d2, w2, g2, g3, g4, v2, v3, v4, t2, t3, t4, scratch, lines, *coarsest):
    gx, gy = lax.axis_index("gx"), lax.axis_index("gy")
    m = Coarse(sizes, 2, [d2, d3_ref, d4_ref], [w2, w3_ref, w4_ref], [g2, g3, g4], [v2, v3, v4], [t2, t3, t4], (*coarsest, ones_ref))
    m.clear_ends()
    core = lax.rem(gy, 2)

    @pl.when(core == 0)
    def _():
        m.take_two(y_ref, other_ref, ((g2, 0.0), (d2, 4.0)))

    @pl.when(core == 1)
    def _():
        m.take_two(other_ref, y_ref, ((g2, 0.0), (d2, 4.0)))

    for l in range(2):
        n = 2 >> l

        def block(base):
            for s in range(n):
                for r in range(n):
                    parts = [m.at(m.d[l], 2 * s + a, 2 * r + b, base) for a in (0, 1) for b in (0, 1)]
                    m.put(m.d[l + 1], s, r, base, ((parts[0] + parts[1]) + (parts[2] + parts[3])) - 12.0)

        m.blocks(block)
    for l in range(3):
        def body(s, r, n, base):
            m.put(m.w[l], s, r, base, DAMPING / m.at(m.d[l], s, r, base))

        m.each(l + 2, body)
    unit = m.unit(True)
    m.fcycle(2, unit)
    m.vcycle(2, False, unit)
    g, d, w = c1_ref[...], d1_ref[...], w1_ref[...]
    v = v1_ref[...] + jnp.where(w > 0.0, m.spread(gx, gy, sc_ref, scratch, lines), 0.0)
    for turn in range(4):
        v = sweep(v, g, w)
    e1_ref[...] = v
    r = g - d * v + around(v)
    g = f32dot_right(pair_rows(scratch, r), rc1_ref[...])
    d, w = d2l_ref[...], w2l_ref[...]
    v = w * g
    v = sweep(v, g, w)
    r = g - d * v + around(v)
    c2_ref[...] = g
    e2_ref[...] = v
    pack_one(sizes, gy, pair_rows(scratch, r[: sizes.rows // 4]), scratch, pc_ref, out_ref)


def up_kernel(sizes, y_ref, d3_ref, d4_ref, w3_ref, w4_ref, ones_ref, c2_ref, w2_ref, e2_ref, c1_ref, w1_ref, e1_ref,
              g0_ref, d0_ref, w0_ref, v0_ref, sc_ref, pc1_ref, pc0_ref,
              solution_ref, residual_ref, g3, g4, v3, v4, t3, t4, scratch, lines, *coarsest):
    gx, gy = lax.axis_index("gx"), lax.axis_index("gy")
    m = Coarse(sizes, 3, [d3_ref, d4_ref], [w3_ref, w4_ref], [g3, g4], [v3, v4], [t3, t4], (*coarsest, ones_ref))
    m.clear_ends()
    m.take_one(y_ref, g3)
    m.vcycle(3, True, m.unit(False))
    g, w = c2_ref[...], w2_ref[...]
    v = e2_ref[...] + jnp.where(w > 0.0, m.spread(gx, gy, sc_ref, scratch, lines), 0.0)
    for turn in range(2):
        v = sweep(v, g, w)
    own = sizes.rows // 2
    g, w = near(c1_ref, own), near(w1_ref, own)
    v = near(e1_ref, own) + near(double_rows(scratch, f32dot_right(v, pc1_ref[...])), own)
    for turn in range(2):
        v = sweep(v, g, w)
    g, d, w = g0_ref[...], d0_ref[...], w0_ref[...]
    v = v0_ref[...] + near(double_rows(scratch, f32dot_right(v, pc0_ref[...])), sizes.rows)
    for turn in range(2):
        v = sweep(v, g, w)
    r = g - d * v + around(v)
    solution_ref[...] = v[: sizes.rows, : sizes.columns]
    residual_ref[...] = r[: sizes.rows, : sizes.columns]


def vmem(count):
    return [pl.BlockSpec(memory_space=pltpu.VMEM)] * count


def call(kernel, sizes, outs, scratch, *operands):
    shapes = [jax.ShapeDtypeStruct(shape, jnp.float32) for shape in outs]
    used = sum(4 * int(np.prod(shape)) for shape in list(outs) + list(scratch))
    used += sum(x.size * x.dtype.itemsize for x in operands)
    return pl.pallas_call(
        lambda *refs: kernel(sizes, *refs),
        name=kernel.__name__,
        out_shape=shapes,
        in_specs=vmem(len(operands)),
        out_specs=vmem(len(outs)),
        scratch_shapes=[pltpu.VMEM(shape, jnp.float32) for shape in scratch],
        compiler_params=pltpu.CompilerParams(vmem_limit_bytes=used + used // 4 + (4 << 20)),
    )(*operands)


def swaps(first, second, axis, spare):
    nx, ny = lax.axis_size("gx"), lax.axis_size("gy")
    count = lax.axis_size(axis)

    def target(gx, gy):
        place = gx if axis == "gx" else gy
        if place in (0, count - 1):
            return (gx ^ 1) * ny + gy if spare == "gx" else gx * ny + (gy ^ 1)
        place = place + 1 if place % 2 else place - 1
        return place * ny + gy if axis == "gx" else gx * ny + place

    pairs = [(gx * ny + gy, target(gx, gy)) for gx in range(nx) for gy in range(ny)]
    return lax.ppermute(first, axis, [(i, i ^ 1) for i in range(count)]), lax.ppermute(second, ("gx", "gy"), pairs)


def gather(copies):
    return lax.all_to_all(copies, ("gx", "gy"), 0, 0, tiled=True)


def gather_by_core(copies, nx, ny):
    index = np.arange(nx * ny)
    groups = [index[core::2].tolist() for core in range(2)]
    own = lax.all_to_all(copies, ("gx", "gy"), 0, 0, tiled=True, axis_index_groups=groups)
    return own, lax.ppermute(own, "gy", [(j, j ^ 1) for j in range(ny)])


def body(right_side, shift):
    nx, ny = lax.axis_size("gx"), lax.axis_size("gy")
    rows, columns = right_side.shape
    z = Sizes(rows, columns, nx, ny)
    even = lax.axis_index("gx") % 2 == 0
    last = rows - HALO

    def strips(start):
        return jnp.stack([lax.dynamic_slice(x, (start, 0), (HALO, columns)) for x in (right_side, shift)])

    rows_a, rows_b = swaps(strips(jnp.where(even, last, 0)), strips(jnp.where(even, 0, last)), "gx", "gy")
    ext = [(z.ext_rows[l], z.ext_columns[l]) for l in range(3)]
    strip = (strip_rows(z)[1], 128)
    first, second = call(strip_kernel, z, [strip] * 2, [], right_side, shift, rows_a, rows_b)
    columns_a, columns_b = swaps(first, second, "gy", "gx")
    rc0, rc1 = z.restrict_columns(0), z.restrict_columns(1)
    tiles = (ext[0][1] // 128, ext[0][0], 128)
    g0, d0, w0, v0, c1, d1, w1, v1, d2, w2, packed = call(
        down_kernel, z, [(rows + 2 * NEAR, ext[0][1])] * 4 + [ext[1]] * 4 + [ext[2]] * 2 + [(nx * ny // 2 * 4 * z.p, 128)], [tiles],
        right_side, shift, rows_a, rows_b, columns_a, columns_b, rc0, rc1, z.pack_pair())
    y, other = gather_by_core(packed, nx, ny)
    slabs = [level_shape(z, level) for level in (2, 3, 4)]
    padded, plain = slabs[2][2:], (z.coarse_rows, z.coarse_columns)
    coarsest = [(7,) + padded] * 2 + [(5,) + plain] * 2 + [(2, 6) + padded] * 2 + [(2, 4) + plain] * 2
    d3, d4, w3, w4, ones, e1, c2, e2, packed = call(
        middle_kernel, z, slabs[1:] * 2 + [plain, ext[1], ext[2], ext[2], (nx * ny * 4, 128)],
        [slabs[0]] * 2 + slabs * 3 + [tiles, (4, 12 * z.p, 128)] + coarsest,
        y, other, c1, d1, w1, v1, w2, d2, z.spread_columns(2),
        rc1, z.pack_single())
    y = gather(packed)
    return call(
        up_kernel, z, [(rows, columns)] * 2, slabs[1:] * 3 + [tiles, (2, 6 * z.p, 128)] + coarsest,
        y, d3, d4, w3, w4, ones, c2, w2, e2, c1, w1, e1, g0, d0, w0, v0,
        z.spread_columns(3), rc1.T, rc0.T)


def solution(mesh):
    specs = (P("gx", "gy"), P("gx", "gy"))

    def run(right_side, shift):
        out = body(right_side, shift)
        return out[0], out[1]

    return jax.shard_map(run, mesh=mesh, in_specs=specs, out_specs=specs, check_vma=False)
```

```python
import numpy as np
import jax
import jax.numpy as jnp
from jax import lax
from jax.experimental import pallas as pl
from jax.experimental.pallas import tpu as pltpu
from jax.sharding import PartitionSpec as P

LEVELS = 4
COARSE_SWEEPS = 6
DAMPING = 0.8
HALOS = (40, 16, 8)
HALO = HALOS[0]
NEAR = 8


def f32dot_right(values, onehot):
    high = values.astype(jnp.bfloat16)
    rest = values - high.astype(jnp.float32)
    middle = rest.astype(jnp.bfloat16)
    low = (rest - middle.astype(jnp.float32)).astype(jnp.bfloat16)
    rows = values.shape[0]
    stacked = jnp.concatenate([high, middle, low], axis=0)
    out = jnp.dot(stacked, onehot, preferred_element_type=jnp.float32)
    return (out[2 * rows :] + out[rows : 2 * rows]) + out[:rows]


def around(v):
    rows, columns = v.shape
    up = pltpu.roll(v, 1, 0)
    down = pltpu.roll(v, rows - 1, 0)
    left = pltpu.roll(v, 1, 1)
    right = pltpu.roll(v, columns - 1, 1)
    return (up + down) + (left + right)


def sweep(v, g, w):
    return (1.0 - DAMPING) * v + w * (g + around(v))


class Sizes:
    def __init__(self, rows, columns, nx, ny):
        self.rows, self.columns, self.nx, self.ny = rows, columns, nx, ny
        self.p, self.q = rows // 16, columns // 16
        self.coarse_rows, self.coarse_columns = nx * self.p, ny * self.q
        assert self.p == 8 and 8 * self.q == 128, "block shape"

        def up(n):
            return -(-n // 128) * 128

        self.ext_rows = [(rows >> l) + 2 * HALOS[l] for l in range(3)]
        self.ext_columns = [up((columns >> l) + 2 * HALOS[l]) for l in range(3)]

    def column_at(self, level):
        own, halo, width = self.columns >> level, HALOS[level], self.ext_columns[level]
        lane = np.arange(width)
        inside = (lane < own + halo) | (lane >= width - halo)
        return np.where(lane < own + halo, lane, lane - width), inside

    def restrict_columns(self, level):
        fine, fine_in = self.column_at(level)
        coarse, coarse_in = self.column_at(level + 1)
        hit = (fine[:, None] // 2 == coarse[None, :]) & fine_in[:, None] & coarse_in[None, :]
        return hit.astype(jnp.bfloat16)

    def pack_pair(self):
        width, own = self.ext_columns[1], self.columns >> 1
        x = np.arange(2 * width)
        column = x % width // 2
        target = (x // width) * (own // 2) + (column % 4) * self.q + column // 4
        hit = (target[:, None] == np.arange(own)[None, :]) & (x % width < own)[:, None]
        return hit.astype(jnp.bfloat16)

    def pack_single(self):
        x = np.arange(self.ext_columns[2])[:, None]
        lane = np.arange(128)[None, :]
        hit = (x // 2 == 2 * (lane % self.q) + (lane // self.q) % 2) & (x < self.columns >> 2)
        return hit.astype(jnp.bfloat16)

    def spread_columns(self, level):
        n = 1 << (LEVELS - level)
        column, inside = self.column_at(level - 1)
        m = column // 2
        r = np.arange(n)[:, None, None]
        lane = np.arange(128)[None, :, None]
        hit = (m % n == r) & (m // n + self.q == lane) & inside
        return hit.reshape(n * 128, -1).astype(jnp.bfloat16)


def iota(shape, axis):
    return lax.broadcasted_iota(jnp.int32, shape, axis)


def inside_mask(sizes, level, gx, gy):
    shape = (sizes.ext_rows[level], sizes.ext_columns[level])
    own_r, own_c, halo = sizes.rows >> level, sizes.columns >> level, HALOS[level]
    row, column = iota(shape, 0), iota(shape, 1)
    last_row = jnp.where(gx < sizes.nx - 1, own_r + halo, own_r)
    first_row = jnp.where(gx > 0, own_r + halo, shape[0])
    last_column = jnp.where(gy < sizes.ny - 1, own_c + halo, own_c)
    first_column = jnp.where(gy > 0, shape[1] - halo, shape[1])
    return ((row < last_row) | (row >= first_row)) & ((column < last_column) | (column >= first_column))


def pair_rows(scratch, values):
    rows, columns = values.shape
    outs = []
    for t in range(columns // 128):
        scratch[t, :rows, :] = values[:, t * 128 : (t + 1) * 128]
    for t in range(columns // 128):
        outs.append(scratch[t, pl.ds(0, rows // 2, stride=2), :] + scratch[t, pl.ds(1, rows // 2, stride=2), :])
    return jnp.concatenate(outs, axis=1)


def double_rows(scratch, values):
    rows, columns = values.shape
    for t in range(columns // 128):
        part = values[:, t * 128 : (t + 1) * 128]
        scratch[t, pl.ds(0, rows, stride=2), :] = part
        scratch[t, pl.ds(1, rows, stride=2), :] = part
    return jnp.concatenate([scratch[t, : 2 * rows, :] for t in range(columns // 128)], axis=1)


def repeat(block, out_ref):
    height = block.shape[0]
    for k in range(out_ref.shape[0] // height):
        out_ref[k * height : (k + 1) * height, :] = block


def pack_two(sizes, gy, first, second, scratch, columns_ref, out_ref):
    rows = first.shape[0]
    scratch[0, :rows, :] = f32dot_right(jnp.concatenate([first, second], axis=1), columns_ref[...])
    block = jnp.concatenate([scratch[0, pl.ds(s, sizes.p, stride=4), :] for s in range(4)], axis=0)
    repeat(pltpu.roll(block, lax.rem(gy, 8) * sizes.q, 1), out_ref)


def pack_one(sizes, gy, values, scratch, columns_ref, out_ref):
    rows = values.shape[0]
    scratch[0, :rows, :] = f32dot_right(values, columns_ref[...])
    part = iota((4, 128), 1) // (2 * sizes.q)
    block = scratch[0, pl.ds(0, 4, stride=2), :]
    for k in range(1, 4):
        block = jnp.where(part == k, scratch[0, pl.ds(8 * (k // 2) + k % 2, 4, stride=2), :], block)
    block = jnp.concatenate([block, block], axis=0)
    repeat(pltpu.roll(block, lax.rem(gy, 8) * sizes.q, 1), out_ref)


def near(values, own):
    return jnp.concatenate([values[: own + NEAR], values[values.shape[0] - NEAR :]], axis=0)


def sides(at, first_ref, second_ref):
    even = lax.rem(at, 2) == 0
    first, second = first_ref[...], second_ref[...]
    return jnp.where(even, first, second), jnp.where(even, second, first)


def strip_rows(sizes):
    groups = 128 // HALO
    return groups, -(-2 * sizes.ext_rows[0] // (8 * groups)) * 8


def fold(sizes, strip, step):
    groups, height = strip_rows(sizes)
    lane = iota((height, 128), 1)
    lane = lane if step > 0 else 127 - lane
    out = strip[:height]
    for k in range(1, groups):
        part = strip[k * height : (k + 1) * height]
        part = pltpu.roll(part, k * step % 128, 1)
        if part.shape[0] < height:
            part = jnp.concatenate([part, jnp.zeros((height - part.shape[0], 128), jnp.float32)], axis=0)
        out = jnp.where(lane >= k * HALO, part, out)
    return out


def unfold(sizes, packed, step):
    groups, _ = strip_rows(sizes)
    parts = [packed] + [pltpu.roll(packed, -k * step % 128, 1) for k in range(1, groups)]
    rows = sizes.ext_rows[0]
    out = jnp.concatenate(parts, axis=0)
    return out[:rows], out[rows : 2 * rows]


def strip_kernel(sizes, g_ref, s_ref, rows_a_ref, rows_b_ref, first_ref, second_ref):
    last = sizes.columns - 128
    even = lax.rem(lax.axis_index("gy"), 2) == 0
    below, above = sides(lax.axis_index("gx"), rows_a_ref, rows_b_ref)
    fields = (g_ref[...], below[0], above[0], s_ref[...], below[1], above[1])
    left = fold(sizes, jnp.concatenate([x[:, :128] for x in fields], axis=0), HALO)
    right = fold(sizes, jnp.concatenate([x[:, last:] for x in fields], axis=0), -HALO)
    first_ref[...] = jnp.where(even, right, left)
    second_ref[...] = jnp.where(even, left, right)


def coefficients(sizes, level, gx, gy, sigma):
    d = 4.0 + sigma
    return d, jnp.where(inside_mask(sizes, level, gx, gy), DAMPING / d, 0.0)


def down_kernel(sizes, g_ref, s_ref, rows_a_ref, rows_b_ref, columns_a_ref, columns_b_ref,
                rc0_ref, rc1_ref, pc_ref,
                g0_ref, d0_ref, w0_ref, v0_ref, c1_ref, d1_ref, w1_ref, v1_ref, d2_ref, w2_ref, out_ref, scratch):
    gx, gy = lax.axis_index("gx"), lax.axis_index("gy")
    rows = sizes.ext_rows[0]
    lane = iota((rows, 128), 1)
    below, above = sides(gx, rows_a_ref, rows_b_ref)
    from_right, from_left = sides(gy, columns_a_ref, columns_b_ref)
    from_right, from_left = unfold(sizes, from_right, HALO), unfold(sizes, from_left, -HALO)
    g = jnp.where(lane < HALO, from_right[0], from_left[0])
    sigma = jnp.where(lane < HALO, from_right[1], from_left[1])
    g = jnp.concatenate([jnp.concatenate([g_ref[...], below[0], above[0]], axis=0), g], axis=1)
    sigma = jnp.concatenate([jnp.concatenate([s_ref[...], below[1], above[1]], axis=0), sigma], axis=1)
    d, w = coefficients(sizes, 0, gx, gy, sigma)
    v = w * g
    v = sweep(v, g, w)
    r = g - d * v + around(v)
    for ref, values in ((g0_ref, g), (d0_ref, d), (w0_ref, w), (v0_ref, v)):
        ref[...] = near(values, sizes.rows)
    both = []
    own, halo = sizes.rows // 2, HALOS[1]
    for values in (r, sigma):
        pairs = pair_rows(scratch, values)
        both += [pairs[: own + halo], pairs[pairs.shape[0] - halo :]]
    both = f32dot_right(jnp.concatenate(both, axis=0), rc0_ref[...])
    half = own + 2 * halo
    g, sigma = both[:half], both[half:]
    d, w = coefficients(sizes, 1, gx, gy, sigma)
    v = w * g
    v = sweep(v, g, w)
    r = g - d * v + around(v)
    c1_ref[...] = g
    d1_ref[...] = d
    w1_ref[...] = w
    v1_ref[...] = v
    own = sizes.rows // 4
    source, sigma = pair_rows(scratch, r), pair_rows(scratch, sigma)
    pack_two(sizes, gy, source[:own], sigma[:own], scratch, pc_ref, out_ref)
    d, w = coefficients(sizes, 2, gx, gy, f32dot_right(sigma, rc1_ref[...]))
    d2_ref[...] = d
    w2_ref[...] = w


class Coarse:
    def __init__(self, sizes, first, d_refs, w_refs, g_refs, v_refs, t_refs, coarsest):
        self.z = sizes
        self.first = first
        self.d, self.w, self.g, self.v, self.t = d_refs, w_refs, g_refs, v_refs, t_refs
        self.va, self.vb, self.wk, self.gk, self.wide_v, self.wide_t, self.wide_w, self.wide_g, self.ones = coarsest
        lane = iota((sizes.p, sizes.coarse_columns), 1)
        self.first_lane, self.last_lane = lane == 0, lane == sizes.coarse_columns - 1

    def blocks(self, body):
        p = self.z.p
        if self.z.nx <= 4:
            for gx in range(self.z.nx):
                body((gx + 1) * p)
        else:
            def step(gx, carry):
                body(pl.multiple_of((gx + 1) * p, 8))
                return carry

            lax.fori_loop(0, self.z.nx, step, 0)

    def at(self, ref, s, r, base):
        return ref[s, r, pl.ds(base, self.z.p), :]

    def put(self, ref, s, r, base, value):
        ref[s, r, pl.ds(base, self.z.p), :] = value

    def beside(self, ref, s, r, base, step):
        p = self.z.p
        if isinstance(base, int):
            return ref[s, r, pl.ds(base + step, p), :]
        return ref[s, r, pl.ds(base - p, 3 * p), :][p + step : 2 * p + step]

    def neighbours(self, ref, s, r, n, base):
        columns = self.z.coarse_columns
        if r < n - 1:
            right = self.at(ref, s, r + 1, base)
        else:
            right = jnp.where(self.last_lane, 0.0, pltpu.roll(self.at(ref, s, 0, base), columns - 1, 1))
        if r > 0:
            left = self.at(ref, s, r - 1, base)
        else:
            left = jnp.where(self.first_lane, 0.0, pltpu.roll(self.at(ref, s, n - 1, base), 1, 1))
        down = self.at(ref, s + 1, r, base) if s < n - 1 else self.beside(ref, 0, r, base, 1)
        up = self.at(ref, s - 1, r, base) if s > 0 else self.beside(ref, n - 1, r, base, -1)
        return (up + down) + (left + right)

    def each(self, level, body):
        n = 1 << (LEVELS - level)

        def block(base):
            for s in range(n):
                for r in range(n):
                    body(s, r, n, base)

        self.blocks(block)

    def first_sweep(self, level):
        l = level - self.first

        def body(s, r, n, base):
            self.put(self.v[l], s, r, base, self.at(self.w[l], s, r, base) * self.at(self.g[l], s, r, base))

        self.each(level, body)

    def sweep(self, level, source, target):
        l = level - self.first

        def body(s, r, n, base):
            v = self.at(source, s, r, base)
            total = self.at(self.g[l], s, r, base) + self.neighbours(source, s, r, n, base)
            self.put(target, s, r, base, (1.0 - DAMPING) * v + self.at(self.w[l], s, r, base) * total)

        self.each(level, body)

    def two_sweeps(self, level):
        l = level - self.first
        self.sweep(level, self.v[l], self.t[l])
        self.sweep(level, self.t[l], self.v[l])

    def start(self, level):
        l = level - self.first
        self.first_sweep(level)
        self.sweep(level, self.v[l], self.t[l])
        self.v[l], self.t[l] = self.t[l], self.v[l]

    def residual(self, level, s, r, n, base):
        l = level - self.first
        v = self.at(self.v[l], s, r, base)
        g = self.at(self.g[l], s, r, base)
        return (g - self.at(self.d[l], s, r, base) * v) + self.neighbours(self.v[l], s, r, n, base)

    def restrict(self, level):
        l = level - self.first
        n = 1 << (LEVELS - level)

        def block(base):
            for s in range(n // 2):
                for r in range(n // 2):
                    parts = [self.residual(level, 2 * s + a, 2 * r + b, n, base) for a in (0, 1) for b in (0, 1)]
                    self.put(self.g[l + 1], s, r, base, (parts[0] + parts[1]) + (parts[2] + parts[3]))

        self.blocks(block)

    def prolong(self, level):
        l = level - self.first

        def body(s, r, n, base):
            e = self.at(self.v[l + 1], s // 2, r // 2, base)
            self.put(self.v[l], s, r, base, self.at(self.v[l], s, r, base) + e)

        self.each(level, body)

    def inner(self, ref, s=0, r=0):
        p = self.z.p
        return ref[s, r, p : p + self.z.coarse_rows, :]

    def shifted(self, x, k):
        if k == 0:
            return x
        columns = self.z.coarse_columns
        lane = iota(x.shape, 1)
        keep = lane < columns - k if k > 0 else lane >= -k
        return jnp.where(keep, pltpu.roll(x, -k % columns, 1), 0.0)

    def unit(self, build):
        z = self.z
        top = LEVELS - self.first
        d, w = self.inner(self.d[top]), self.inner(self.w[top])
        missing = 2.0 * (z.coarse_rows + z.coarse_columns)
        for k in range(-2, 3):
            self.wk[k + 2] = self.shifted(w, k)
        self.widen(self.w[top - 1], self.wide_w, 1, False)
        if build:
            lane = iota(d.shape, 1)
            for k in range(-3, 4):
                self.put_shifted(self.va, k, jnp.where((lane < d.shape[1] - k) & (lane >= -k), 1.0, 0.0))
            self.ones[...] = self.coarse_sweeps(False, False)
        return 1.0 / (jnp.sum(d - 4.0, keepdims=True) + missing)

    def shifted_at(self, ref, k, step=0):
        p = self.z.p
        return ref[k + 3, p + step : p + step + self.z.coarse_rows, :]

    def put_shifted(self, ref, k, value):
        ref[k + 3, self.z.p : self.z.p + self.z.coarse_rows, :] = value

    def coarse_sweeps(self, from_zero, with_source):
        at = self.shifted_at
        for turn in range(COARSE_SWEEPS // 3):
            if turn:
                for k in range(-3, 4):
                    self.put_shifted(self.va, k, self.shifted(value, k))
            source, target = self.va, self.vb
            for reach in (2, 1, 0):
                for k in range(-reach, reach + 1):
                    if from_zero and not turn and reach == 2:
                        value = self.wk[k + 2] * self.gk[k + 2]
                    else:
                        total = (at(source, k, -1) + at(source, k, 1)) + (at(source, k - 1) + at(source, k + 1))
                        if with_source:
                            total = self.gk[k + 2] + total
                        value = (1.0 - DAMPING) * at(source, k) + self.wk[k + 2] * total
                    if reach:
                        self.put_shifted(target, k, value)
                source, target = target, source
        return value

    def coarse(self, fresh, unit):
        top = LEVELS - self.first
        g = self.inner(self.g[top])
        for k in range(-2, 3):
            self.gk[k + 2] = self.shifted(g, k)
        if fresh:
            left = jnp.sum(g, keepdims=True)
        else:
            v = self.inner(self.v[top])
            for k in range(-3, 4):
                self.put_shifted(self.va, k, self.shifted(v, k))
            at = self.shifted_at
            beside = (at(self.va, 0, -1) + at(self.va, 0, 1)) + (at(self.va, -1) + at(self.va, 1))
            left = jnp.sum((g - self.inner(self.d[top]) * v) + beside, keepdims=True)
        value = self.coarse_sweeps(fresh, True)
        left = jnp.broadcast_to(left * unit, g.shape)
        self.v[top][0, 0, self.z.p : self.z.p + self.z.coarse_rows, :] = value + left * self.ones[...]

    def widen(self, source, target, reach, padded):
        rows = slice(self.z.p, self.z.p + self.z.coarse_rows) if padded else slice(None)
        for s in range(2):
            for k in range(-reach, 2 + reach):
                target[s, k + reach, rows, :] = self.shifted(self.inner(source, s, k % 2), k // 2)

    def twice(self, restricting):
        l = LEVELS - 1 - self.first
        p, height = self.z.p, self.z.coarse_rows
        rows = slice(p, p + height)

        def at(ref, s, k, step=0):
            return ref[s, k + 2, p + step : p + step + height, :]

        def beside(ref, s, k):
            up = at(ref, 0, k) if s else at(ref, 1, k, -1)
            down = at(ref, 0, k, 1) if s else at(ref, 1, k)
            return (up + down) + (at(ref, s, k - 1) + at(ref, s, k + 1))

        def swept(ref, s, k):
            total = self.wide_g[s, k + 1] + beside(ref, s, k)
            return (1.0 - DAMPING) * at(ref, s, k) + self.wide_w[s, k + 1] * total

        self.widen(self.v[l], self.wide_v, 2, True)
        for s in range(2):
            for k in range(-1, 3):
                self.wide_t[s, k + 2, rows, :] = swept(self.wide_v, s, k)
        parts = []
        for s in range(2):
            for k in range(2):
                if restricting:
                    v = at(self.wide_t, s, k)
                    self.v[l][s, k, rows, :] = v
                    left = self.wide_g[s, k + 1] - self.inner(self.d[l], s, k) * v
                    parts.append(left + beside(self.wide_t, s, k))
                else:
                    self.v[l][s, k, rows, :] = swept(self.wide_t, s, k)
        if restricting:
            self.g[l + 1][0, 0, rows, :] = (parts[0] + parts[1]) + (parts[2] + parts[3])

    def before(self, level, fresh, new_source):
        l = level - self.first
        if level < LEVELS - 1:
            if fresh:
                self.start(level)
            else:
                self.two_sweeps(level)
            self.restrict(level)
            return
        if new_source:
            self.widen(self.g[l], self.wide_g, 1, False)
        if fresh:
            self.first_sweep(level)
        else:
            self.sweep(level, self.v[l], self.t[l])
            self.v[l], self.t[l] = self.t[l], self.v[l]
        self.twice(True)

    def after(self, level):
        self.prolong(level)
        if level < LEVELS - 1:
            self.two_sweeps(level)
        else:
            self.twice(False)

    def vcycle(self, level, fresh, unit):
        if level == LEVELS:
            self.coarse(fresh, unit)
            return
        self.before(level, fresh, fresh)
        self.vcycle(level + 1, True, unit)
        self.after(level)

    def fcycle(self, level, unit):
        if level == LEVELS:
            self.coarse(True, unit)
            return
        self.before(level, True, True)
        self.fcycle(level + 1, unit)
        self.vcycle(level + 1, False, unit)
        self.after(level)

    def clear_ends(self):
        z = self.z
        zero = jnp.zeros((z.p, z.coarse_columns), jnp.float32)
        for refs in (self.v, self.t):
            for ref in refs:
                n = ref.shape[0]
                for s in range(n):
                    for r in range(n):
                        ref[s, r, : z.p, :] = zero
                        ref[s, r, z.p + z.coarse_rows :, :] = zero
        for ref in (self.va, self.vb, self.wide_v.at[0], self.wide_v.at[1], self.wide_t.at[0], self.wide_t.at[1]):
            for k in range(ref.shape[0]):
                ref[k, : z.p, :] = zero
                ref[k, z.p + z.coarse_rows :, :] = zero

    def turned(self, blocks, k):
        q = self.z.q
        part = iota(blocks[0].shape, 1) // q
        out = blocks[-k % 8]
        for x in range(1, 8):
            out = jnp.where(part == x, blocks[(x - k) % 8], out)
        return pltpu.roll(out, -k * q % 128, 1) if k else out

    def take_two(self, even_ref, odd_ref, targets):
        z = self.z
        for gx in range(z.nx):
            for group in range(z.ny // 8):
                lanes = slice(group * 128, (group + 1) * 128)
                for s in range(4):
                    blocks = []
                    for g in range(8):
                        first = (gx * (z.ny // 2) + group * 4 + g // 2) * 4 * z.p + s * z.p
                        blocks.append((even_ref, odd_ref)[g % 2][first : first + z.p, :])
                    for k in range(8):
                        target, add = targets[k // 4]
                        value = self.turned(blocks, k)
                        target[s, k % 4, (gx + 1) * z.p : (gx + 2) * z.p, lanes] = value + add if add else value

    def take_one(self, y_ref, target):
        z = self.z
        low = iota((8, 128), 0) < 4
        for gx in range(z.nx):
            for group in range(z.ny // 8):
                upper, lower = [], []
                for g in range(0, 8, 2):
                    first = (gx * z.ny + group * 8 + g) * 4
                    pair = y_ref[first : first + 8, :]
                    swapped = pltpu.roll(pair, 4, 0)
                    upper += [pair, swapped]
                    lower += [swapped, pair]
                for k in range(4):
                    value = jnp.where(low, self.turned(upper, k), self.turned(lower, k + 4))
                    target[k // 2, k % 2, (gx + 1) * z.p : (gx + 2) * z.p, group * 128 : (group + 1) * 128] = value

    def spread(self, gx, gy, columns_ref, scratch, lines):
        z = self.z
        n = 1 << (LEVELS - self.first)
        above = self.first - 1
        columns = z.coarse_columns
        turn = lax.rem(columns + z.q - gy * z.q, columns)
        start = pl.multiple_of(gx * z.p, 8)
        for s in range(n):
            for r in range(n):
                part = pltpu.roll(self.v[0][s, r, pl.ds(start, 3 * z.p), :], turn, 1)[:, :128]
                lines[r, pl.ds(s, 3 * z.p, stride=n), :] = part
        own, halo = z.rows >> self.first, HALOS[above]
        window = slice(n * z.p - 8, n * z.p + own + 8)
        wide = f32dot_right(jnp.concatenate([lines[r, window, :] for r in range(n)], axis=1), columns_ref[...])
        doubled = double_rows(scratch, jnp.concatenate([wide[8:], wide[:8]], axis=0))
        height = doubled.shape[0]
        return jnp.concatenate([doubled[: 2 * own + halo], doubled[height - halo :]], axis=0)


def level_shape(sizes, level):
    n = 1 << (LEVELS - level)
    return (n, n, sizes.coarse_rows + 2 * sizes.p, sizes.coarse_columns)


def middle_kernel(sizes, y_ref, other_ref, c1_ref, d1_ref, w1_ref, v1_ref, w2l_ref, d2l_ref, sc_ref,
                  rc1_ref, pc_ref,
                  d3_ref, d4_ref, w3_ref, w4_ref, ones_ref, e1_ref, c2_ref, e2_ref, out_ref,
                  d2, w2, g2, g3, g4, v2, v3, v4, t2, t3, t4, scratch, lines, *coarsest):
    gx, gy = lax.axis_index("gx"), lax.axis_index("gy")
    m = Coarse(sizes, 2, [d2, d3_ref, d4_ref], [w2, w3_ref, w4_ref], [g2, g3, g4], [v2, v3, v4], [t2, t3, t4], (*coarsest, ones_ref))
    m.clear_ends()
    core = lax.rem(gy, 2)

    @pl.when(core == 0)
    def _():
        m.take_two(y_ref, other_ref, ((g2, 0.0), (d2, 4.0)))

    @pl.when(core == 1)
    def _():
        m.take_two(other_ref, y_ref, ((g2, 0.0), (d2, 4.0)))

    for l in range(2):
        n = 2 >> l

        def block(base):
            for s in range(n):
                for r in range(n):
                    parts = [m.at(m.d[l], 2 * s + a, 2 * r + b, base) for a in (0, 1) for b in (0, 1)]
                    m.put(m.d[l + 1], s, r, base, ((parts[0] + parts[1]) + (parts[2] + parts[3])) - 12.0)

        m.blocks(block)
    for l in range(3):
        def body(s, r, n, base):
            m.put(m.w[l], s, r, base, DAMPING / m.at(m.d[l], s, r, base))

        m.each(l + 2, body)
    unit = m.unit(True)
    m.fcycle(2, unit)
    m.vcycle(2, False, unit)
    g, d, w = c1_ref[...], d1_ref[...], w1_ref[...]
    v = v1_ref[...] + jnp.where(w > 0.0, m.spread(gx, gy, sc_ref, scratch, lines), 0.0)
    for _ in range(4):
        v = sweep(v, g, w)
    e1_ref[...] = v
    r = g - d * v + around(v)
    g = f32dot_right(pair_rows(scratch, r), rc1_ref[...])
    d, w = d2l_ref[...], w2l_ref[...]
    v = w * g
    v = sweep(v, g, w)
    r = g - d * v + around(v)
    c2_ref[...] = g
    e2_ref[...] = v
    pack_one(sizes, gy, pair_rows(scratch, r[: sizes.rows // 4]), scratch, pc_ref, out_ref)


def up_kernel(sizes, y_ref, d3_ref, d4_ref, w3_ref, w4_ref, ones_ref, c2_ref, w2_ref, e2_ref, c1_ref, w1_ref, e1_ref,
              g0_ref, d0_ref, w0_ref, v0_ref, sc_ref, pc1_ref, pc0_ref,
              solution_ref, residual_ref, g3, g4, v3, v4, t3, t4, scratch, lines, *coarsest):
    gx, gy = lax.axis_index("gx"), lax.axis_index("gy")
    m = Coarse(sizes, 3, [d3_ref, d4_ref], [w3_ref, w4_ref], [g3, g4], [v3, v4], [t3, t4], (*coarsest, ones_ref))
    m.clear_ends()
    m.take_one(y_ref, g3)
    m.vcycle(3, True, m.unit(False))
    g, w = c2_ref[...], w2_ref[...]
    v = e2_ref[...] + jnp.where(w > 0.0, m.spread(gx, gy, sc_ref, scratch, lines), 0.0)
    for _ in range(2):
        v = sweep(v, g, w)
    own = sizes.rows // 2
    g, w = near(c1_ref, own), near(w1_ref, own)
    v = near(e1_ref, own) + near(double_rows(scratch, f32dot_right(v, pc1_ref[...])), own)
    for _ in range(2):
        v = sweep(v, g, w)
    g, d, w = g0_ref[...], d0_ref[...], w0_ref[...]
    v = v0_ref[...] + near(double_rows(scratch, f32dot_right(v, pc0_ref[...])), sizes.rows)
    for _ in range(2):
        v = sweep(v, g, w)
    r = g - d * v + around(v)
    solution_ref[...] = v[: sizes.rows, : sizes.columns]
    residual_ref[...] = r[: sizes.rows, : sizes.columns]


def vmem(count):
    return [pl.BlockSpec(memory_space=pltpu.VMEM)] * count


def call(kernel, sizes, outs, scratch, *operands):
    shapes = [jax.ShapeDtypeStruct(shape, jnp.float32) for shape in outs]
    used = sum(4 * int(np.prod(shape)) for shape in list(outs) + list(scratch))
    used += sum(x.size * x.dtype.itemsize for x in operands)
    return pl.pallas_call(
        lambda *refs: kernel(sizes, *refs),
        out_shape=shapes,
        in_specs=vmem(len(operands)),
        out_specs=vmem(len(outs)),
        scratch_shapes=[pltpu.VMEM(shape, jnp.float32) for shape in scratch],
        compiler_params=pltpu.CompilerParams(vmem_limit_bytes=used + used // 4 + (4 << 20)),
    )(*operands)


def swaps(first, second, axis, spare):
    nx, ny = lax.axis_size("gx"), lax.axis_size("gy")
    count = lax.axis_size(axis)

    def target(gx, gy):
        place = gx if axis == "gx" else gy
        if place in (0, count - 1):
            return (gx ^ 1) * ny + gy if spare == "gx" else gx * ny + (gy ^ 1)
        place = place + 1 if place % 2 else place - 1
        return place * ny + gy if axis == "gx" else gx * ny + place

    pairs = [(gx * ny + gy, target(gx, gy)) for gx in range(nx) for gy in range(ny)]
    other = lax.ppermute(second, ("gx", "gy"), pairs)
    return lax.ppermute(first, axis, [(i, i ^ 1) for i in range(count)]), other


def gather(copies):
    return lax.all_to_all(copies, ("gx", "gy"), 0, 0, tiled=True)


def gather_by_core(copies, nx, ny):
    index = np.arange(nx * ny)
    groups = [index[core::2].tolist() for core in range(2)]
    own = lax.all_to_all(copies, ("gx", "gy"), 0, 0, tiled=True, axis_index_groups=groups)
    return own, lax.ppermute(own, "gy", [(j, j ^ 1) for j in range(ny)])


def body(right_side, shift):
    nx, ny = lax.axis_size("gx"), lax.axis_size("gy")
    rows, columns = right_side.shape
    z = Sizes(rows, columns, nx, ny)
    even = lax.axis_index("gx") % 2 == 0
    last = rows - HALO

    def strips(start, fields):
        return jnp.stack([lax.dynamic_slice(x, (start, 0), (HALO, columns)) for x in fields])

    fields = (right_side, shift)
    later = lax.optimization_barrier(fields)
    rows_a, rows_b = swaps(
        strips(jnp.where(even, last, 0), later), strips(jnp.where(even, 0, last), fields), "gx", "gy")
    ext = [(z.ext_rows[l], z.ext_columns[l]) for l in range(3)]
    strip = (strip_rows(z)[1], 128)
    first, second = call(strip_kernel, z, [strip] * 2, [], right_side, shift, rows_a, rows_b)
    columns_a, columns_b = swaps(first, second, "gy", "gx")
    rc0, rc1 = z.restrict_columns(0), z.restrict_columns(1)
    tiles = (ext[0][1] // 128, ext[0][0], 128)
    g0, d0, w0, v0, c1, d1, w1, v1, d2, w2, packed = call(
        down_kernel, z, [(rows + 2 * NEAR, ext[0][1])] * 4 + [ext[1]] * 4 + [ext[2]] * 2 + [(nx * ny // 2 * 4 * z.p, 128)], [tiles],
        right_side, shift, rows_a, rows_b, columns_a, columns_b, rc0, rc1, z.pack_pair())
    y, other = gather_by_core(packed, nx, ny)
    slabs = [level_shape(z, level) for level in (2, 3, 4)]
    padded, plain = slabs[2][2:], (z.coarse_rows, z.coarse_columns)
    coarsest = [(7,) + padded] * 2 + [(5,) + plain] * 2 + [(2, 6) + padded] * 2 + [(2, 4) + plain] * 2
    d3, d4, w3, w4, ones, e1, c2, e2, packed = call(
        middle_kernel, z, slabs[1:] * 2 + [plain, ext[1], ext[2], ext[2], (nx * ny * 4, 128)],
        [slabs[0]] * 2 + slabs * 3 + [tiles, (4, 12 * z.p, 128)] + coarsest,
        y, other, c1, d1, w1, v1, w2, d2, z.spread_columns(2),
        rc1, z.pack_single())
    y = gather(packed)
    return call(
        up_kernel, z, [(rows, columns)] * 2, slabs[1:] * 3 + [tiles, (2, 6 * z.p, 128)] + coarsest,
        y, d3, d4, w3, w4, ones, c2, w2, e2, c1, w1, e1, g0, d0, w0, v0,
        z.spread_columns(3), rc1.T, rc0.T)


def solution(mesh):
    specs = (P("gx", "gy"), P("gx", "gy"))

    def run(right_side, shift):
        out = body(right_side, shift)
        return out[0], out[1]

    return jax.shard_map(run, mesh=mesh, in_specs=specs, out_specs=specs, check_vma=False)
```

```python
import numpy as np
import jax
import jax.numpy as jnp
from jax import lax
from jax.experimental import pallas as pl
from jax.experimental.pallas import tpu as pltpu
from jax.sharding import PartitionSpec as P

LEVELS = 4
COARSE_SWEEPS = 6
DAMPING = 0.8
HALOS = (40, 16, 8)
HALO = HALOS[0]
NEAR = 8


def f32dot_right(values, onehot):
    high = values.astype(jnp.bfloat16)
    rest = values - high.astype(jnp.float32)
    middle = rest.astype(jnp.bfloat16)
    low = (rest - middle.astype(jnp.float32)).astype(jnp.bfloat16)
    rows = values.shape[0]
    stacked = jnp.concatenate([high, middle, low], axis=0)
    out = jnp.dot(stacked, onehot, preferred_element_type=jnp.float32)
    return (out[2 * rows :] + out[rows : 2 * rows]) + out[:rows]


def restrict_right(values, onehot):
    high = values.astype(jnp.bfloat16)
    middle = (values - high.astype(jnp.float32)).astype(jnp.bfloat16)
    rows = values.shape[0]
    out = jnp.dot(jnp.concatenate([high, middle], axis=0), onehot, preferred_element_type=jnp.float32)
    return out[rows:] + out[:rows]


def around(v):
    rows, columns = v.shape
    up = pltpu.roll(v, 1, 0)
    down = pltpu.roll(v, rows - 1, 0)
    left = pltpu.roll(v, 1, 1)
    right = pltpu.roll(v, columns - 1, 1)
    return (up + down) + (left + right)


def sweep(v, g, w):
    return (1.0 - DAMPING) * v + w * (g + around(v))


class Sizes:
    def __init__(self, rows, columns, nx, ny):
        self.rows, self.columns, self.nx, self.ny = rows, columns, nx, ny
        self.p, self.q = rows // 16, columns // 16
        self.coarse_rows, self.coarse_columns = nx * self.p, ny * self.q
        assert self.p == 8 and 8 * self.q == 128, "block shape"

        def up(n):
            return -(-n // 128) * 128

        self.ext_rows = [(rows >> l) + 2 * HALOS[l] for l in range(3)]
        self.ext_columns = [up((columns >> l) + 2 * HALOS[l]) for l in range(3)]

    def column_at(self, level):
        own, halo, width = self.columns >> level, HALOS[level], self.ext_columns[level]
        lane = np.arange(width)
        inside = (lane < own + halo) | (lane >= width - halo)
        return np.where(lane < own + halo, lane, lane - width), inside

    def restrict_columns(self, level):
        fine, fine_in = self.column_at(level)
        coarse, coarse_in = self.column_at(level + 1)
        hit = (fine[:, None] // 2 == coarse[None, :]) & fine_in[:, None] & coarse_in[None, :]
        return hit.astype(jnp.bfloat16)

    def pack_pair(self):
        width, own = self.ext_columns[1], self.columns >> 1
        x = np.arange(2 * width)
        column = x % width // 2
        target = (x // width) * (own // 2) + (column % 4) * self.q + column // 4
        hit = (target[:, None] == np.arange(own)[None, :]) & (x % width < own)[:, None]
        return hit.astype(jnp.bfloat16)

    def pack_single(self):
        x = np.arange(self.ext_columns[2])[:, None]
        lane = np.arange(128)[None, :]
        hit = (x // 2 == 2 * (lane % self.q) + (lane // self.q) % 2) & (x < self.columns >> 2)
        return hit.astype(jnp.bfloat16)

    def spread_columns(self, level):
        n = 1 << (LEVELS - level)
        column, inside = self.column_at(level - 1)
        m = column // 2
        r = np.arange(n)[:, None, None]
        lane = np.arange(128)[None, :, None]
        hit = (m % n == r) & (m // n + self.q == lane) & inside
        return hit.reshape(n * 128, -1).astype(jnp.bfloat16)


def iota(shape, axis):
    return lax.broadcasted_iota(jnp.int32, shape, axis)


def inside_mask(sizes, level, gx, gy):
    shape = (sizes.ext_rows[level], sizes.ext_columns[level])
    own_r, own_c, halo = sizes.rows >> level, sizes.columns >> level, HALOS[level]
    row, column = iota(shape, 0), iota(shape, 1)
    last_row = jnp.where(gx < sizes.nx - 1, own_r + halo, own_r)
    first_row = jnp.where(gx > 0, own_r + halo, shape[0])
    last_column = jnp.where(gy < sizes.ny - 1, own_c + halo, own_c)
    first_column = jnp.where(gy > 0, shape[1] - halo, shape[1])
    return ((row < last_row) | (row >= first_row)) & ((column < last_column) | (column >= first_column))


def pair_rows(scratch, values):
    rows, columns = values.shape
    outs = []
    for t in range(columns // 128):
        scratch[t, :rows, :] = values[:, t * 128 : (t + 1) * 128]
    for t in range(columns // 128):
        outs.append(scratch[t, pl.ds(0, rows // 2, stride=2), :] + scratch[t, pl.ds(1, rows // 2, stride=2), :])
    return jnp.concatenate(outs, axis=1)


def double_rows(scratch, values):
    rows, columns = values.shape
    for t in range(columns // 128):
        part = values[:, t * 128 : (t + 1) * 128]
        scratch[t, pl.ds(0, rows, stride=2), :] = part
        scratch[t, pl.ds(1, rows, stride=2), :] = part
    return jnp.concatenate([scratch[t, : 2 * rows, :] for t in range(columns // 128)], axis=1)


def repeat(block, out_ref):
    height = block.shape[0]
    for k in range(out_ref.shape[0] // height):
        out_ref[k * height : (k + 1) * height, :] = block


def pack_two(sizes, gy, first, second, scratch, columns_ref, out_ref):
    rows = first.shape[0]
    scratch[0, :rows, :] = restrict_right(jnp.concatenate([first, second], axis=1), columns_ref[...])
    block = jnp.concatenate([scratch[0, pl.ds(s, sizes.p, stride=4), :] for s in range(4)], axis=0)
    repeat(pltpu.roll(block, lax.rem(gy, 8) * sizes.q, 1), out_ref)


def pack_one(sizes, gy, values, scratch, columns_ref, out_ref):
    rows = values.shape[0]
    scratch[0, :rows, :] = restrict_right(values, columns_ref[...])
    part = iota((4, 128), 1) // (2 * sizes.q)
    block = scratch[0, pl.ds(0, 4, stride=2), :]
    for k in range(1, 4):
        block = jnp.where(part == k, scratch[0, pl.ds(8 * (k // 2) + k % 2, 4, stride=2), :], block)
    block = jnp.concatenate([block, block], axis=0)
    repeat(pltpu.roll(block, lax.rem(gy, 8) * sizes.q, 1), out_ref)


def near(values, own):
    return jnp.concatenate([values[: own + NEAR], values[values.shape[0] - NEAR :]], axis=0)


def sides(at, first_ref, second_ref):
    even = lax.rem(at, 2) == 0
    first, second = first_ref[...], second_ref[...]
    return jnp.where(even, first, second), jnp.where(even, second, first)


def strip_rows(sizes):
    groups = 128 // HALO
    return groups, -(-2 * sizes.ext_rows[0] // (8 * groups)) * 8


def fold(sizes, strip, step):
    groups, height = strip_rows(sizes)
    lane = iota((height, 128), 1)
    lane = lane if step > 0 else 127 - lane
    out = strip[:height]
    for k in range(1, groups):
        part = strip[k * height : (k + 1) * height]
        part = pltpu.roll(part, k * step % 128, 1)
        if part.shape[0] < height:
            part = jnp.concatenate([part, jnp.zeros((height - part.shape[0], 128), jnp.float32)], axis=0)
        out = jnp.where(lane >= k * HALO, part, out)
    return out


def unfold(sizes, packed, step):
    groups, _ = strip_rows(sizes)
    parts = [packed] + [pltpu.roll(packed, -k * step % 128, 1) for k in range(1, groups)]
    rows = sizes.ext_rows[0]
    out = jnp.concatenate(parts, axis=0)
    return out[:rows], out[rows : 2 * rows]


def strip_kernel(sizes, g_ref, s_ref, rows_a_ref, rows_b_ref, first_ref, second_ref):
    last = sizes.columns - 128
    even = lax.rem(lax.axis_index("gy"), 2) == 0
    below, above = sides(lax.axis_index("gx"), rows_a_ref, rows_b_ref)
    fields = (g_ref[...], below[0], above[0], s_ref[...], below[1], above[1])
    left = fold(sizes, jnp.concatenate([x[:, :128] for x in fields], axis=0), HALO)
    right = fold(sizes, jnp.concatenate([x[:, last:] for x in fields], axis=0), -HALO)
    first_ref[...] = jnp.where(even, right, left)
    second_ref[...] = jnp.where(even, left, right)


def coefficients(sizes, level, gx, gy, sigma):
    d = 4.0 + sigma
    return d, jnp.where(inside_mask(sizes, level, gx, gy), DAMPING / d, 0.0)


def down_kernel(sizes, g_ref, s_ref, rows_a_ref, rows_b_ref, columns_a_ref, columns_b_ref,
                rc0_ref, rc1_ref, pc_ref,
                g0_ref, d0_ref, w0_ref, v0_ref, c1_ref, d1_ref, w1_ref, v1_ref, d2_ref, w2_ref, out_ref, scratch):
    gx, gy = lax.axis_index("gx"), lax.axis_index("gy")
    rows = sizes.ext_rows[0]
    lane = iota((rows, 128), 1)
    below, above = sides(gx, rows_a_ref, rows_b_ref)
    from_right, from_left = sides(gy, columns_a_ref, columns_b_ref)
    from_right, from_left = unfold(sizes, from_right, HALO), unfold(sizes, from_left, -HALO)
    g = jnp.where(lane < HALO, from_right[0], from_left[0])
    sigma = jnp.where(lane < HALO, from_right[1], from_left[1])
    g = jnp.concatenate([jnp.concatenate([g_ref[...], below[0], above[0]], axis=0), g], axis=1)
    sigma = jnp.concatenate([jnp.concatenate([s_ref[...], below[1], above[1]], axis=0), sigma], axis=1)
    d, w = coefficients(sizes, 0, gx, gy, sigma)
    v = w * g
    v = sweep(v, g, w)
    r = g - d * v + around(v)
    for ref, values in ((g0_ref, g), (d0_ref, d), (w0_ref, w), (v0_ref, v)):
        ref[...] = near(values, sizes.rows)
    both = []
    own, halo = sizes.rows // 2, HALOS[1]
    for values in (r, sigma):
        pairs = pair_rows(scratch, values)
        both += [pairs[: own + halo], pairs[pairs.shape[0] - halo :]]
    both = restrict_right(jnp.concatenate(both, axis=0), rc0_ref[...])
    half = own + 2 * halo
    g, sigma = both[:half], both[half:]
    d, w = coefficients(sizes, 1, gx, gy, sigma)
    v = w * g
    v = sweep(v, g, w)
    r = g - d * v + around(v)
    c1_ref[...] = g
    d1_ref[...] = d
    w1_ref[...] = w
    v1_ref[...] = v
    own = sizes.rows // 4
    source, sigma = pair_rows(scratch, r), pair_rows(scratch, sigma)
    pack_two(sizes, gy, source[:own], sigma[:own], scratch, pc_ref, out_ref)
    d, w = coefficients(sizes, 2, gx, gy, restrict_right(sigma, rc1_ref[...]))
    d2_ref[...] = d
    w2_ref[...] = w


class Coarse:
    def __init__(self, sizes, first, d_refs, w_refs, g_refs, v_refs, t_refs, coarsest):
        self.z = sizes
        self.first = first
        self.d, self.w, self.g, self.v, self.t = d_refs, w_refs, g_refs, v_refs, t_refs
        self.va, self.vb, self.wk, self.gk, self.wide_v, self.wide_t, self.wide_w, self.wide_g, self.ones = coarsest
        lane = iota((sizes.p, sizes.coarse_columns), 1)
        self.first_lane, self.last_lane = lane == 0, lane == sizes.coarse_columns - 1

    def blocks(self, body):
        p = self.z.p
        if self.z.nx <= 4:
            for gx in range(self.z.nx):
                body((gx + 1) * p)
        else:
            def step(gx, carry):
                body(pl.multiple_of((gx + 1) * p, 8))
                return carry

            lax.fori_loop(0, self.z.nx, step, 0)

    def at(self, ref, s, r, base):
        return ref[s, r, pl.ds(base, self.z.p), :]

    def put(self, ref, s, r, base, value):
        ref[s, r, pl.ds(base, self.z.p), :] = value

    def beside(self, ref, s, r, base, step):
        p = self.z.p
        if isinstance(base, int):
            return ref[s, r, pl.ds(base + step, p), :]
        return ref[s, r, pl.ds(base - p, 3 * p), :][p + step : 2 * p + step]

    def neighbours(self, ref, s, r, n, base):
        columns = self.z.coarse_columns
        if r < n - 1:
            right = self.at(ref, s, r + 1, base)
        else:
            right = jnp.where(self.last_lane, 0.0, pltpu.roll(self.at(ref, s, 0, base), columns - 1, 1))
        if r > 0:
            left = self.at(ref, s, r - 1, base)
        else:
            left = jnp.where(self.first_lane, 0.0, pltpu.roll(self.at(ref, s, n - 1, base), 1, 1))
        down = self.at(ref, s + 1, r, base) if s < n - 1 else self.beside(ref, 0, r, base, 1)
        up = self.at(ref, s - 1, r, base) if s > 0 else self.beside(ref, n - 1, r, base, -1)
        return (up + down) + (left + right)

    def each(self, level, body):
        n = 1 << (LEVELS - level)

        def block(base):
            for s in range(n):
                for r in range(n):
                    body(s, r, n, base)

        self.blocks(block)

    def first_sweep(self, level):
        l = level - self.first

        def body(s, r, n, base):
            self.put(self.v[l], s, r, base, self.at(self.w[l], s, r, base) * self.at(self.g[l], s, r, base))

        self.each(level, body)

    def sweep(self, level, source, target):
        l = level - self.first

        def body(s, r, n, base):
            v = self.at(source, s, r, base)
            total = self.at(self.g[l], s, r, base) + self.neighbours(source, s, r, n, base)
            self.put(target, s, r, base, (1.0 - DAMPING) * v + self.at(self.w[l], s, r, base) * total)

        self.each(level, body)

    def two_sweeps(self, level):
        l = level - self.first
        self.sweep(level, self.v[l], self.t[l])
        self.sweep(level, self.t[l], self.v[l])

    def start(self, level):
        l = level - self.first
        self.first_sweep(level)
        self.sweep(level, self.v[l], self.t[l])
        self.v[l], self.t[l] = self.t[l], self.v[l]

    def residual(self, level, s, r, n, base):
        l = level - self.first
        v = self.at(self.v[l], s, r, base)
        g = self.at(self.g[l], s, r, base)
        return (g - self.at(self.d[l], s, r, base) * v) + self.neighbours(self.v[l], s, r, n, base)

    def restrict(self, level):
        l = level - self.first
        n = 1 << (LEVELS - level)

        def block(base):
            for s in range(n // 2):
                for r in range(n // 2):
                    parts = [self.residual(level, 2 * s + a, 2 * r + b, n, base) for a in (0, 1) for b in (0, 1)]
                    self.put(self.g[l + 1], s, r, base, (parts[0] + parts[1]) + (parts[2] + parts[3]))

        self.blocks(block)

    def prolong(self, level):
        l = level - self.first

        def body(s, r, n, base):
            e = self.at(self.v[l + 1], s // 2, r // 2, base)
            self.put(self.v[l], s, r, base, self.at(self.v[l], s, r, base) + e)

        self.each(level, body)

    def inner(self, ref, s=0, r=0):
        p = self.z.p
        return ref[s, r, p : p + self.z.coarse_rows, :]

    def shifted(self, x, k):
        if k == 0:
            return x
        columns = self.z.coarse_columns
        lane = iota(x.shape, 1)
        keep = lane < columns - k if k > 0 else lane >= -k
        return jnp.where(keep, pltpu.roll(x, -k % columns, 1), 0.0)

    def unit(self, build):
        z = self.z
        top = LEVELS - self.first
        d, w = self.inner(self.d[top]), self.inner(self.w[top])
        missing = 2.0 * (z.coarse_rows + z.coarse_columns)
        for k in range(-2, 3):
            self.wk[k + 2] = self.shifted(w, k)
        self.widen(self.w[top - 1], self.wide_w, 1, False)
        if build:
            lane = iota(d.shape, 1)
            for k in range(-3, 4):
                self.put_shifted(self.va, k, jnp.where((lane < d.shape[1] - k) & (lane >= -k), 1.0, 0.0))
            self.ones[...] = self.coarse_sweeps(False, False)
        return 1.0 / (jnp.sum(d - 4.0, keepdims=True) + missing)

    def shifted_at(self, ref, k, step=0):
        p = self.z.p
        return ref[k + 3, p + step : p + step + self.z.coarse_rows, :]

    def put_shifted(self, ref, k, value):
        ref[k + 3, self.z.p : self.z.p + self.z.coarse_rows, :] = value

    def coarse_sweeps(self, from_zero, with_source):
        at = self.shifted_at
        for turn in range(COARSE_SWEEPS // 3):
            if turn:
                for k in range(-3, 4):
                    self.put_shifted(self.va, k, self.shifted(value, k))
            source, target = self.va, self.vb
            for reach in (2, 1, 0):
                for k in range(-reach, reach + 1):
                    if from_zero and not turn and reach == 2:
                        value = self.wk[k + 2] * self.gk[k + 2]
                    else:
                        total = (at(source, k, -1) + at(source, k, 1)) + (at(source, k - 1) + at(source, k + 1))
                        if with_source:
                            total = self.gk[k + 2] + total
                        value = (1.0 - DAMPING) * at(source, k) + self.wk[k + 2] * total
                    if reach:
                        self.put_shifted(target, k, value)
                source, target = target, source
        return value

    def coarse(self, fresh, unit):
        top = LEVELS - self.first
        g = self.inner(self.g[top])
        for k in range(-2, 3):
            self.gk[k + 2] = self.shifted(g, k)
        if fresh:
            left = jnp.sum(g, keepdims=True)
        else:
            v = self.inner(self.v[top])
            for k in range(-3, 4):
                self.put_shifted(self.va, k, self.shifted(v, k))
            at = self.shifted_at
            beside = (at(self.va, 0, -1) + at(self.va, 0, 1)) + (at(self.va, -1) + at(self.va, 1))
            left = jnp.sum((g - self.inner(self.d[top]) * v) + beside, keepdims=True)
        value = self.coarse_sweeps(fresh, True)
        left = jnp.broadcast_to(left * unit, g.shape)
        self.v[top][0, 0, self.z.p : self.z.p + self.z.coarse_rows, :] = value + left * self.ones[...]

    def widen(self, source, target, reach, padded):
        rows = slice(self.z.p, self.z.p + self.z.coarse_rows) if padded else slice(None)
        for s in range(2):
            for k in range(-reach, 2 + reach):
                target[s, k + reach, rows, :] = self.shifted(self.inner(source, s, k % 2), k // 2)

    def twice(self, restricting):
        l = LEVELS - 1 - self.first
        p, height = self.z.p, self.z.coarse_rows
        rows = slice(p, p + height)

        def at(ref, s, k, step=0):
            return ref[s, k + 2, p + step : p + step + height, :]

        def beside(ref, s, k):
            up = at(ref, 0, k) if s else at(ref, 1, k, -1)
            down = at(ref, 0, k, 1) if s else at(ref, 1, k)
            return (up + down) + (at(ref, s, k - 1) + at(ref, s, k + 1))

        def swept(ref, s, k):
            total = self.wide_g[s, k + 1] + beside(ref, s, k)
            return (1.0 - DAMPING) * at(ref, s, k) + self.wide_w[s, k + 1] * total

        self.widen(self.v[l], self.wide_v, 2, True)
        for s in range(2):
            for k in range(-1, 3):
                self.wide_t[s, k + 2, rows, :] = swept(self.wide_v, s, k)
        parts = []
        for s in range(2):
            for k in range(2):
                if restricting:
                    v = at(self.wide_t, s, k)
                    self.v[l][s, k, rows, :] = v
                    left = self.wide_g[s, k + 1] - self.inner(self.d[l], s, k) * v
                    parts.append(left + beside(self.wide_t, s, k))
                else:
                    self.v[l][s, k, rows, :] = swept(self.wide_t, s, k)
        if restricting:
            self.g[l + 1][0, 0, rows, :] = (parts[0] + parts[1]) + (parts[2] + parts[3])

    def before(self, level, fresh, new_source):
        l = level - self.first
        if level < LEVELS - 1:
            if fresh:
                self.start(level)
            else:
                self.two_sweeps(level)
            self.restrict(level)
            return
        if new_source:
            self.widen(self.g[l], self.wide_g, 1, False)
        if fresh:
            self.first_sweep(level)
        else:
            self.sweep(level, self.v[l], self.t[l])
            self.v[l], self.t[l] = self.t[l], self.v[l]
        self.twice(True)

    def after(self, level):
        self.prolong(level)
        if level < LEVELS - 1:
            self.two_sweeps(level)
        else:
            self.twice(False)

    def vcycle(self, level, fresh, unit):
        if level == LEVELS:
            self.coarse(fresh, unit)
            return
        self.before(level, fresh, fresh)
        self.vcycle(level + 1, True, unit)
        self.after(level)

    def fcycle(self, level, unit):
        if level == LEVELS:
            self.coarse(True, unit)
            return
        self.before(level, True, True)
        self.fcycle(level + 1, unit)
        self.vcycle(level + 1, False, unit)
        self.after(level)

    def clear_ends(self):
        z = self.z
        zero = jnp.zeros((z.p, z.coarse_columns), jnp.float32)
        for refs in (self.v, self.t):
            for ref in refs:
                n = ref.shape[0]
                for s in range(n):
                    for r in range(n):
                        ref[s, r, : z.p, :] = zero
                        ref[s, r, z.p + z.coarse_rows :, :] = zero
        for ref in (self.va, self.vb, self.wide_v.at[0], self.wide_v.at[1], self.wide_t.at[0], self.wide_t.at[1]):
            for k in range(ref.shape[0]):
                ref[k, : z.p, :] = zero
                ref[k, z.p + z.coarse_rows :, :] = zero

    def turned(self, blocks, k):
        q = self.z.q
        part = iota(blocks[0].shape, 1) // q
        out = blocks[-k % 8]
        for x in range(1, 8):
            out = jnp.where(part == x, blocks[(x - k) % 8], out)
        return pltpu.roll(out, -k * q % 128, 1) if k else out

    def take_two(self, even_ref, odd_ref, targets):
        z = self.z
        for gx in range(z.nx):
            for group in range(z.ny // 8):
                lanes = slice(group * 128, (group + 1) * 128)
                for s in range(4):
                    blocks = []
                    for g in range(8):
                        first = (gx * (z.ny // 2) + group * 4 + g // 2) * 4 * z.p + s * z.p
                        blocks.append((even_ref, odd_ref)[g % 2][first : first + z.p, :])
                    for k in range(8):
                        target, add = targets[k // 4]
                        value = self.turned(blocks, k)
                        target[s, k % 4, (gx + 1) * z.p : (gx + 2) * z.p, lanes] = value + add if add else value

    def take_one(self, y_ref, target):
        z = self.z
        low = iota((8, 128), 0) < 4
        for gx in range(z.nx):
            for group in range(z.ny // 8):
                upper, lower = [], []
                for g in range(0, 8, 2):
                    first = (gx * z.ny + group * 8 + g) * 4
                    pair = y_ref[first : first + 8, :]
                    swapped = pltpu.roll(pair, 4, 0)
                    upper += [pair, swapped]
                    lower += [swapped, pair]
                for k in range(4):
                    value = jnp.where(low, self.turned(upper, k), self.turned(lower, k + 4))
                    target[k // 2, k % 2, (gx + 1) * z.p : (gx + 2) * z.p, group * 128 : (group + 1) * 128] = value

    def spread(self, gx, gy, columns_ref, scratch, lines):
        z = self.z
        n = 1 << (LEVELS - self.first)
        above = self.first - 1
        columns = z.coarse_columns
        turn = lax.rem(columns + z.q - gy * z.q, columns)
        start = pl.multiple_of(gx * z.p, 8)
        for s in range(n):
            for r in range(n):
                part = pltpu.roll(self.v[0][s, r, pl.ds(start, 3 * z.p), :], turn, 1)[:, :128]
                lines[r, pl.ds(s, 3 * z.p, stride=n), :] = part
        own, halo = z.rows >> self.first, HALOS[above]
        window = slice(n * z.p - 8, n * z.p + own + 8)
        wide = f32dot_right(jnp.concatenate([lines[r, window, :] for r in range(n)], axis=1), columns_ref[...])
        doubled = double_rows(scratch, jnp.concatenate([wide[8:], wide[:8]], axis=0))
        height = doubled.shape[0]
        return jnp.concatenate([doubled[: 2 * own + halo], doubled[height - halo :]], axis=0)


def level_shape(sizes, level):
    n = 1 << (LEVELS - level)
    return (n, n, sizes.coarse_rows + 2 * sizes.p, sizes.coarse_columns)


def middle_kernel(sizes, y_ref, other_ref, c1_ref, d1_ref, w1_ref, v1_ref, w2l_ref, d2l_ref, sc_ref,
                  rc1_ref, pc_ref,
                  d3_ref, d4_ref, w3_ref, w4_ref, ones_ref, e1_ref, c2_ref, e2_ref, out_ref,
                  d2, w2, g2, g3, g4, v2, v3, v4, t2, t3, t4, scratch, lines, *coarsest):
    gx, gy = lax.axis_index("gx"), lax.axis_index("gy")
    m = Coarse(sizes, 2, [d2, d3_ref, d4_ref], [w2, w3_ref, w4_ref], [g2, g3, g4], [v2, v3, v4], [t2, t3, t4], (*coarsest, ones_ref))
    m.clear_ends()
    core = lax.rem(gy, 2)

    @pl.when(core == 0)
    def _():
        m.take_two(y_ref, other_ref, ((g2, 0.0), (d2, 4.0)))

    @pl.when(core == 1)
    def _():
        m.take_two(other_ref, y_ref, ((g2, 0.0), (d2, 4.0)))

    for l in range(2):
        n = 2 >> l

        def block(base):
            for s in range(n):
                for r in range(n):
                    parts = [m.at(m.d[l], 2 * s + a, 2 * r + b, base) for a in (0, 1) for b in (0, 1)]
                    m.put(m.d[l + 1], s, r, base, ((parts[0] + parts[1]) + (parts[2] + parts[3])) - 12.0)

        m.blocks(block)
    for l in range(3):
        def body(s, r, n, base):
            m.put(m.w[l], s, r, base, DAMPING / m.at(m.d[l], s, r, base))

        m.each(l + 2, body)
    unit = m.unit(True)
    m.fcycle(2, unit)
    m.vcycle(2, False, unit)
    g, d, w = c1_ref[...], d1_ref[...], w1_ref[...]
    v = v1_ref[...] + jnp.where(w > 0.0, m.spread(gx, gy, sc_ref, scratch, lines), 0.0)
    for _ in range(4):
        v = sweep(v, g, w)
    e1_ref[...] = v
    r = g - d * v + around(v)
    g = restrict_right(pair_rows(scratch, r), rc1_ref[...])
    d, w = d2l_ref[...], w2l_ref[...]
    v = w * g
    v = sweep(v, g, w)
    r = g - d * v + around(v)
    c2_ref[...] = g
    e2_ref[...] = v
    pack_one(sizes, gy, pair_rows(scratch, r[: sizes.rows // 4]), scratch, pc_ref, out_ref)


def up_kernel(sizes, y_ref, d3_ref, d4_ref, w3_ref, w4_ref, ones_ref, c2_ref, w2_ref, e2_ref, c1_ref, w1_ref, e1_ref,
              g0_ref, d0_ref, w0_ref, v0_ref, sc_ref, pc1_ref, pc0_ref,
              solution_ref, residual_ref, g3, g4, v3, v4, t3, t4, scratch, lines, *coarsest):
    gx, gy = lax.axis_index("gx"), lax.axis_index("gy")
    m = Coarse(sizes, 3, [d3_ref, d4_ref], [w3_ref, w4_ref], [g3, g4], [v3, v4], [t3, t4], (*coarsest, ones_ref))
    m.clear_ends()
    m.take_one(y_ref, g3)
    m.vcycle(3, True, m.unit(False))
    g, w = c2_ref[...], w2_ref[...]
    v = e2_ref[...] + jnp.where(w > 0.0, m.spread(gx, gy, sc_ref, scratch, lines), 0.0)
    for _ in range(2):
        v = sweep(v, g, w)
    own = sizes.rows // 2
    g, w = near(c1_ref, own), near(w1_ref, own)
    v = near(e1_ref, own) + near(double_rows(scratch, f32dot_right(v, pc1_ref[...])), own)
    for _ in range(2):
        v = sweep(v, g, w)
    g, d, w = g0_ref[...], d0_ref[...], w0_ref[...]
    v = v0_ref[...] + near(double_rows(scratch, f32dot_right(v, pc0_ref[...])), sizes.rows)
    for _ in range(2):
        v = sweep(v, g, w)
    r = g - d * v + around(v)
    solution_ref[...] = v[: sizes.rows, : sizes.columns]
    residual_ref[...] = r[: sizes.rows, : sizes.columns]


def vmem(count):
    return [pl.BlockSpec(memory_space=pltpu.VMEM)] * count


def call(kernel, sizes, outs, scratch, *operands):
    shapes = [jax.ShapeDtypeStruct(shape, jnp.float32) for shape in outs]
    used = sum(4 * int(np.prod(shape)) for shape in list(outs) + list(scratch))
    used += sum(x.size * x.dtype.itemsize for x in operands)
    return pl.pallas_call(
        lambda *refs: kernel(sizes, *refs),
        out_shape=shapes,
        in_specs=vmem(len(operands)),
        out_specs=vmem(len(outs)),
        scratch_shapes=[pltpu.VMEM(shape, jnp.float32) for shape in scratch],
        compiler_params=pltpu.CompilerParams(vmem_limit_bytes=used + used // 4 + (4 << 20)),
    )(*operands)


def swaps(first, second, axis, spare):
    nx, ny = lax.axis_size("gx"), lax.axis_size("gy")
    count = lax.axis_size(axis)

    def target(gx, gy):
        place = gx if axis == "gx" else gy
        if place in (0, count - 1):
            return (gx ^ 1) * ny + gy if spare == "gx" else gx * ny + (gy ^ 1)
        place = place + 1 if place % 2 else place - 1
        return place * ny + gy if axis == "gx" else gx * ny + place

    pairs = [(gx * ny + gy, target(gx, gy)) for gx in range(nx) for gy in range(ny)]
    other = lax.ppermute(second, ("gx", "gy"), pairs)
    return lax.ppermute(first, axis, [(i, i ^ 1) for i in range(count)]), other


def gather(copies):
    return lax.all_to_all(copies, ("gx", "gy"), 0, 0, tiled=True)


def gather_by_core(copies, nx, ny):
    index = np.arange(nx * ny)
    groups = [index[core::2].tolist() for core in range(2)]
    own = lax.all_to_all(copies, ("gx", "gy"), 0, 0, tiled=True, axis_index_groups=groups)
    return own, lax.ppermute(own, "gy", [(j, j ^ 1) for j in range(ny)])


def body(right_side, shift):
    nx, ny = lax.axis_size("gx"), lax.axis_size("gy")
    rows, columns = right_side.shape
    z = Sizes(rows, columns, nx, ny)
    even = lax.axis_index("gx") % 2 == 0
    last = rows - HALO

    def strips(start, fields):
        return jnp.stack([lax.dynamic_slice(x, (start, 0), (HALO, columns)) for x in fields])

    fields = (right_side, shift)
    later = lax.optimization_barrier(fields)
    rows_a, rows_b = swaps(
        strips(jnp.where(even, last, 0), fields), strips(jnp.where(even, 0, last), later), "gx", "gy")
    ext = [(z.ext_rows[l], z.ext_columns[l]) for l in range(3)]
    strip = (strip_rows(z)[1], 128)
    first, second = call(strip_kernel, z, [strip] * 2, [], right_side, shift, rows_a, rows_b)
    columns_a, columns_b = swaps(first, second, "gy", "gx")
    rc0, rc1 = z.restrict_columns(0), z.restrict_columns(1)
    tiles = (ext[0][1] // 128, ext[0][0], 128)
    g0, d0, w0, v0, c1, d1, w1, v1, d2, w2, packed = call(
        down_kernel, z, [(rows + 2 * NEAR, ext[0][1])] * 4 + [ext[1]] * 4 + [ext[2]] * 2 + [(nx * ny // 2 * 4 * z.p, 128)], [tiles],
        right_side, shift, rows_a, rows_b, columns_a, columns_b, rc0, rc1, z.pack_pair())
    y, other = gather_by_core(packed, nx, ny)
    slabs = [level_shape(z, level) for level in (2, 3, 4)]
    padded, plain = slabs[2][2:], (z.coarse_rows, z.coarse_columns)
    coarsest = [(7,) + padded] * 2 + [(5,) + plain] * 2 + [(2, 6) + padded] * 2 + [(2, 4) + plain] * 2
    d3, d4, w3, w4, ones, e1, c2, e2, packed = call(
        middle_kernel, z, slabs[1:] * 2 + [plain, ext[1], ext[2], ext[2], (nx * ny * 4, 128)],
        [slabs[0]] * 2 + slabs * 3 + [tiles, (4, 12 * z.p, 128)] + coarsest,
        y, other, c1, d1, w1, v1, w2, d2, z.spread_columns(2),
        rc1, z.pack_single())
    y = gather(packed)
    return call(
        up_kernel, z, [(rows, columns)] * 2, slabs[1:] * 3 + [tiles, (2, 6 * z.p, 128)] + coarsest,
        y, d3, d4, w3, w4, ones, c2, w2, e2, c1, w1, e1, g0, d0, w0, v0,
        z.spread_columns(3), rc1.T, rc0.T)


def solution(mesh):
    specs = (P("gx", "gy"), P("gx", "gy"))

    def run(right_side, shift):
        out = body(right_side, shift)
        return out[0], out[1]

    return jax.shard_map(run, mesh=mesh, in_specs=specs, out_specs=specs, check_vma=False)
```

```python
import numpy as np
import jax
import jax.numpy as jnp
from jax import lax
from jax.experimental import pallas as pl
from jax.experimental.pallas import tpu as pltpu
from jax.sharding import PartitionSpec as P

LEVELS = 4
COARSE_SWEEPS = 6
DAMPING = 0.8
HALOS = (40, 16, 8)
HALO = HALOS[0]
NEAR = 8


def f32dot_right(values, onehot):
    high = values.astype(jnp.bfloat16)
    rest = values - high.astype(jnp.float32)
    middle = rest.astype(jnp.bfloat16)
    low = (rest - middle.astype(jnp.float32)).astype(jnp.bfloat16)
    rows = values.shape[0]
    stacked = jnp.concatenate([high, middle, low], axis=0)
    out = jnp.dot(stacked, onehot, preferred_element_type=jnp.float32)
    return (out[2 * rows :] + out[rows : 2 * rows]) + out[:rows]


def around(v):
    rows, columns = v.shape
    up = pltpu.roll(v, 1, 0)
    down = pltpu.roll(v, rows - 1, 0)
    left = pltpu.roll(v, 1, 1)
    right = pltpu.roll(v, columns - 1, 1)
    return (up + down) + (left + right)


def sweep(v, g, w):
    return (1.0 - DAMPING) * v + w * (g + around(v))


class Sizes:
    def __init__(self, rows, columns, nx, ny):
        self.rows, self.columns, self.nx, self.ny = rows, columns, nx, ny
        self.p, self.q = rows // 16, columns // 16
        self.coarse_rows, self.coarse_columns = nx * self.p, ny * self.q
        assert self.p == 8 and 8 * self.q == 128, "block shape"

        def up(n):
            return -(-n // 128) * 128

        self.ext_rows = [(rows >> l) + 2 * HALOS[l] for l in range(3)]
        self.ext_columns = [up((columns >> l) + 2 * HALOS[l]) for l in range(3)]

    def column_at(self, level):
        own, halo, width = self.columns >> level, HALOS[level], self.ext_columns[level]
        lane = np.arange(width)
        inside = (lane < own + halo) | (lane >= width - halo)
        return np.where(lane < own + halo, lane, lane - width), inside

    def restrict_columns(self, level):
        fine, fine_in = self.column_at(level)
        coarse, coarse_in = self.column_at(level + 1)
        hit = (fine[:, None] // 2 == coarse[None, :]) & fine_in[:, None] & coarse_in[None, :]
        return hit.astype(jnp.bfloat16)

    def pack_pair(self):
        width, own = self.ext_columns[1], self.columns >> 1
        x = np.arange(2 * width)
        column = x % width // 2
        target = (x // width) * (own // 2) + (column % 4) * self.q + column // 4
        hit = (target[:, None] == np.arange(own)[None, :]) & (x % width < own)[:, None]
        return hit.astype(jnp.bfloat16)

    def pack_single(self):
        x = np.arange(self.ext_columns[2])[:, None]
        lane = np.arange(128)[None, :]
        hit = (x // 2 == 2 * (lane % self.q) + (lane // self.q) % 2) & (x < self.columns >> 2)
        return hit.astype(jnp.bfloat16)

    def spread_columns(self, level):
        n = 1 << (LEVELS - level)
        column, inside = self.column_at(level - 1)
        m = column // 2
        r = np.arange(n)[:, None, None]
        lane = np.arange(128)[None, :, None]
        hit = (m % n == r) & (m // n + self.q == lane) & inside
        return hit.reshape(n * 128, -1).astype(jnp.bfloat16)


def iota(shape, axis):
    return lax.broadcasted_iota(jnp.int32, shape, axis)


def inside_mask(sizes, level, gx, gy):
    shape = (sizes.ext_rows[level], sizes.ext_columns[level])
    own_r, own_c, halo = sizes.rows >> level, sizes.columns >> level, HALOS[level]
    row, column = iota(shape, 0), iota(shape, 1)
    last_row = jnp.where(gx < sizes.nx - 1, own_r + halo, own_r)
    first_row = jnp.where(gx > 0, own_r + halo, shape[0])
    last_column = jnp.where(gy < sizes.ny - 1, own_c + halo, own_c)
    first_column = jnp.where(gy > 0, shape[1] - halo, shape[1])
    return ((row < last_row) | (row >= first_row)) & ((column < last_column) | (column >= first_column))


def pair_rows(scratch, values):
    rows, columns = values.shape
    outs = []
    for t in range(columns // 128):
        scratch[t, :rows, :] = values[:, t * 128 : (t + 1) * 128]
    for t in range(columns // 128):
        outs.append(scratch[t, pl.ds(0, rows // 2, stride=2), :] + scratch[t, pl.ds(1, rows // 2, stride=2), :])
    return jnp.concatenate(outs, axis=1)


def double_rows(scratch, values):
    rows, columns = values.shape
    for t in range(columns // 128):
        part = values[:, t * 128 : (t + 1) * 128]
        scratch[t, pl.ds(0, rows, stride=2), :] = part
        scratch[t, pl.ds(1, rows, stride=2), :] = part
    return jnp.concatenate([scratch[t, : 2 * rows, :] for t in range(columns // 128)], axis=1)


def repeat(block, out_ref):
    height = block.shape[0]
    for k in range(out_ref.shape[0] // height):
        out_ref[k * height : (k + 1) * height, :] = block


def pack_two(sizes, gy, first, second, scratch, columns_ref, out_ref):
    rows = first.shape[0]
    scratch[0, :rows, :] = f32dot_right(jnp.concatenate([first, second], axis=1), columns_ref[...])
    block = jnp.concatenate([scratch[0, pl.ds(s, sizes.p, stride=4), :] for s in range(4)], axis=0)
    repeat(pltpu.roll(block, lax.rem(gy, 8) * sizes.q, 1), out_ref)


def pack_one(sizes, gy, values, scratch, columns_ref, out_ref):
    rows = values.shape[0]
    scratch[0, :rows, :] = f32dot_right(values, columns_ref[...])
    part = iota((4, 128), 1) // (2 * sizes.q)
    block = scratch[0, pl.ds(0, 4, stride=2), :]
    for k in range(1, 4):
        block = jnp.where(part == k, scratch[0, pl.ds(8 * (k // 2) + k % 2, 4, stride=2), :], block)
    block = jnp.concatenate([block, block], axis=0)
    repeat(pltpu.roll(block, lax.rem(gy, 8) * sizes.q, 1), out_ref)


def near(values, own):
    return jnp.concatenate([values[: own + NEAR], values[values.shape[0] - NEAR :]], axis=0)


def sides(at, first_ref, second_ref):
    even = lax.rem(at, 2) == 0
    first, second = first_ref[...], second_ref[...]
    return jnp.where(even, first, second), jnp.where(even, second, first)


def strip_rows(sizes):
    groups = 128 // HALO
    return groups, -(-2 * sizes.ext_rows[0] // (8 * groups)) * 8


def fold(sizes, strip, step):
    groups, height = strip_rows(sizes)
    lane = iota((height, 128), 1)
    lane = lane if step > 0 else 127 - lane
    out = strip[:height]
    for k in range(1, groups):
        part = strip[k * height : (k + 1) * height]
        part = pltpu.roll(part, k * step % 128, 1)
        if part.shape[0] < height:
            part = jnp.concatenate([part, jnp.zeros((height - part.shape[0], 128), jnp.float32)], axis=0)
        out = jnp.where(lane >= k * HALO, part, out)
    return out


def unfold(sizes, packed, step):
    groups, _ = strip_rows(sizes)
    parts = [packed] + [pltpu.roll(packed, -k * step % 128, 1) for k in range(1, groups)]
    rows = sizes.ext_rows[0]
    out = jnp.concatenate(parts, axis=0)
    return out[:rows], out[rows : 2 * rows]


def strip_kernel(sizes, g_ref, s_ref, rows_a_ref, rows_b_ref, first_ref, second_ref):
    last = sizes.columns - 128
    even = lax.rem(lax.axis_index("gy"), 2) == 0
    below, above = sides(lax.axis_index("gx"), rows_a_ref, rows_b_ref)
    fields = (g_ref[...], below[0], above[0], s_ref[...], below[1], above[1])
    left = fold(sizes, jnp.concatenate([x[:, :128] for x in fields], axis=0), HALO)
    right = fold(sizes, jnp.concatenate([x[:, last:] for x in fields], axis=0), -HALO)
    first_ref[...] = jnp.where(even, right, left)
    second_ref[...] = jnp.where(even, left, right)


def coefficients(sizes, level, gx, gy, sigma):
    d = 4.0 + sigma
    return d, jnp.where(inside_mask(sizes, level, gx, gy), DAMPING / d, 0.0)


def down_kernel(sizes, g_ref, s_ref, rows_a_ref, rows_b_ref, columns_a_ref, columns_b_ref,
                rc0_ref, rc1_ref, pc_ref,
                g0_ref, d0_ref, w0_ref, v0_ref, c1_ref, d1_ref, w1_ref, v1_ref, d2_ref, w2_ref, out_ref, scratch):
    gx, gy = lax.axis_index("gx"), lax.axis_index("gy")
    rows = sizes.ext_rows[0]
    lane = iota((rows, 128), 1)
    below, above = sides(gx, rows_a_ref, rows_b_ref)
    from_right, from_left = sides(gy, columns_a_ref, columns_b_ref)
    from_right, from_left = unfold(sizes, from_right, HALO), unfold(sizes, from_left, -HALO)
    g = jnp.where(lane < HALO, from_right[0], from_left[0])
    sigma = jnp.where(lane < HALO, from_right[1], from_left[1])
    g = jnp.concatenate([jnp.concatenate([g_ref[...], below[0], above[0]], axis=0), g], axis=1)
    sigma = jnp.concatenate([jnp.concatenate([s_ref[...], below[1], above[1]], axis=0), sigma], axis=1)
    d, w = coefficients(sizes, 0, gx, gy, sigma)
    v = w * g
    v = sweep(v, g, w)
    r = g - d * v + around(v)
    for ref, values in ((g0_ref, g), (d0_ref, d), (w0_ref, w), (v0_ref, v)):
        ref[...] = near(values, sizes.rows)
    both = []
    own, halo = sizes.rows // 2, HALOS[1]
    for values in (r, sigma):
        pairs = pair_rows(scratch, values)
        both += [pairs[: own + halo], pairs[pairs.shape[0] - halo :]]
    both = f32dot_right(jnp.concatenate(both, axis=0), rc0_ref[...])
    half = own + 2 * halo
    g, sigma = both[:half], both[half:]
    d, w = coefficients(sizes, 1, gx, gy, sigma)
    v = w * g
    v = sweep(v, g, w)
    r = g - d * v + around(v)
    c1_ref[...] = g
    d1_ref[...] = d
    w1_ref[...] = w
    v1_ref[...] = v
    own = sizes.rows // 4
    source, sigma = pair_rows(scratch, r), pair_rows(scratch, sigma)
    pack_two(sizes, gy, source[:own], sigma[:own], scratch, pc_ref, out_ref)
    d, w = coefficients(sizes, 2, gx, gy, f32dot_right(sigma, rc1_ref[...]))
    d2_ref[...] = d
    w2_ref[...] = w


class Coarse:
    def __init__(self, sizes, first, d_refs, w_refs, g_refs, v_refs, t_refs, coarsest):
        self.z = sizes
        self.first = first
        self.d, self.w, self.g, self.v, self.t = d_refs, w_refs, g_refs, v_refs, t_refs
        self.va, self.vb, self.wk, self.gk, self.wide_v, self.wide_t, self.wide_w, self.wide_g, self.ones = coarsest
        lane = iota((sizes.p, sizes.coarse_columns), 1)
        self.first_lane, self.last_lane = lane == 0, lane == sizes.coarse_columns - 1

    def blocks(self, body):
        p = self.z.p
        if self.z.nx <= 4:
            for gx in range(self.z.nx):
                body((gx + 1) * p)
        else:
            def step(gx, carry):
                body(pl.multiple_of((gx + 1) * p, 8))
                return carry

            lax.fori_loop(0, self.z.nx, step, 0)

    def at(self, ref, s, r, base):
        return ref[s, r, pl.ds(base, self.z.p), :]

    def put(self, ref, s, r, base, value):
        ref[s, r, pl.ds(base, self.z.p), :] = value

    def beside(self, ref, s, r, base, step):
        p = self.z.p
        if isinstance(base, int):
            return ref[s, r, pl.ds(base + step, p), :]
        return ref[s, r, pl.ds(base - p, 3 * p), :][p + step : 2 * p + step]

    def neighbours(self, ref, s, r, n, base):
        columns = self.z.coarse_columns
        if r < n - 1:
            right = self.at(ref, s, r + 1, base)
        else:
            right = jnp.where(self.last_lane, 0.0, pltpu.roll(self.at(ref, s, 0, base), columns - 1, 1))
        if r > 0:
            left = self.at(ref, s, r - 1, base)
        else:
            left = jnp.where(self.first_lane, 0.0, pltpu.roll(self.at(ref, s, n - 1, base), 1, 1))
        down = self.at(ref, s + 1, r, base) if s < n - 1 else self.beside(ref, 0, r, base, 1)
        up = self.at(ref, s - 1, r, base) if s > 0 else self.beside(ref, n - 1, r, base, -1)
        return (up + down) + (left + right)

    def each(self, level, body):
        n = 1 << (LEVELS - level)

        def block(base):
            for s in range(n):
                for r in range(n):
                    body(s, r, n, base)

        self.blocks(block)

    def first_sweep(self, level):
        l = level - self.first

        def body(s, r, n, base):
            self.put(self.v[l], s, r, base, self.at(self.w[l], s, r, base) * self.at(self.g[l], s, r, base))

        self.each(level, body)

    def sweep(self, level, source, target):
        l = level - self.first

        def body(s, r, n, base):
            v = self.at(source, s, r, base)
            total = self.at(self.g[l], s, r, base) + self.neighbours(source, s, r, n, base)
            self.put(target, s, r, base, (1.0 - DAMPING) * v + self.at(self.w[l], s, r, base) * total)

        self.each(level, body)

    def two_sweeps(self, level):
        l = level - self.first
        self.sweep(level, self.v[l], self.t[l])
        self.sweep(level, self.t[l], self.v[l])

    def start(self, level):
        l = level - self.first
        self.first_sweep(level)
        self.sweep(level, self.v[l], self.t[l])
        self.v[l], self.t[l] = self.t[l], self.v[l]

    def residual(self, level, s, r, n, base):
        l = level - self.first
        v = self.at(self.v[l], s, r, base)
        g = self.at(self.g[l], s, r, base)
        return (g - self.at(self.d[l], s, r, base) * v) + self.neighbours(self.v[l], s, r, n, base)

    def restrict(self, level):
        l = level - self.first
        n = 1 << (LEVELS - level)

        def block(base):
            for s in range(n // 2):
                for r in range(n // 2):
                    parts = [self.residual(level, 2 * s + a, 2 * r + b, n, base) for a in (0, 1) for b in (0, 1)]
                    self.put(self.g[l + 1], s, r, base, (parts[0] + parts[1]) + (parts[2] + parts[3]))

        self.blocks(block)

    def prolong(self, level):
        l = level - self.first

        def body(s, r, n, base):
            e = self.at(self.v[l + 1], s // 2, r // 2, base)
            self.put(self.v[l], s, r, base, self.at(self.v[l], s, r, base) + e)

        self.each(level, body)

    def inner(self, ref, s=0, r=0):
        p = self.z.p
        return ref[s, r, p : p + self.z.coarse_rows, :]

    def shifted(self, x, k):
        if k == 0:
            return x
        columns = self.z.coarse_columns
        lane = iota(x.shape, 1)
        keep = lane < columns - k if k > 0 else lane >= -k
        return jnp.where(keep, pltpu.roll(x, -k % columns, 1), 0.0)

    def unit(self, build):
        z = self.z
        top = LEVELS - self.first
        d, w = self.inner(self.d[top]), self.inner(self.w[top])
        missing = 2.0 * (z.coarse_rows + z.coarse_columns)
        for k in range(-2, 3):
            self.wk[k + 2] = self.shifted(w, k)
        self.widen(self.w[top - 1], self.wide_w, 1, False)
        if build:
            lane = iota(d.shape, 1)
            for k in range(-3, 4):
                self.put_shifted(self.va, k, jnp.where((lane < d.shape[1] - k) & (lane >= -k), 1.0, 0.0))
            self.ones[...] = self.coarse_sweeps(False, False)
        return 1.0 / (jnp.sum(d - 4.0, keepdims=True) + missing)

    def shifted_at(self, ref, k, step=0):
        p = self.z.p
        return ref[k + 3, p + step : p + step + self.z.coarse_rows, :]

    def put_shifted(self, ref, k, value):
        ref[k + 3, self.z.p : self.z.p + self.z.coarse_rows, :] = value

    def coarse_sweeps(self, from_zero, with_source):
        at = self.shifted_at
        for turn in range(COARSE_SWEEPS // 3):
            if turn:
                for k in range(-3, 4):
                    self.put_shifted(self.va, k, self.shifted(value, k))
            source, target = self.va, self.vb
            for reach in (2, 1, 0):
                for k in range(-reach, reach + 1):
                    if from_zero and not turn and reach == 2:
                        value = self.wk[k + 2] * self.gk[k + 2]
                    else:
                        total = (at(source, k, -1) + at(source, k, 1)) + (at(source, k - 1) + at(source, k + 1))
                        if with_source:
                            total = self.gk[k + 2] + total
                        value = (1.0 - DAMPING) * at(source, k) + self.wk[k + 2] * total
                    if reach:
                        self.put_shifted(target, k, value)
                source, target = target, source
        return value

    def coarse(self, fresh, unit):
        top = LEVELS - self.first
        g = self.inner(self.g[top])
        for k in range(-2, 3):
            self.gk[k + 2] = self.shifted(g, k)
        if fresh:
            left = jnp.sum(g, keepdims=True)
        else:
            v = self.inner(self.v[top])
            for k in range(-3, 4):
                self.put_shifted(self.va, k, self.shifted(v, k))
            at = self.shifted_at
            beside = (at(self.va, 0, -1) + at(self.va, 0, 1)) + (at(self.va, -1) + at(self.va, 1))
            left = jnp.sum((g - self.inner(self.d[top]) * v) + beside, keepdims=True)
        value = self.coarse_sweeps(fresh, True)
        left = jnp.broadcast_to(left * unit, g.shape)
        self.v[top][0, 0, self.z.p : self.z.p + self.z.coarse_rows, :] = value + left * self.ones[...]

    def widen(self, source, target, reach, padded):
        rows = slice(self.z.p, self.z.p + self.z.coarse_rows) if padded else slice(None)
        for s in range(2):
            for k in range(-reach, 2 + reach):
                target[s, k + reach, rows, :] = self.shifted(self.inner(source, s, k % 2), k // 2)

    def twice(self, restricting):
        l = LEVELS - 1 - self.first
        p, height = self.z.p, self.z.coarse_rows
        rows = slice(p, p + height)

        def at(ref, s, k, step=0):
            return ref[s, k + 2, p + step : p + step + height, :]

        def beside(ref, s, k):
            up = at(ref, 0, k) if s else at(ref, 1, k, -1)
            down = at(ref, 0, k, 1) if s else at(ref, 1, k)
            return (up + down) + (at(ref, s, k - 1) + at(ref, s, k + 1))

        def swept(ref, s, k):
            total = self.wide_g[s, k + 1] + beside(ref, s, k)
            return (1.0 - DAMPING) * at(ref, s, k) + self.wide_w[s, k + 1] * total

        self.widen(self.v[l], self.wide_v, 2, True)
        for s in range(2):
            for k in range(-1, 3):
                self.wide_t[s, k + 2, rows, :] = swept(self.wide_v, s, k)
        parts = []
        for s in range(2):
            for k in range(2):
                if restricting:
                    v = at(self.wide_t, s, k)
                    self.v[l][s, k, rows, :] = v
                    left = self.wide_g[s, k + 1] - self.inner(self.d[l], s, k) * v
                    parts.append(left + beside(self.wide_t, s, k))
                else:
                    self.v[l][s, k, rows, :] = swept(self.wide_t, s, k)
        if restricting:
            self.g[l + 1][0, 0, rows, :] = (parts[0] + parts[1]) + (parts[2] + parts[3])

    def before(self, level, fresh, new_source):
        l = level - self.first
        if level < LEVELS - 1:
            if fresh:
                self.start(level)
            else:
                self.two_sweeps(level)
            self.restrict(level)
            return
        if new_source:
            self.widen(self.g[l], self.wide_g, 1, False)
        if fresh:
            self.first_sweep(level)
        else:
            self.sweep(level, self.v[l], self.t[l])
            self.v[l], self.t[l] = self.t[l], self.v[l]
        self.twice(True)

    def after(self, level):
        self.prolong(level)
        if level < LEVELS - 1:
            self.two_sweeps(level)
        else:
            self.twice(False)

    def vcycle(self, level, fresh, unit):
        if level == LEVELS:
            self.coarse(fresh, unit)
            return
        self.before(level, fresh, fresh)
        self.vcycle(level + 1, True, unit)
        self.after(level)

    def fcycle(self, level, unit):
        if level == LEVELS:
            self.coarse(True, unit)
            return
        self.before(level, True, True)
        self.fcycle(level + 1, unit)
        self.vcycle(level + 1, False, unit)
        self.after(level)

    def clear_ends(self):
        z = self.z
        zero = jnp.zeros((z.p, z.coarse_columns), jnp.float32)
        for refs in (self.v, self.t):
            for ref in refs:
                n = ref.shape[0]
                for s in range(n):
                    for r in range(n):
                        ref[s, r, : z.p, :] = zero
                        ref[s, r, z.p + z.coarse_rows :, :] = zero
        for ref in (self.va, self.vb, self.wide_v.at[0], self.wide_v.at[1], self.wide_t.at[0], self.wide_t.at[1]):
            for k in range(ref.shape[0]):
                ref[k, : z.p, :] = zero
                ref[k, z.p + z.coarse_rows :, :] = zero

    def turned(self, blocks, k):
        q = self.z.q
        part = iota(blocks[0].shape, 1) // q
        out = blocks[-k % 8]
        for x in range(1, 8):
            out = jnp.where(part == x, blocks[(x - k) % 8], out)
        return pltpu.roll(out, -k * q % 128, 1) if k else out

    def take_two(self, even_ref, odd_ref, targets):
        z = self.z
        for gx in range(z.nx):
            for group in range(z.ny // 8):
                lanes = slice(group * 128, (group + 1) * 128)
                for s in range(4):
                    blocks = []
                    for g in range(8):
                        first = (gx * (z.ny // 2) + group * 4 + g // 2) * 4 * z.p + s * z.p
                        blocks.append((even_ref, odd_ref)[g % 2][first : first + z.p, :])
                    for k in range(8):
                        target, add = targets[k // 4]
                        value = self.turned(blocks, k)
                        target[s, k % 4, (gx + 1) * z.p : (gx + 2) * z.p, lanes] = value + add if add else value

    def take_one(self, y_ref, target):
        z = self.z
        low = iota((8, 128), 0) < 4
        for gx in range(z.nx):
            for group in range(z.ny // 8):
                upper, lower = [], []
                for g in range(0, 8, 2):
                    first = (gx * z.ny + group * 8 + g) * 4
                    pair = y_ref[first : first + 8, :]
                    swapped = pltpu.roll(pair, 4, 0)
                    upper += [pair, swapped]
                    lower += [swapped, pair]
                for k in range(4):
                    value = jnp.where(low, self.turned(upper, k), self.turned(lower, k + 4))
                    target[k // 2, k % 2, (gx + 1) * z.p : (gx + 2) * z.p, group * 128 : (group + 1) * 128] = value

    def spread(self, gx, gy, columns_ref, scratch, lines):
        z = self.z
        n = 1 << (LEVELS - self.first)
        above = self.first - 1
        columns = z.coarse_columns
        turn = lax.rem(columns + z.q - gy * z.q, columns)
        start = pl.multiple_of(gx * z.p, 8)
        for s in range(n):
            for r in range(n):
                part = pltpu.roll(self.v[0][s, r, pl.ds(start, 3 * z.p), :], turn, 1)[:, :128]
                lines[r, pl.ds(s, 3 * z.p, stride=n), :] = part
        own, halo = z.rows >> self.first, HALOS[above]
        window = slice(n * z.p - 8, n * z.p + own + 8)
        wide = f32dot_right(jnp.concatenate([lines[r, window, :] for r in range(n)], axis=1), columns_ref[...])
        doubled = double_rows(scratch, jnp.concatenate([wide[8:], wide[:8]], axis=0))
        height = doubled.shape[0]
        return jnp.concatenate([doubled[: 2 * own + halo], doubled[height - halo :]], axis=0)


def level_shape(sizes, level):
    n = 1 << (LEVELS - level)
    return (n, n, sizes.coarse_rows + 2 * sizes.p, sizes.coarse_columns)


def middle_kernel(sizes, y_ref, other_ref, c1_ref, d1_ref, w1_ref, v1_ref, w2l_ref, d2l_ref, sc_ref,
                  rc1_ref, pc_ref,
                  d3_ref, d4_ref, w3_ref, w4_ref, ones_ref, e1_ref, c2_ref, e2_ref, out_ref,
                  d2, w2, g2, g3, g4, v2, v3, v4, t2, t3, t4, scratch, lines, *coarsest):
    gx, gy = lax.axis_index("gx"), lax.axis_index("gy")
    m = Coarse(sizes, 2, [d2, d3_ref, d4_ref], [w2, w3_ref, w4_ref], [g2, g3, g4], [v2, v3, v4], [t2, t3, t4], (*coarsest, ones_ref))
    m.clear_ends()
    core = lax.rem(gy, 2)

    @pl.when(core == 0)
    def _():
        m.take_two(y_ref, other_ref, ((g2, 0.0), (d2, 4.0)))

    @pl.when(core == 1)
    def _():
        m.take_two(other_ref, y_ref, ((g2, 0.0), (d2, 4.0)))

    for l in range(2):
        n = 2 >> l

        def block(base):
            for s in range(n):
                for r in range(n):
                    parts = [m.at(m.d[l], 2 * s + a, 2 * r + b, base) for a in (0, 1) for b in (0, 1)]
                    m.put(m.d[l + 1], s, r, base, ((parts[0] + parts[1]) + (parts[2] + parts[3])) - 12.0)

        m.blocks(block)
    for l in range(3):
        def body(s, r, n, base):
            m.put(m.w[l], s, r, base, DAMPING / m.at(m.d[l], s, r, base))

        m.each(l + 2, body)
    unit = m.unit(True)
    m.fcycle(2, unit)
    m.vcycle(2, False, unit)
    g, d, w = c1_ref[...], d1_ref[...], w1_ref[...]
    v = v1_ref[...] + jnp.where(w > 0.0, m.spread(gx, gy, sc_ref, scratch, lines), 0.0)
    for _ in range(4):
        v = sweep(v, g, w)
    e1_ref[...] = v
    r = g - d * v + around(v)
    g = f32dot_right(pair_rows(scratch, r), rc1_ref[...])
    d, w = d2l_ref[...], w2l_ref[...]
    v = w * g
    v = sweep(v, g, w)
    r = g - d * v + around(v)
    c2_ref[...] = g
    e2_ref[...] = v
    pack_one(sizes, gy, pair_rows(scratch, r[: sizes.rows // 4]), scratch, pc_ref, out_ref)


def up_kernel(sizes, y_ref, d3_ref, d4_ref, w3_ref, w4_ref, ones_ref, c2_ref, w2_ref, e2_ref, c1_ref, w1_ref, e1_ref,
              g0_ref, d0_ref, w0_ref, v0_ref, sc_ref, pc1_ref, pc0_ref,
              solution_ref, residual_ref, g3, g4, v3, v4, t3, t4, scratch, lines, *coarsest):
    gx, gy = lax.axis_index("gx"), lax.axis_index("gy")
    m = Coarse(sizes, 3, [d3_ref, d4_ref], [w3_ref, w4_ref], [g3, g4], [v3, v4], [t3, t4], (*coarsest, ones_ref))
    m.clear_ends()
    m.take_one(y_ref, g3)
    m.vcycle(3, True, m.unit(False))
    g, w = c2_ref[...], w2_ref[...]
    v = e2_ref[...] + jnp.where(w > 0.0, m.spread(gx, gy, sc_ref, scratch, lines), 0.0)
    for _ in range(2):
        v = sweep(v, g, w)
    own = sizes.rows // 2
    g, w = near(c1_ref, own), near(w1_ref, own)
    v = near(e1_ref, own) + near(double_rows(scratch, f32dot_right(v, pc1_ref[...])), own)
    for _ in range(2):
        v = sweep(v, g, w)
    g, d, w = g0_ref[...], d0_ref[...], w0_ref[...]
    v = v0_ref[...] + near(double_rows(scratch, f32dot_right(v, pc0_ref[...])), sizes.rows)
    for _ in range(2):
        v = sweep(v, g, w)
    r = g - d * v + around(v)
    solution_ref[...] = v[: sizes.rows, : sizes.columns]
    residual_ref[...] = r[: sizes.rows, : sizes.columns]


def vmem(count):
    return [pl.BlockSpec(memory_space=pltpu.VMEM)] * count


def call(kernel, sizes, outs, scratch, *operands):
    shapes = [jax.ShapeDtypeStruct(shape, jnp.float32) for shape in outs]
    used = sum(4 * int(np.prod(shape)) for shape in list(outs) + list(scratch))
    used += sum(x.size * x.dtype.itemsize for x in operands)
    return pl.pallas_call(
        lambda *refs: kernel(sizes, *refs),
        out_shape=shapes,
        in_specs=vmem(len(operands)),
        out_specs=vmem(len(outs)),
        scratch_shapes=[pltpu.VMEM(shape, jnp.float32) for shape in scratch],
        compiler_params=pltpu.CompilerParams(vmem_limit_bytes=used + used // 4 + (4 << 20)),
    )(*operands)


def swaps(first, second, axis, spare):
    nx, ny = lax.axis_size("gx"), lax.axis_size("gy")
    count = lax.axis_size(axis)

    def target(gx, gy):
        place = gx if axis == "gx" else gy
        if place in (0, count - 1):
            return (gx ^ 1) * ny + gy if spare == "gx" else gx * ny + (gy ^ 1)
        place = place + 1 if place % 2 else place - 1
        return place * ny + gy if axis == "gx" else gx * ny + place

    pairs = [(gx * ny + gy, target(gx, gy)) for gx in range(nx) for gy in range(ny)]
    other = lax.ppermute(second, ("gx", "gy"), pairs)
    return lax.ppermute(first, axis, [(i, i ^ 1) for i in range(count)]), other


def gather(copies):
    return lax.all_to_all(copies, ("gx", "gy"), 0, 0, tiled=True)


def gather_by_core(copies, nx, ny):
    index = np.arange(nx * ny)
    groups = [index[core::2].tolist() for core in range(2)]
    own = lax.all_to_all(copies, ("gx", "gy"), 0, 0, tiled=True, axis_index_groups=groups)
    return own, lax.ppermute(own, "gy", [(j, j ^ 1) for j in range(ny)])


def body(right_side, shift):
    nx, ny = lax.axis_size("gx"), lax.axis_size("gy")
    rows, columns = right_side.shape
    z = Sizes(rows, columns, nx, ny)
    even = lax.axis_index("gx") % 2 == 0
    last = rows - HALO

    def strips(start):
        return jnp.stack([lax.dynamic_slice(x, (start, 0), (HALO, columns)) for x in (right_side, shift)])

    rows_a, rows_b = swaps(strips(jnp.where(even, last, 0)), strips(jnp.where(even, 0, last)), "gx", "gy")
    ext = [(z.ext_rows[l], z.ext_columns[l]) for l in range(3)]
    strip = (strip_rows(z)[1], 128)
    first, second = call(strip_kernel, z, [strip] * 2, [], right_side, shift, rows_a, rows_b)
    columns_a, columns_b = swaps(first, second, "gy", "gx")
    rc0, rc1 = z.restrict_columns(0), z.restrict_columns(1)
    tiles = (ext[0][1] // 128, ext[0][0], 128)
    g0, d0, w0, v0, c1, d1, w1, v1, d2, w2, packed = call(
        down_kernel, z, [(rows + 2 * NEAR, ext[0][1])] * 4 + [ext[1]] * 4 + [ext[2]] * 2 + [(nx * ny // 2 * 4 * z.p, 128)], [tiles],
        right_side, shift, rows_a, rows_b, columns_a, columns_b, rc0, rc1, z.pack_pair())
    y, other = gather_by_core(packed, nx, ny)
    slabs = [level_shape(z, level) for level in (2, 3, 4)]
    padded, plain = slabs[2][2:], (z.coarse_rows, z.coarse_columns)
    coarsest = [(7,) + padded] * 2 + [(5,) + plain] * 2 + [(2, 6) + padded] * 2 + [(2, 4) + plain] * 2
    d3, d4, w3, w4, ones, e1, c2, e2, packed = call(
        middle_kernel, z, slabs[1:] * 2 + [plain, ext[1], ext[2], ext[2], (nx * ny * 4, 128)],
        [slabs[0]] * 2 + slabs * 3 + [tiles, (4, 12 * z.p, 128)] + coarsest,
        y, other, c1, d1, w1, v1, w2, d2, z.spread_columns(2),
        rc1, z.pack_single())
    y = gather(packed)
    return call(
        up_kernel, z, [(rows, columns)] * 2, slabs[1:] * 3 + [tiles, (2, 6 * z.p, 128)] + coarsest,
        y, d3, d4, w3, w4, ones, c2, w2, e2, c1, w1, e1, g0, d0, w0, v0,
        z.spread_columns(3), rc1.T, rc0.T)


def solution(mesh):
    specs = (P("gx", "gy"), P("gx", "gy"))

    def run(right_side, shift):
        out = body(right_side, shift)
        return out[0], out[1]

    return jax.shard_map(run, mesh=mesh, in_specs=specs, out_specs=specs, check_vma=False)
```
